32 devices in a mesh: pipe: 2 (over y), dp: 4 (over z), tensor: 4 (over x, core).
Axes of the slice: x: 2, y: 2, z: 4, core: 2. Of those that a mesh axis runs over, the one named last changes fastest.
Arguments:
- saved: bfloat16 [2, 2, 256, 1024], P('pipe', None, 'dp'), may hold values from -6 to 6
- top_grad: bfloat16 [2, 256, 1024], P(None, 'dp'), may hold values from -6 to 6
- gain: bfloat16 [2, 1024], P('pipe', 'dp'), may hold values from 0.25 to 1.75
- w_query: bfloat16 [2, 1024, 1536], P('pipe', 'dp', 'tensor'), may hold values from -0.1875 to 0.1875
- w_latent: bfloat16 [2, 1024, 576], P('pipe', 'dp'), may hold values from -0.1875 to 0.1875
- compressed_gain: bfloat16 [2, 512], P('pipe', 'dp'), may hold values from 0.25 to 1.75
- expand_weight: bfloat16 [2, 512, 2048], P('pipe', 'dp', 'tensor'), may hold values from -0.25 to 0.25
- w_output: bfloat16 [2, 1024, 1024], P('pipe', 'tensor', 'dp'), may hold values from -0.1875 to 0.1875
Outputs:
- input_grad: bfloat16 [2, 2, 256, 1024], P('pipe', None, ('dp', 'tensor'))
- grad_gain: float32 [2, 1024], P('pipe', 'dp')
- grad_query: float32 [2, 1024, 1536], P('pipe', 'dp', 'tensor')
- grad_latent: float32 [2, 1024, 576], P('pipe', 'dp')
- grad_latent_gain: float32 [2, 512], P('pipe', 'dp')
- grad_expand: float32 [2, 512, 2048], P('pipe', 'dp', 'tensor')
- grad_output: float32 [2, 1024, 1024], P('pipe', 'tensor', 'dp')
The draws below stay inside these ranges and needn't reach their ends.
All inputs are finite; a program needn't handle non-finite values.
Results may differ from the reference program's by a relative error of at most 0.04.
Values may be sent and summed in bfloat16 or wider, within the bound.
A program may use at most 64 MiB of HBM per device.

```python
import jax
import jax.numpy as jnp
from jax import lax

MODEL_WIDTH = 1024
NOPE = 128
ROPE = 64
VDIM = 128
COMPRESSED_RANK = 512
MB = 2
MB_TOK = 64
SECTION_COUNT = 2
TOKENS = 256
QUERY_COLUMNS = 1536
LATENT_COLUMNS = 576
EXPAND_COLUMNS = 2048
OUTPUT_ROWS = 1024
N_DP = 4
N_TENSOR = 4


def steps_of(rng, dims, pieces, low, top_value):
    def one(position, blocks):
        heights = jax.random.uniform(jax.random.fold_in(jax.random.fold_in(rng, 6), position), (blocks,), jnp.float32, low / len(pieces), top_value / len(pieces))
        return jnp.repeat(jnp.exp(heights), dims[position] // blocks).reshape((-1,) + (1,) * (len(dims) - position - 1))

    level = one(*pieces[0])
    for cut in pieces[1:]:
        level = level * one(*cut)
    return level


def normal_values(rng, dims, deviation, bound, shards=(), kind=jnp.bfloat16):
    array = jax.random.normal(rng, dims, jnp.float32) * deviation
    if len(shards) > 0:
        array = steps_of(rng, dims, shards, -0.22, 0.18) * array
    return jnp.clip(array, min=-bound, max=bound).astype(kind)


def setup_inputs(seed: int = 0) -> dict:
    seeds = jax.random.split(jax.random.key(seed), 9)
    return {
        "saved": normal_values(seeds[0], (SECTION_COUNT, MB, TOKENS, MODEL_WIDTH), 1.0, 6.0, ((0, 2), (2, 4))),
        "top_grad": normal_values(seeds[1], (MB, TOKENS, MODEL_WIDTH), 1.0, 6.0, ((1, 4),)),
        "gain": jnp.clip(1.0 + 0.15 * jax.random.normal(seeds[2], (SECTION_COUNT, MODEL_WIDTH), jnp.float32), 0.25, 1.75).astype(jnp.bfloat16),
        "w_query": normal_values(seeds[3], (SECTION_COUNT, MODEL_WIDTH, QUERY_COLUMNS), MODEL_WIDTH ** -0.5, 0.1875, ((0, 2), (1, 4), (2, 4))),
        "w_latent": normal_values(seeds[4], (SECTION_COUNT, MODEL_WIDTH, LATENT_COLUMNS), MODEL_WIDTH ** -0.5, 0.1875, ((0, 2), (1, 4))),
        "compressed_gain": jnp.clip(1.0 + 0.15 * jax.random.normal(seeds[5], (SECTION_COUNT, COMPRESSED_RANK), jnp.float32), 0.25, 1.75).astype(jnp.bfloat16),
        "expand_weight": normal_values(seeds[6], (SECTION_COUNT, COMPRESSED_RANK, EXPAND_COLUMNS), COMPRESSED_RANK ** -0.5, 0.25, ((0, 2), (1, 4), (2, 4))),
        "w_output": normal_values(seeds[7], (SECTION_COUNT, OUTPUT_ROWS, MODEL_WIDTH), OUTPUT_ROWS ** -0.5, 0.1875, ((0, 2), (1, 4), (2, 4))),
    }


EPS = 1e-06

def root_mean_scale(values, scale):
    return values * lax.rsqrt(lax.optimization_barrier(jnp.mean(values * values, axis=-1, keepdims=True)) + EPS) * scale

def rotary_angles(values):
    length = values.shape[0]
    half = values.shape[-1] // 2
    freq = jnp.exp(-jnp.log(10000.0) * jnp.arange(half, dtype=jnp.float32) / half)
    angle = jnp.arange(length, dtype=jnp.float32)[:, None] * freq[None, :]
    cosine = jnp.cos(angle)[:, None, :]
    sine = jnp.sin(angle)[:, None, :]
    first = values[..., :half]
    second = values[..., half:]
    return jnp.concatenate([first * cosine - second * sine, second * cosine + first * sine], axis=-1)

def branch(normed, w_q, w_lat, latent_norm_gain, w_exp, w_out):
    length = normed.shape[0]
    heads = w_q.shape[1] // (NOPE + ROPE)
    rounded = normed.astype(jnp.bfloat16)
    query = jnp.dot(rounded, w_q, preferred_element_type=jnp.float32).reshape(length, heads, NOPE + ROPE)
    latent_state = jnp.dot(rounded, w_lat, preferred_element_type=jnp.float32)
    compressed_state = root_mean_scale(latent_state[:, :COMPRESSED_RANK], latent_norm_gain).astype(jnp.bfloat16)
    rotary_key_part = rotary_angles(latent_state[:, None, COMPRESSED_RANK:])[:, 0, :]
    expanded = jnp.dot(compressed_state, w_exp, preferred_element_type=jnp.float32).reshape(length, heads, NOPE + VDIM)
    key_nope = expanded[:, :, :NOPE]
    values = expanded[:, :, NOPE:].astype(jnp.bfloat16)
    query_rope = rotary_angles(query[:, :, NOPE:])
    scores = jnp.einsum('qhd,khd->hqk', query[:, :, :NOPE], key_nope) + jnp.einsum('qhd,kd->hqk', query_rope, rotary_key_part)
    scores = scores * (NOPE + ROPE) ** (-0.5)
    causal = jnp.arange(length)[:, None] >= jnp.arange(length)[None, :]
    scores = jnp.where(causal[None], scores, -1e+30)
    weights = jax.nn.softmax(scores, axis=-1).astype(jnp.bfloat16)
    mixed = jnp.einsum('hqk,khd->qhd', weights.astype(jnp.float32), values.astype(jnp.float32))
    mixed = mixed.astype(jnp.bfloat16).reshape(length, heads * VDIM)
    return jnp.dot(mixed, w_out, preferred_element_type=jnp.float32)

def reference(saved, top_grad, gain, w_query, w_latent, compressed_gain, expand_weight, w_output):
    head_groups = N_TENSOR
    dgrads = []
    all_input = []
    upstream = top_grad
    for section_index in reversed(range(SECTION_COUNT)):
        gain32 = gain[section_index].astype(jnp.float32)
        lgain32 = compressed_gain[section_index].astype(jnp.float32)
        lat_w = w_latent[section_index]
        q_groups = w_query[section_index].reshape(MODEL_WIDTH, head_groups, QUERY_COLUMNS // head_groups).transpose(1, 0, 2)
        expand_groups = expand_weight[section_index].reshape(COMPRESSED_RANK, head_groups, EXPAND_COLUMNS // head_groups).transpose(1, 0, 2)
        o_groups = w_output[section_index].reshape(head_groups, OUTPUT_ROWS // head_groups, MODEL_WIDTH)

        def one_sequence(loop_carry, pair):
            x_rows, up_rows = pair
            normed, norm_pull = jax.vjp(root_mean_scale, x_rows.astype(jnp.float32), gain32)
            cot = up_rows.astype(jnp.float32)

            def one_group(wq_g, we_g, wo_g):
                unused, pull = jax.vjp(branch, normed, wq_g, lat_w, lgain32, we_g, wo_g)
                return pull(cot)
            d_norm, d_q, d_lat, d_lg, expand_gradient, d_o = jax.vmap(one_group)(q_groups, expand_groups, o_groups)
            d_normed = lax.optimization_barrier(jnp.sum(d_norm, axis=0))
            dx_norm, d_gain = norm_pull(d_normed)
            dx = (cot + dx_norm).astype(jnp.bfloat16)
            g_q = d_q.astype(jnp.float32).transpose(1, 0, 2).reshape(MODEL_WIDTH, QUERY_COLUMNS)
            expand_weight_grad = expand_gradient.astype(jnp.float32).transpose(1, 0, 2).reshape(COMPRESSED_RANK, EXPAND_COLUMNS)
            g_o = d_o.astype(jnp.float32).reshape(OUTPUT_ROWS, MODEL_WIDTH)
            g_lat = lax.optimization_barrier(jnp.sum(d_lat.astype(jnp.float32), axis=0))
            g_lg = lax.optimization_barrier(jnp.sum(d_lg, axis=0))
            loop_carry = (loop_carry[0] + d_gain, loop_carry[1] + g_q, loop_carry[2] + g_lat, loop_carry[3] + g_lg, loop_carry[4] + expand_weight_grad, loop_carry[5] + g_o)
            return (loop_carry, dx)
        loop_carry = (jnp.zeros((MODEL_WIDTH,), jnp.float32), jnp.zeros((MODEL_WIDTH, QUERY_COLUMNS), jnp.float32), jnp.zeros((MODEL_WIDTH, LATENT_COLUMNS), jnp.float32), jnp.zeros((COMPRESSED_RANK,), jnp.float32), jnp.zeros((COMPRESSED_RANK, EXPAND_COLUMNS), jnp.float32), jnp.zeros((OUTPUT_ROWS, MODEL_WIDTH), jnp.float32))
        section_inputs = []
        for micro in range(MB):
            x_seq = saved[section_index, micro].reshape(N_DP, MB_TOK, MODEL_WIDTH)
            up_seq = upstream[micro].reshape(N_DP, MB_TOK, MODEL_WIDTH)
            loop_carry, dx = lax.scan(one_sequence, loop_carry, (x_seq, up_seq))
            section_inputs.append(dx.reshape(TOKENS, MODEL_WIDTH))
        upstream = jnp.stack(section_inputs)
        all_input.append(upstream)
        dgrads.append(loop_carry)
    all_input = all_input[::-1]
    dgrads = dgrads[::-1]
    input_grad = jnp.stack(all_input)
    outs = [jnp.stack([entry[k] for entry in dgrads]) for k in range(6)]
    return (input_grad, outs[0], outs[1], outs[2], outs[3], outs[4], outs[5])
```

```python
import jax
import jax.numpy as jnp
from jax import lax
import numpy as np
from jax.experimental import pallas as pl
from jax.experimental.pallas import tpu as pltpu
from jax.sharding import PartitionSpec as P

NOPE = 128
ROPE = 64
VDIM = 128
COMPRESSED_RANK = 512


EPS = 1e-06


def passed_along(value, axis, steps):
    count = lax.axis_size(axis)
    first, last = (max(0, -steps), min(count, count - steps))
    return lax.ppermute(value, axis, [(source, source + steps) for source in range(first, last)])


def root_mean_scale(values, scale):
    return values * lax.rsqrt(jnp.mean(values * values, axis=-1, keepdims=True) + EPS) * scale


def rotary_angles(values):
    length = values.shape[0]
    half = values.shape[-1] // 2
    freq = jnp.exp(-jnp.log(10000.0) * jnp.arange(half, dtype=jnp.float32) / half)
    angle = jnp.arange(length, dtype=jnp.float32)[:, None] * freq[None, :]
    cosine = jnp.cos(angle)[:, None, :]
    sine = jnp.sin(angle)[:, None, :]
    first = values[..., :half]
    second = values[..., half:]
    return jnp.concatenate(
        [first * cosine - second * sine, second * cosine + first * sine], axis=-1
    )


def branch(normed, w_q, w_lat, latent_norm_gain, w_exp, w_out):
    length = normed.shape[0]
    heads = w_q.shape[1] // (NOPE + ROPE)
    rounded = normed.astype(jnp.bfloat16)
    query = jnp.dot(rounded, w_q, preferred_element_type=jnp.float32).reshape(
        length, heads, NOPE + ROPE
    )
    latent_state = jnp.dot(rounded, w_lat, preferred_element_type=jnp.float32)
    compressed_state = root_mean_scale(latent_state[:, :COMPRESSED_RANK], latent_norm_gain).astype(
        jnp.bfloat16
    )
    rotary_key_part = rotary_angles(latent_state[:, None, COMPRESSED_RANK:])[:, 0, :]
    expanded = jnp.dot(compressed_state, w_exp, preferred_element_type=jnp.float32).reshape(
        length, heads, NOPE + VDIM
    )
    key_nope = expanded[:, :, :NOPE]
    values = expanded[:, :, NOPE:].astype(jnp.bfloat16)
    query_rope = rotary_angles(query[:, :, NOPE:])
    scores = jnp.einsum("qhd,khd->hqk", query[:, :, :NOPE], key_nope) + jnp.einsum(
        "qhd,kd->hqk", query_rope, rotary_key_part
    )
    scores = scores * (NOPE + ROPE) ** (-0.5)
    causal = jnp.arange(length)[:, None] >= jnp.arange(length)[None, :]
    scores = jnp.where(causal[None], scores, -1e30)
    weights = jax.nn.softmax(scores, axis=-1).astype(jnp.bfloat16)
    mixed = jnp.einsum("hqk,khd->qhd", weights.astype(jnp.float32), values.astype(jnp.float32))
    mixed = mixed.astype(jnp.bfloat16).reshape(length, heads * VDIM)
    return jnp.dot(mixed, w_out, preferred_element_type=jnp.float32)


def shards(saved, top_grad, gain, w_query, w_latent, compressed_gain, expand_weight, w_output):
    gathered = (
        lax.all_gather(gain, "dp", axis=1, tiled=True),
        lax.all_gather(w_query, "dp", axis=1, tiled=True),
        lax.all_gather(w_latent, "dp", axis=1, tiled=True),
        lax.all_gather(compressed_gain, "dp", axis=1, tiled=True),
        lax.all_gather(expand_weight, "dp", axis=1, tiled=True),
        lax.all_gather(w_output, "dp", axis=2, tiled=True),
    )
    gain32 = gathered[0][0].astype(jnp.float32)
    query_all = gathered[1][0]
    latent_all = gathered[2][0]
    lgain32 = gathered[3][0].astype(jnp.float32)
    expand_all = gathered[4][0]
    output_all = gathered[5][0]
    sections = lax.axis_size("pipe")
    section_index = lax.axis_index("pipe")
    tensor_count = lax.axis_size("tensor")
    tensor_rank = lax.axis_index("tensor")
    micro_count = saved.shape[1]
    length = saved.shape[2]
    width = saved.shape[3]
    share = length // tensor_count

    def compute(normed, upstream):
        unused, pull = jax.vjp(
            lambda value: branch(value, query_all, latent_all, lgain32, expand_all, output_all),
            normed,
        )
        return pull(upstream.astype(jnp.float32))[0]

    def skip(normed, upstream):
        return jnp.zeros_like(normed)

    gain_total = jnp.zeros((width,), jnp.float32)
    results = jnp.zeros((micro_count, share, width), jnp.bfloat16)
    stored = jnp.zeros((micro_count, length, width), jnp.bfloat16)
    received = jnp.zeros((length, width), jnp.bfloat16)
    for tick in range(sections + micro_count - 1):
        micro = tick - (sections - 1 - section_index)
        active = jnp.logical_and(micro >= 0, micro < micro_count)
        picked = jnp.clip(micro, 0, micro_count - 1)
        x_rows = lax.dynamic_index_in_dim(saved[0], picked, 0, keepdims=False)
        top_rows = lax.dynamic_index_in_dim(top_grad, picked, 0, keepdims=False)
        arrived = received
        upstream = jnp.where(section_index == sections - 1, top_rows, arrived)
        x_float = x_rows.astype(jnp.float32)
        normed, norm_pull = jax.vjp(root_mean_scale, x_float, gain32)
        branch_grad = lax.cond(active, compute, skip, normed, upstream)
        d_normed = lax.psum(branch_grad.astype(jnp.bfloat16), "tensor").astype(jnp.float32)
        dx_norm, d_gain = norm_pull(d_normed)
        dx = (upstream.astype(jnp.float32) + dx_norm).astype(jnp.bfloat16)
        gain_total = gain_total + jnp.where(active, d_gain, 0.0)
        mine = lax.dynamic_slice_in_dim(dx, tensor_rank * share, share, 0)
        chosen = (jnp.arange(micro_count) == micro)[:, None, None]
        results = jnp.where(chosen, mine[None], results)
        stored = jnp.where(chosen, upstream[None], stored)
        received = passed_along(dx, "pipe", -1)
    totals = (
        jnp.zeros(query_all.shape, jnp.float32),
        jnp.zeros(latent_all.shape, jnp.float32),
        jnp.zeros(lgain32.shape, jnp.float32),
        jnp.zeros(expand_all.shape, jnp.float32),
        jnp.zeros(output_all.shape, jnp.float32),
    )
    for micro_index in range(micro_count):
        normed_again = root_mean_scale(saved[0, micro_index].astype(jnp.float32), gain32)
        unused, weight_pull = jax.vjp(
            lambda w_q, w_lat, lat_gain, w_exp, w_out: branch(
                normed_again, w_q, w_lat, lat_gain, w_exp, w_out
            ),
            query_all,
            latent_all,
            lgain32,
            expand_all,
            output_all,
        )
        cotangents = weight_pull(stored[micro_index].astype(jnp.float32))
        totals = tuple(
            (total + piece.astype(jnp.float32) for total, piece in zip(totals, cotangents))
        )
    gain_part = jnp.where(tensor_rank == 0, gain_total, 0.0)
    grad_q, grad_lat, grad_lg, grad_e, grad_o = totals
    out_q, part_lat, part_lg, out_e, out_o, part_gain = (
        lax.psum_scatter(grad_q.astype(jnp.bfloat16), "dp", scatter_dimension=0, tiled=True).astype(
            jnp.float32
        ),
        lax.psum_scatter(
            grad_lat.astype(jnp.bfloat16), "dp", scatter_dimension=0, tiled=True
        ).astype(jnp.float32),
        lax.psum_scatter(
            grad_lg.astype(jnp.bfloat16), "dp", scatter_dimension=0, tiled=True
        ).astype(jnp.float32),
        lax.psum_scatter(grad_e.astype(jnp.bfloat16), "dp", scatter_dimension=0, tiled=True).astype(
            jnp.float32
        ),
        lax.psum_scatter(grad_o.astype(jnp.bfloat16), "dp", scatter_dimension=1, tiled=True).astype(
            jnp.float32
        ),
        lax.psum_scatter(
            gain_part.astype(jnp.bfloat16), "dp", scatter_dimension=0, tiled=True
        ).astype(jnp.float32),
    )
    out_lat, out_lg, out_gain = (
        lax.psum(part_lat.astype(jnp.bfloat16), "tensor").astype(jnp.float32),
        lax.psum(part_lg.astype(jnp.bfloat16), "tensor").astype(jnp.float32),
        lax.psum(part_gain.astype(jnp.bfloat16), "tensor").astype(jnp.float32),
    )
    return (
        results[None],
        out_gain[None],
        out_q[None],
        out_lat[None],
        out_lg[None],
        out_e[None],
        out_o[None],
    )


MESH = pl.DeviceIdType.MESH
BF = jnp.bfloat16
F32 = jnp.float32


def mm(a, b):
    return lax.dot_general(a, b, (((1,), (0,)), ((), ())), preferred_element_type=F32)


def mm_nt(a, b):
    return lax.dot_general(a, b, (((1,), (1,)), ((), ())), preferred_element_type=F32)


def mm_tn(a, b):
    return lax.dot_general(a, b, (((0,), (0,)), ((), ())), preferred_element_type=F32)


def half_swap(v):
    lane = lax.broadcasted_iota(jnp.int32, v.shape, 1)
    ahead = pltpu.roll(v, v.shape[1] - ROPE // 2, 1)
    behind = pltpu.roll(v, ROPE // 2, 1)
    return jnp.where(lax.rem(lane, ROPE) < ROPE // 2, ahead, behind)


def section_kernel(
    dims,
    saved_ref, top_ref, gain_ref, lgain_ref, wq_ref, wl_ref, we_ref, wo_ref, cos_ref, sin_ref,
    ig_ref, gg_ref, gq_ref, gl_ref, glg_ref, ge_ref, go_ref,
    x_v, xs_v, own_v, sm_v, nm_v, u_v, um_v, cb_v, wq_v, wl_v, we_v, wo_v,
    nc_v, cc_v, uc_v, dl_v, fo_v, fw_v, so_v, sv_v, part_v, rs_v, lp_v, ls_v, dx_v, sg_v, sr_v, st_v,
    dq_v, de_v,
    dp_s, dp_r, x_s, x_r, line_s, line_r, wt_s, wt_r, w_s, w_r, f_s, f_r, z_s, z_r, t_s, t_r,
    b_s, b_r, rs_s, rs_r, p_s, u_r, um_r, uf_s, uf_r, st_s, st_r,
):
    n_pipe, n, n_t, micros, seq = dims
    sec, me, ten = lax.axis_index("pipe"), lax.axis_index("dp"), lax.axis_index("tensor")
    rows = micros * seq
    chunk = seq // n_t
    share = micros * chunk
    width = x_v.shape[1]
    wcol, ccol = wq_v.shape[1], we_v.shape[1]
    rank = n * ccol
    quarter = wl_v.shape[2]
    core = lax.rem(ten, 2)
    partner = ten + 1 - 2 * core
    par = lax.rem(me, 2)
    mate = me + 1 - 2 * par
    group = ten - core + par
    block = me - par + core
    primary = core == par
    secondary = jnp.logical_not(primary)
    last = sec == n_pipe - 1
    lower = jnp.logical_not(last)
    both = jnp.logical_and
    drains = []

    def rcopy(a, b, ss, rs, dev):
        return pltpu.make_async_remote_copy(
            src_ref=a, dst_ref=b, send_sem=ss, recv_sem=rs, device_id=dev, device_id_type=MESH
        )

    def begin(cond, copy):
        @pl.when(cond)
        def _():
            copy.start()

        drains.append((cond, copy))

    def arrived(cond, ref, rs):
        @pl.when(cond)
        def _():
            rcopy(ref, ref, x_s.at[0], rs, dev(me, partner)).wait_recv()

    def dev(d, t):
        return (sec, d, t)

    def cols(j, size):
        return slice(j * size, (j + 1) * size)

    def mine(ref):
        at = pl.ds(pl.multiple_of(ten * chunk, chunk), chunk)
        return jnp.concatenate([ref[m, at] for m in range(micros)], axis=0)

    def by_share(store, ref):
        for j in range(n_t):
            for m in range(micros):
                store(j, m, ref[m, j * chunk : (j + 1) * chunk])

    def x_store(j, m, value):
        x_v[j * share + m * chunk : j * share + (m + 1) * chunk] = value

    def u_store(j, m, value):
        u_v[j, m * chunk : (m + 1) * chunk] = value

    own_v[:, :wcol] = jnp.broadcast_to(gain_ref[...].astype(F32), (8, wcol))
    own_v[:, wcol:] = jnp.broadcast_to(lgain_ref[...].astype(F32), (8, ccol))

    @pl.when(last)
    def _():
        um_v[...] = mine(top_ref)

    @pl.when(both(last, primary))
    def _():
        by_share(u_store, top_ref)

    barrier = pltpu.get_barrier_semaphore()
    for j in range(n_t):
        for d in range(n):
            @pl.when(jnp.logical_or(d != me, j != ten))
            def _():
                pl.semaphore_signal(barrier, inc=1, device_id=dev(d, j), device_id_type=MESH)

        @pl.when(sec > 0)
        def _():
            pl.semaphore_signal(barrier, inc=1, device_id=(sec - 1, me, j), device_id_type=MESH)

        @pl.when(lower)
        def _():
            pl.semaphore_signal(barrier, inc=1, device_id=(sec + 1, me, j), device_id_type=MESH)

    neighbours = jnp.minimum(sec, 1) + jnp.minimum(n_pipe - 1 - sec, 1)
    pl.semaphore_wait(barrier, n * n_t - 1 + neighbours * n_t)

    def spread_dp(k, source, dest):
        for j in range(n):
            begin(j != me, rcopy(source(j), dest.at[me], dp_s.at[k, j], dp_r.at[k, me], dev(j, ten)))

    def collect_dp(k, dest):
        for j in range(n):
            arrived(j != me, dest.at[j], dp_r.at[k, j])

    def spread_z(k, source, dest, slot, rank_to, gate=None):
        for e in range(n):
            cond = jnp.logical_or(e != me, rank_to != ten)
            if gate is not None:
                cond = both(cond, gate)
            begin(cond, rcopy(source(e), dest.at[slot, rank_to], z_s.at[k, e], z_r.at[k, slot], dev(e, rank_to)))

    def relay(k, dest, owned=None):
        for b in range(n):
            here = b == me if owned is None else both(b == me, owned)
            arrived(jnp.logical_not(here), dest.at[b, ten], z_r.at[k, b])
            for j in range(n_t):
                begin(
                    j != ten,
                    rcopy(dest.at[b, ten], dest.at[b, ten], t_s.at[k, b, j], t_r.at[k, b, ten], dev(me, j)),
                )

    def collect(k, dest):
        for b in range(n):
            for j in range(n_t):
                arrived(j != ten, dest.at[b, j], t_r.at[k, b, j])

    def spread_block(k, source, dest, gate=None):
        for e in range(n):
            cond = jnp.logical_or(e != me, secondary)
            if gate is not None:
                cond = both(cond, gate)
            begin(cond, rcopy(source, dest.at[block], b_s.at[k, e], b_r.at[k, block], dev(e, group)))

    def collect_block(k, dest):
        for b in range(n):
            arrived(jnp.logical_or(b != me, secondary), dest.at[b], b_r.at[k, b])

    def line_start(source, at):
        begin(me < n - 1, rcopy(source, at(me), line_s.at[0, 0], line_r.at[me], dev(me + 1, ten)))
        begin(me > 0, rcopy(source, at(me), line_s.at[1, 0], line_r.at[me], dev(me - 1, ten)))

    def line_step(at, s, extra):
        for way, b, valid, more, dest in (
            (0, jnp.maximum(me - 1 - s, 0), me - 1 - s >= 0, me < n - 1, me + 1),
            (1, jnp.minimum(me + 1 + s, n - 1), me + 1 + s <= n - 1, me > 0, me - 1),
        ):
            copy = rcopy(at(b), at(b), line_s.at[way, s + 1], line_r.at[b], dev(dest, ten))

            @pl.when(valid)
            def _():
                copy.wait_recv()

            if s < n - 2:
                begin(both(valid, more), copy)
            extra(b, valid)

    spread_dp(0, lambda j: own_v, sm_v)
    sm_v[me] = own_v[...]
    begin(primary, rcopy(saved_ref, xs_v, x_s.at[0], x_r.at[0], dev(mate, ten)))
    line_start(
        wl_ref.at[pl.ds(pl.multiple_of(ten * quarter, quarter), quarter)], lambda b: wl_v.at[b, ten]
    )
    weights = ((wq_ref, wq_v), (we_ref, we_v), (wo_ref, wo_v))
    for k, (ref, store) in enumerate(weights):
        for i in range(n // 2):
            level = 2 * i + core
            begin(level != me, rcopy(ref, store.at[me], w_s.at[k, i], w_r.at[k, me], dev(level, ten)))
        begin(primary, rcopy(ref, store.at[me], f_s.at[k, me], f_r.at[k, me], dev(me, partner)))
    for s in range(n_t):
        begin(both(last, primary), rcopy(u_v.at[s], u_v.at[s], uf_s.at[s], uf_r.at[s], dev(mate, ten)))
    um_cols = lambda e: um_v.at[:, pl.ds(e * wcol, wcol)]
    spread_z(2, um_cols, uc_v, me, ten, gate=last)

    for j in range(n_t):
        wl_v[me, j] = wl_ref[j * quarter : (j + 1) * quarter]

    @pl.when(primary)
    def _():
        for ref, store in weights:
            store[me] = ref[...]

        by_share(x_store, saved_ref)

    collect_dp(0, sm_v)
    gain = jnp.concatenate([sm_v[d][0:1, :wcol] for d in range(n)], axis=1)
    lgain = jnp.concatenate([sm_v[d][0:1, wcol : wcol + ccol] for d in range(n)], axis=1)
    x_my = mine(saved_ref).astype(F32)
    r_my = lax.rsqrt(jnp.mean(x_my * x_my, axis=1, keepdims=True) + EPS)
    nm_v[...] = (x_my * r_my * gain).astype(BF)
    spread_z(0, lambda e: nm_v.at[:, pl.ds(e * wcol, wcol)], nc_v, me, ten)
    for j in range(n):
        @pl.when(j == me)
        def _():
            nc_v[j, ten] = nm_v[:, cols(j, wcol)]

    @pl.when(secondary)
    def _():
        rcopy(xs_v, xs_v, x_s.at[0], x_r.at[0], dev(me, partner)).wait_recv()
        by_share(x_store, xs_v)

    x32 = x_v[...].astype(F32)
    r = lax.rsqrt(jnp.mean(x32 * x32, axis=1, keepdims=True) + EPS)
    nb = (x32 * r * gain).astype(BF)

    def to_ten(b, valid):
        for j in range(n_t):
            begin(
                both(valid, j != ten),
                rcopy(wl_v.at[b, ten], wl_v.at[b, ten], wt_s.at[b, j], wt_r.at[b, ten], dev(me, j)),
            )

    def take(k):
        store = weights[k][1]
        for d in range(n):
            cond = both(primary, d != me)
            arrived(cond, store.at[d], w_r.at[k, d])
            begin(cond, rcopy(store.at[d], store.at[d], f_s.at[k, d], f_r.at[k, d], dev(me, partner)))
        for d in range(n):
            arrived(secondary, store.at[d], f_r.at[k, d])

    for s in range(n - 1):
        line_step(lambda b: wl_v.at[b, ten], s, to_ten)
    take(0)
    for d in range(n):
        for j in range(n_t):
            arrived(both(d != me, j != ten), wl_v.at[d, j], wt_r.at[d, j])

    wq = wq_v[...].reshape(width, wq_v.shape[2])
    wl = [wl_v[d].reshape(n_t * quarter, wcol) for d in range(n)]
    q = mm(nb, wq)
    lat = jnp.zeros((rows, n_t * quarter), F32)
    for d in range(n):
        lat = lat + mm_nt(nb[:, cols(d, wcol)], wl[d])
    l32 = lat[:, :rank]
    rl = lax.rsqrt(jnp.mean(l32 * l32, axis=1, keepdims=True) + EPS)
    cb = (l32 * rl * lgain).astype(BF)
    cb_v[...] = cb
    my_rows = pl.ds(pl.multiple_of(group * share, share), share)
    spread_z(1, lambda e: cb_v.at[my_rows, pl.ds(e * ccol, ccol)], cc_v, block, group)
    for j in range(n):
        @pl.when(both(j == me, primary))
        def _():
            cc_v[j, ten] = cb_v[my_rows, cols(j, ccol)]

    cosine, sine = cos_ref[...], sin_ref[...]
    lr = lat[:, rank:]
    lr2 = jnp.concatenate([lr, lr], axis=1)
    rk = (lr2 * cosine + half_swap(lr2) * sine).astype(BF)
    lane = lax.broadcasted_iota(jnp.int32, (rows, 2 * ROPE), 1)
    low = lane < ROPE
    q1, q2 = q[:, NOPE : 2 * NOPE], q[:, 2 * NOPE :]
    nope = (q[:, :NOPE], pltpu.roll(jnp.where(low, q2, q1), ROPE, 1))
    qr_all = jnp.where(low, q1, q2)
    qr = qr_all * cosine + half_swap(qr_all) * sine
    row = lax.broadcasted_iota(jnp.int32, (rows, rows), 0)
    col = lax.broadcasted_iota(jnp.int32, (rows, rows), 1)

    def place(i):
        return (i // share) * chunk + lax.rem(i, chunk)

    same = lax.rem(row, share) // chunk == lax.rem(col, share) // chunk
    keep = jnp.logical_and(same, place(row) >= place(col))
    picks = [jnp.where(place(row) + h * seq == col, 1.0, 0.0).astype(BF) for h in range(2)]
    scale = (NOPE + ROPE) ** (-0.5)
    masks = (low, jnp.logical_not(low))
    take(1)
    we = we_v[...].reshape(n * ccol, we_v.shape[2])
    ex = mm(cb, we)
    heads = []
    for h in range(2):
        qn = nope[h].astype(BF)
        kn = ex[:, h * (NOPE + VDIM) : h * (NOPE + VDIM) + NOPE].astype(BF)
        vv = ex[:, h * (NOPE + VDIM) + NOPE : (h + 1) * (NOPE + VDIM)].astype(BF)
        qh = jnp.where(masks[h], qr, 0.0).astype(BF)
        scores = (mm_nt(qn, kn) + mm_nt(qh, rk)) * scale
        scores = jnp.where(keep, scores, -1e30)
        e = jnp.exp(scores - jnp.max(scores, axis=1, keepdims=True))
        w32 = e / jnp.sum(e, axis=1, keepdims=True)
        wb = w32.astype(BF)
        fo_v[:, cols(h, NOPE)] = qn
        fo_v[:, cols(2 + h, NOPE)] = kn
        fo_v[:, cols(5 + h, VDIM)] = mm(wb, vv).astype(BF)
        heads.append((qn, kn, vv, qh, w32, wb))
    fo_v[:, cols(4, NOPE)] = rk

    @pl.when(primary)
    def _():
        fw_v[me] = fo_v[...]

    spread_block(0, fo_v, fw_v, gate=lower)
    take(2)

    for s in range(n_t):
        cond = both(lower, primary)
        arrived(cond, u_v.at[s], u_r.at[s])
        begin(cond, rcopy(u_v.at[s], u_v.at[s], uf_s.at[s], uf_r.at[s], dev(mate, ten)))

    @pl.when(both(lower, primary))
    def _():
        um_v[...] = u_v[ten]

    arrived(both(lower, secondary), um_v, um_r.at[0])
    spread_z(2, um_cols, uc_v, me, ten, gate=lower)
    for j in range(n):
        @pl.when(j == me)
        def _():
            uc_v[j, ten] = um_v[:, cols(j, wcol)]

    for s in range(n_t):
        arrived(secondary, u_v.at[s], uf_r.at[s])

    ub = u_v[...].reshape(rows, width)
    dm = jnp.zeros((rows, wo_v.shape[1]), F32)
    for j in range(n):
        dm = dm + mm_nt(ub[:, cols(j, wcol)], wo_v[j])
    dm = dm.astype(BF)

    def query_grad(slope, kn0, kn1, rk_b):
        dqr = jnp.where(low, mm(slope[0], rk_b), mm(slope[1], rk_b))
        dqr = dqr * cosine - half_swap(dqr) * sine
        turned = pltpu.roll(mm(slope[1], kn1), ROPE, 1)
        return jnp.concatenate(
            [
                mm(slope[0], kn0).astype(BF),
                jnp.where(low, dqr, turned).astype(BF),
                jnp.where(low, turned, dqr).astype(BF),
            ],
            axis=1,
        )

    drk = jnp.zeros((rows, 2 * ROPE), F32)
    slopes, pieces = [], []
    for h, (qn, kn, vv, qh, w32, wb) in enumerate(heads):
        dmh = dm[:, cols(h, VDIM)]
        dw = mm_nt(dmh, vv).astype(BF).astype(F32)
        ds = (w32 * (dw - jnp.sum(dw * w32, axis=1, keepdims=True)) * scale).astype(BF)
        drk = drk + mm_tn(ds, qh)
        slopes.append(ds)
        pieces += [mm_tn(ds, qn).astype(BF), mm_tn(wb, dmh).astype(BF)]
    drk = drk * cosine - half_swap(drk) * sine
    drk = drk + pltpu.roll(drk, ROPE, 1)
    so_v[:, cols(0, NOPE)] = (mm(slopes[0], picks[0]) + mm(slopes[1], picks[1])).astype(BF)
    so_v[:, cols(1, VDIM)] = pieces[1]
    so_v[:, cols(2, VDIM)] = pieces[3]
    dc = mm_nt(jnp.concatenate(pieces, axis=1), we)
    dlg = jnp.sum(dc * l32 * rl, axis=0, keepdims=True)
    dcg = dc * lgain
    dl = rl * dcg - l32 * (rl * rl * rl) * jnp.mean(l32 * dcg, axis=1, keepdims=True)
    dlat = jnp.concatenate([dl.astype(BF), drk[:, :ROPE].astype(BF)], axis=1)
    dq = query_grad(slopes, heads[0][1], heads[1][1], rk)
    dn = mm_nt(dq, wq) + jnp.concatenate([mm(dlat, wl[d]) for d in range(n)], axis=1)
    part_v[...] = dn.astype(BF).reshape(n_t, share, width)
    lp_v[...] = dlat.reshape(n_t, share, dlat.shape[1])
    for k, (source, dest) in enumerate(((part_v, rs_v), (lp_v, ls_v))):
        for s in range(n_t):
            begin(
                jnp.logical_or(s != ten, secondary),
                rcopy(source.at[s], dest.at[group], rs_s.at[k, s], rs_r.at[k, group], dev(block, s)),
            )

    @pl.when(primary)
    def _():
        rs_v[group] = part_v[ten]
        ls_v[group] = lp_v[ten]
        sv_v[me] = so_v[...]

    spread_block(1, so_v, sv_v, gate=lower)
    relay(0, nc_v)
    relay(1, cc_v, owned=primary)

    def collect_shares(k, dest):
        for g in range(n_t):
            arrived(jnp.logical_or(g != ten, secondary), dest.at[g], rs_r.at[k, g])

    collect_shares(0, rs_v)
    dns = jnp.sum(rs_v[...].astype(F32), axis=0)
    dng = dns * gain
    u_my = um_v[...].astype(F32)
    dx = u_my + r_my * dng - x_my * (r_my * r_my * r_my) * jnp.mean(x_my * dng, axis=1, keepdims=True)
    dx_v[...] = dx.astype(BF)
    below = jnp.maximum(sec - 1, 0)
    for i in range(n_t // 2):
        begin(sec > 0, rcopy(dx_v, u_v.at[ten], p_s.at[i], u_r.at[ten], (below, me, 2 * i + par)))
    begin(both(sec > 0, secondary), rcopy(dx_v, um_v, p_s.at[n_t // 2], um_r.at[0], (below, me, ten)))
    collect_shares(1, ls_v)
    dl_v[me, ten] = jnp.sum(ls_v[...].astype(F32), axis=0).astype(BF)
    spread_z(3, lambda e: dl_v.at[me, ten], dl_v, me, ten)
    dgain = jnp.sum(dns * x_my * r_my, axis=0, keepdims=True)
    for j in range(n):
        piece = jnp.concatenate([dgain[:, cols(j, wcol)], dlg[:, cols(j, ccol)]], axis=1)
        sg_v[j] = jnp.broadcast_to(piece, sg_v.shape[1:])
    spread_dp(1, lambda j: sg_v.at[j], sr_v)
    sr_v[me] = sg_v[me]
    spread_block(1, so_v, sv_v, gate=last)
    spread_block(0, fo_v, fw_v, gate=last)
    for m in range(micros):
        ig_ref[m] = dx[m * chunk : (m + 1) * chunk].astype(BF)
    relay(2, uc_v)
    relay(3, dl_v)
    collect_dp(1, sr_v)
    st_v[ten] = jnp.sum(sr_v[...], axis=0)
    for j in range(n_t):
        begin(j != ten, rcopy(st_v.at[ten], st_v.at[ten], st_s.at[j], st_r.at[ten], dev(me, j)))
    collect_block(0, fw_v)
    collect_block(1, sv_v)
    for b in range(n):
        few = sv_v[b, :, :NOPE]
        ds = [jnp.where(same, mm_nt(few, picks[h]), 0.0).astype(BF) for h in range(2)]
        part = lambda i: fw_v[b, :, cols(i, NOPE)]
        dq_v[b] = query_grad(ds, part(2), part(3), part(4))
        for h in range(2):
            de_v[b, :, cols(2 * h, NOPE)] = mm_tn(ds[h], part(h)).astype(BF)
            de_v[b, :, cols(2 * h + 1, NOPE)] = sv_v[b, :, cols(1 + h, VDIM)]
    collect(0, nc_v)
    collect(1, cc_v)
    gq_ref[...] = mm_tn(nc_v[...].reshape(n * rows, wcol), dq_v[...].reshape(n * rows, dq_v.shape[2]))
    ge_ref[...] = mm_tn(cc_v[...].reshape(n * rows, ccol), de_v[...].reshape(n * rows, de_v.shape[2]))
    collect(2, uc_v)
    mixed = fw_v[:, :, 5 * NOPE :].reshape(n * rows, 2 * VDIM)
    go_ref[...] = mm_tn(mixed, uc_v[...].reshape(n * rows, wcol))
    collect(3, dl_v)
    gl_ref[...] = mm_tn(dl_v[...].reshape(n * rows, dl_v.shape[3]), nc_v[...].reshape(n * rows, wcol))
    for j in range(n_t):
        arrived(j != ten, st_v.at[j], st_r.at[j])
    summed = jnp.sum(st_v[...], axis=0)
    gg_ref[...] = summed[0:1, :wcol]
    glg_ref[...] = summed[0:1, wcol:]
    for cond, copy in drains:
        @pl.when(cond)
        def _(copy=copy):
            copy.wait_send()


def hand_over(*refs):
    for source, dest in zip(refs[:7], refs[7:]):
        dest[...] = source[...]


def section_step(saved, top_grad, gain, w_query, w_latent, compressed_gain, expand_weight, w_output):
    n_pipe, n, n_t = (lax.axis_size(a) for a in ("pipe", "dp", "tensor"))
    micros, seq, width = saved.shape[1:]
    wcol, ccol = gain.shape[1], compressed_gain.shape[1]
    rows, share = micros * seq, micros * seq // n_t
    qcols, lcols = w_query.shape[2], w_latent.shape[2]
    ecols, orows = expand_weight.shape[2], w_output.shape[1]
    order = np.arange(rows)
    place = (order // share) * (seq // n_t) + order % (seq // n_t)
    pair = np.arange(2 * ROPE) % (ROPE // 2)
    angle = place[:, None] * np.exp(-np.log(10000.0) * pair / (ROPE // 2))[None, :]
    sign = np.where(np.arange(2 * ROPE) % ROPE < ROPE // 2, -1.0, 1.0)
    cosine = jnp.asarray(np.cos(angle), F32)
    sine = jnp.asarray(np.sin(angle) * sign, F32)
    vm = pl.BlockSpec(memory_space=pltpu.VMEM)
    shape = jax.ShapeDtypeStruct
    sem = lambda *dims: pltpu.SemaphoreType.DMA(dims)
    small = wcol + ccol
    ig, gg, gq, gl, glg, ge, go = pl.pallas_call(
        lambda *refs: section_kernel((n_pipe, n, n_t, micros, seq), *refs),
        name="section_step",
        out_shape=(
            shape((micros, seq // n_t, width), BF),
            shape((1, wcol), F32),
            shape((wcol, qcols), F32),
            shape((lcols, wcol), F32),
            shape((1, ccol), F32),
            shape((ccol, ecols), F32),
            shape((orows, wcol), F32),
        ),
        in_specs=[vm] * 10,
        out_specs=(vm,) * 7,
        scratch_shapes=[
            pltpu.VMEM((rows, width), BF),
            pltpu.VMEM((micros, seq, width), BF),
            pltpu.VMEM((8, small), F32),
            pltpu.VMEM((n, 8, small), F32),
            pltpu.VMEM((share, width), BF),
            pltpu.VMEM((n_t, share, width), BF),
            pltpu.VMEM((share, width), BF),
            pltpu.VMEM((rows, n * ccol), BF),
            pltpu.VMEM((n, wcol, qcols), BF),
            pltpu.VMEM((n, n_t, lcols // n_t, wcol), BF),
            pltpu.VMEM((n, ccol, ecols), BF),
            pltpu.VMEM((n, orows, wcol), BF),
            pltpu.VMEM((n, n_t, share, wcol), BF),
            pltpu.VMEM((n, n_t, share, ccol), BF),
            pltpu.VMEM((n, n_t, share, wcol), BF),
            pltpu.VMEM((n, n_t, share, lcols), BF),
            pltpu.VMEM((rows, 5 * NOPE + orows), BF),
            pltpu.VMEM((n, rows, 5 * NOPE + orows), BF),
            pltpu.VMEM((rows, NOPE + orows), BF),
            pltpu.VMEM((n, rows, NOPE + orows), BF),
            pltpu.VMEM((n_t, share, width), BF),
            pltpu.VMEM((n_t, share, width), BF),
            pltpu.VMEM((n_t, share, lcols), BF),
            pltpu.VMEM((n_t, share, lcols), BF),
            pltpu.VMEM((share, width), BF),
            pltpu.VMEM((n, 8, small), F32),
            pltpu.VMEM((n, 8, small), F32),
            pltpu.VMEM((n_t, 8, small), F32),
            pltpu.VMEM((n, rows, qcols), BF),
            pltpu.VMEM((n, rows, ecols), BF),
            sem(2, n), sem(2, n), sem(1), sem(1), sem(2, n), sem(n), sem(n, n_t), sem(n, n_t),
            sem(3, n // 2), sem(3, n), sem(3, n), sem(3, n), sem(4, n), sem(4, n), sem(4, n, n_t), sem(4, n, n_t),
            sem(2, n), sem(2, n), sem(2, n_t), sem(2, n_t), sem(n_t // 2 + 1), sem(n_t), sem(1), sem(n_t), sem(n_t),
            sem(n_t), sem(n_t),
        ],
        compiler_params=pltpu.CompilerParams(
            collective_id=0, has_side_effects=True, vmem_limit_bytes=60 * 1024 * 1024
        ),
    )(
        saved[0], top_grad, gain, compressed_gain, w_query[0], w_latent[0].T,
        expand_weight[0], w_output[0], cosine, sine,
    )
    parts = (ig, gg, gq, gl, glg, ge, go)
    ig, gg, gq, gl, glg, ge, go = pl.pallas_call(
        hand_over,
        name="hand_over",
        out_shape=tuple(shape(p.shape, p.dtype) for p in parts),
        in_specs=[vm] * 7,
        out_specs=(vm,) * 7,
    )(*parts)
    return ig[None], gg, gq[None], gl.T[None], glg, ge[None], go[None]


def choose(saved, top_grad, gain, w_query, w_latent, compressed_gain, expand_weight, w_output):
    arrays = (saved, top_grad, gain, w_query, w_latent, compressed_gain, expand_weight, w_output)
    n, n_t = lax.axis_size("dp"), lax.axis_size("tensor")
    fits = (
        n % 2 == 0
        and n_t == 4
        and saved.shape[1] == 2
        and saved.shape[2] == ROPE
        and w_query.shape[2] == 2 * (NOPE + ROPE)
        and w_output.shape[1] == 2 * VDIM
        and gain.shape[1] % 128 == 0
        and compressed_gain.shape[1] % 128 == 0
        and n * compressed_gain.shape[1] + ROPE == w_latent.shape[2]
        and w_latent.shape[2] % (16 * n_t) == 0
        and n <= 8
    )
    return section_step(*arrays) if fits else shards(*arrays)


def solution(mesh):
    in_specs = (
        P("pipe", None, "dp", None),
        P(None, "dp", None),
        P("pipe", "dp"),
        P("pipe", "dp", "tensor"),
        P("pipe", "dp", None),
        P("pipe", "dp"),
        P("pipe", "dp", "tensor"),
        P("pipe", "tensor", "dp"),
    )
    out_specs = (
        P("pipe", None, ("dp", "tensor"), None),
        P("pipe", "dp"),
        P("pipe", "dp", "tensor"),
        P("pipe", "dp", None),
        P("pipe", "dp"),
        P("pipe", "dp", "tensor"),
        P("pipe", "tensor", "dp"),
    )
    return jax.shard_map(choose, mesh=mesh, in_specs=in_specs, out_specs=out_specs, check_vma=False)
```

```python
import jax
import jax.numpy as jnp
from jax import lax
import numpy as np
from jax.experimental import pallas as pl
from jax.experimental.pallas import tpu as pltpu
from jax.sharding import PartitionSpec as P

NOPE = 128
ROPE = 64
VDIM = 128
COMPRESSED_RANK = 512


EPS = 1e-06


def passed_along(value, axis, steps):
    count = lax.axis_size(axis)
    first, last = (max(0, -steps), min(count, count - steps))
    return lax.ppermute(value, axis, [(source, source + steps) for source in range(first, last)])


def root_mean_scale(values, scale):
    return values * lax.rsqrt(jnp.mean(values * values, axis=-1, keepdims=True) + EPS) * scale


def rotary_angles(values):
    length = values.shape[0]
    half = values.shape[-1] // 2
    freq = jnp.exp(-jnp.log(10000.0) * jnp.arange(half, dtype=jnp.float32) / half)
    angle = jnp.arange(length, dtype=jnp.float32)[:, None] * freq[None, :]
    cosine = jnp.cos(angle)[:, None, :]
    sine = jnp.sin(angle)[:, None, :]
    first = values[..., :half]
    second = values[..., half:]
    return jnp.concatenate(
        [first * cosine - second * sine, second * cosine + first * sine], axis=-1
    )


def branch(normed, w_q, w_lat, latent_norm_gain, w_exp, w_out):
    length = normed.shape[0]
    heads = w_q.shape[1] // (NOPE + ROPE)
    rounded = normed.astype(jnp.bfloat16)
    query = jnp.dot(rounded, w_q, preferred_element_type=jnp.float32).reshape(
        length, heads, NOPE + ROPE
    )
    latent_state = jnp.dot(rounded, w_lat, preferred_element_type=jnp.float32)
    compressed_state = root_mean_scale(latent_state[:, :COMPRESSED_RANK], latent_norm_gain).astype(
        jnp.bfloat16
    )
    rotary_key_part = rotary_angles(latent_state[:, None, COMPRESSED_RANK:])[:, 0, :]
    expanded = jnp.dot(compressed_state, w_exp, preferred_element_type=jnp.float32).reshape(
        length, heads, NOPE + VDIM
    )
    key_nope = expanded[:, :, :NOPE]
    values = expanded[:, :, NOPE:].astype(jnp.bfloat16)
    query_rope = rotary_angles(query[:, :, NOPE:])
    scores = jnp.einsum("qhd,khd->hqk", query[:, :, :NOPE], key_nope) + jnp.einsum(
        "qhd,kd->hqk", query_rope, rotary_key_part
    )
    scores = scores * (NOPE + ROPE) ** (-0.5)
    causal = jnp.arange(length)[:, None] >= jnp.arange(length)[None, :]
    scores = jnp.where(causal[None], scores, -1e30)
    weights = jax.nn.softmax(scores, axis=-1).astype(jnp.bfloat16)
    mixed = jnp.einsum("hqk,khd->qhd", weights.astype(jnp.float32), values.astype(jnp.float32))
    mixed = mixed.astype(jnp.bfloat16).reshape(length, heads * VDIM)
    return jnp.dot(mixed, w_out, preferred_element_type=jnp.float32)


def shards(saved, top_grad, gain, w_query, w_latent, compressed_gain, expand_weight, w_output):
    gathered = (
        lax.all_gather(gain, "dp", axis=1, tiled=True),
        lax.all_gather(w_query, "dp", axis=1, tiled=True),
        lax.all_gather(w_latent, "dp", axis=1, tiled=True),
        lax.all_gather(compressed_gain, "dp", axis=1, tiled=True),
        lax.all_gather(expand_weight, "dp", axis=1, tiled=True),
        lax.all_gather(w_output, "dp", axis=2, tiled=True),
    )
    gain32 = gathered[0][0].astype(jnp.float32)
    query_all = gathered[1][0]
    latent_all = gathered[2][0]
    lgain32 = gathered[3][0].astype(jnp.float32)
    expand_all = gathered[4][0]
    output_all = gathered[5][0]
    sections = lax.axis_size("pipe")
    section_index = lax.axis_index("pipe")
    tensor_count = lax.axis_size("tensor")
    tensor_rank = lax.axis_index("tensor")
    micro_count = saved.shape[1]
    length = saved.shape[2]
    width = saved.shape[3]
    share = length // tensor_count

    def compute(normed, upstream):
        unused, pull = jax.vjp(
            lambda value: branch(value, query_all, latent_all, lgain32, expand_all, output_all),
            normed,
        )
        return pull(upstream.astype(jnp.float32))[0]

    def skip(normed, upstream):
        return jnp.zeros_like(normed)

    gain_total = jnp.zeros((width,), jnp.float32)
    results = jnp.zeros((micro_count, share, width), jnp.bfloat16)
    stored = jnp.zeros((micro_count, length, width), jnp.bfloat16)
    received = jnp.zeros((length, width), jnp.bfloat16)
    for tick in range(sections + micro_count - 1):
        micro = tick - (sections - 1 - section_index)
        active = jnp.logical_and(micro >= 0, micro < micro_count)
        picked = jnp.clip(micro, 0, micro_count - 1)
        x_rows = lax.dynamic_index_in_dim(saved[0], picked, 0, keepdims=False)
        top_rows = lax.dynamic_index_in_dim(top_grad, picked, 0, keepdims=False)
        arrived = received
        upstream = jnp.where(section_index == sections - 1, top_rows, arrived)
        x_float = x_rows.astype(jnp.float32)
        normed, norm_pull = jax.vjp(root_mean_scale, x_float, gain32)
        branch_grad = lax.cond(active, compute, skip, normed, upstream)
        d_normed = lax.psum(branch_grad.astype(jnp.bfloat16), "tensor").astype(jnp.float32)
        dx_norm, d_gain = norm_pull(d_normed)
        dx = (upstream.astype(jnp.float32) + dx_norm).astype(jnp.bfloat16)
        gain_total = gain_total + jnp.where(active, d_gain, 0.0)
        mine = lax.dynamic_slice_in_dim(dx, tensor_rank * share, share, 0)
        chosen = (jnp.arange(micro_count) == micro)[:, None, None]
        results = jnp.where(chosen, mine[None], results)
        stored = jnp.where(chosen, upstream[None], stored)
        received = passed_along(dx, "pipe", -1)
    totals = (
        jnp.zeros(query_all.shape, jnp.float32),
        jnp.zeros(latent_all.shape, jnp.float32),
        jnp.zeros(lgain32.shape, jnp.float32),
        jnp.zeros(expand_all.shape, jnp.float32),
        jnp.zeros(output_all.shape, jnp.float32),
    )
    for micro_index in range(micro_count):
        normed_again = root_mean_scale(saved[0, micro_index].astype(jnp.float32), gain32)
        unused, weight_pull = jax.vjp(
            lambda w_q, w_lat, lat_gain, w_exp, w_out: branch(
                normed_again, w_q, w_lat, lat_gain, w_exp, w_out
            ),
            query_all,
            latent_all,
            lgain32,
            expand_all,
            output_all,
        )
        cotangents = weight_pull(stored[micro_index].astype(jnp.float32))
        totals = tuple(
            (total + piece.astype(jnp.float32) for total, piece in zip(totals, cotangents))
        )
    gain_part = jnp.where(tensor_rank == 0, gain_total, 0.0)
    grad_q, grad_lat, grad_lg, grad_e, grad_o = totals
    out_q, part_lat, part_lg, out_e, out_o, part_gain = (
        lax.psum_scatter(grad_q.astype(jnp.bfloat16), "dp", scatter_dimension=0, tiled=True).astype(
            jnp.float32
        ),
        lax.psum_scatter(
            grad_lat.astype(jnp.bfloat16), "dp", scatter_dimension=0, tiled=True
        ).astype(jnp.float32),
        lax.psum_scatter(
            grad_lg.astype(jnp.bfloat16), "dp", scatter_dimension=0, tiled=True
        ).astype(jnp.float32),
        lax.psum_scatter(grad_e.astype(jnp.bfloat16), "dp", scatter_dimension=0, tiled=True).astype(
            jnp.float32
        ),
        lax.psum_scatter(grad_o.astype(jnp.bfloat16), "dp", scatter_dimension=1, tiled=True).astype(
            jnp.float32
        ),
        lax.psum_scatter(
            gain_part.astype(jnp.bfloat16), "dp", scatter_dimension=0, tiled=True
        ).astype(jnp.float32),
    )
    out_lat, out_lg, out_gain = (
        lax.psum(part_lat.astype(jnp.bfloat16), "tensor").astype(jnp.float32),
        lax.psum(part_lg.astype(jnp.bfloat16), "tensor").astype(jnp.float32),
        lax.psum(part_gain.astype(jnp.bfloat16), "tensor").astype(jnp.float32),
    )
    return (
        results[None],
        out_gain[None],
        out_q[None],
        out_lat[None],
        out_lg[None],
        out_e[None],
        out_o[None],
    )


MESH = pl.DeviceIdType.MESH
BF = jnp.bfloat16
F32 = jnp.float32


def mm(a, b):
    return lax.dot_general(a, b, (((1,), (0,)), ((), ())), preferred_element_type=F32)


def mm_nt(a, b):
    return lax.dot_general(a, b, (((1,), (1,)), ((), ())), preferred_element_type=F32)


def mm_tn(a, b):
    return lax.dot_general(a, b, (((0,), (0,)), ((), ())), preferred_element_type=F32)


def half_swap(v):
    lane = lax.broadcasted_iota(jnp.int32, v.shape, 1)
    ahead = pltpu.roll(v, v.shape[1] - ROPE // 2, 1)
    behind = pltpu.roll(v, ROPE // 2, 1)
    return jnp.where(lax.rem(lane, ROPE) < ROPE // 2, ahead, behind)


def section_kernel(
    dims,
    saved_ref, top_ref, gain_ref, lgain_ref, wq_ref, wl_ref, we_ref, wo_ref, cos_ref, sin_ref,
    ig_ref, gg_ref, gq_ref, gl_ref, glg_ref, ge_ref, go_ref,
    x_v, xs_v, own_v, sm_v, nm_v, u_v, um_v, cb_v, wq_v, wl_v, we_v, wo_v,
    nc_v, cc_v, uc_v, dl_v, rk_v, ro_v, fo_v, fw_v, so_v, sv_v, part_v, rs_v, lp_v, ls_v, dx_v, sg_v, sr_v, st_v,
    dq_v, de_v,
    dp_s, dp_r, x_s, x_r, wz_s, wz_r, wh_s, wt_s, wt_r, w_s, w_r, f_s, f_r, z_s, z_r, t_s, t_r,
    b_s, b_r, bh_s, rs_s, rs_r, p_s, u_r, um_r, uf_s, uf_r, st_s, st_r,
):
    n_pipe, n, n_t, micros, seq = dims
    sec, me, ten = lax.axis_index("pipe"), lax.axis_index("dp"), lax.axis_index("tensor")
    rows = micros * seq
    chunk = seq // n_t
    share = micros * chunk
    width = x_v.shape[1]
    wcol, ccol = wq_v.shape[1], we_v.shape[1]
    rank = n * ccol
    quarter = wl_v.shape[2]
    core = lax.rem(ten, 2)
    partner = ten + 1 - 2 * core
    par = lax.rem(me, 2)
    mate = me + 1 - 2 * par
    group = ten - core + par
    block = me - par + core
    primary = core == par
    secondary = jnp.logical_not(primary)
    half = me // 2
    near = 2 - half
    middle = jnp.logical_or(me == 1, me == 2)
    last = sec == n_pipe - 1
    lower = jnp.logical_not(last)
    both = jnp.logical_and
    drains = []

    def rcopy(a, b, ss, rs, dev):
        return pltpu.make_async_remote_copy(
            src_ref=a, dst_ref=b, send_sem=ss, recv_sem=rs, device_id=dev, device_id_type=MESH
        )

    def begin(cond, copy):
        @pl.when(cond)
        def _():
            copy.start()

        drains.append((cond, copy))

    def arrived(cond, ref, rs):
        @pl.when(cond)
        def _():
            rcopy(ref, ref, x_s.at[0], rs, dev(me, partner)).wait_recv()

    def dev(d, t):
        return (sec, d, t)

    def cols(j, size):
        return slice(j * size, (j + 1) * size)

    def mine(ref):
        at = pl.ds(pl.multiple_of(ten * chunk, chunk), chunk)
        return jnp.concatenate([ref[m, at] for m in range(micros)], axis=0)

    def by_share(store, ref):
        for j in range(n_t):
            for m in range(micros):
                store(j, m, ref[m, j * chunk : (j + 1) * chunk])

    def x_store(j, m, value):
        x_v[j * share + m * chunk : j * share + (m + 1) * chunk] = value

    def u_store(j, m, value):
        u_v[j, m * chunk : (m + 1) * chunk] = value

    own_v[:, :wcol] = jnp.broadcast_to(gain_ref[...].astype(F32), (8, wcol))
    own_v[:, wcol:] = jnp.broadcast_to(lgain_ref[...].astype(F32), (8, ccol))

    @pl.when(last)
    def _():
        um_v[...] = mine(top_ref)

    @pl.when(both(last, primary))
    def _():
        by_share(u_store, top_ref)

    barrier = pltpu.get_barrier_semaphore()
    for j in range(n_t):
        for d in range(n):
            @pl.when(jnp.logical_or(d != me, j != ten))
            def _():
                pl.semaphore_signal(barrier, inc=1, device_id=dev(d, j), device_id_type=MESH)

        @pl.when(sec > 0)
        def _():
            pl.semaphore_signal(barrier, inc=1, device_id=(sec - 1, me, j), device_id_type=MESH)

        @pl.when(lower)
        def _():
            pl.semaphore_signal(barrier, inc=1, device_id=(sec + 1, me, j), device_id_type=MESH)

    neighbours = jnp.minimum(sec, 1) + jnp.minimum(n_pipe - 1 - sec, 1)
    pl.semaphore_wait(barrier, n * n_t - 1 + neighbours * n_t)

    def spread_dp(k, source, dest):
        for j in range(n):
            begin(j != me, rcopy(source(j), dest.at[me], dp_s.at[k, j], dp_r.at[k, me], dev(j, ten)))

    def collect_dp(k, dest):
        for j in range(n):
            arrived(j != me, dest.at[j], dp_r.at[k, j])

    def spread_z(k, source, dest, slot, rank_to, gate=None):
        for e in range(n):
            cond = jnp.logical_or(e != me, rank_to != ten)
            if gate is not None:
                cond = both(cond, gate)
            begin(cond, rcopy(source(e), dest.at[slot, rank_to], z_s.at[k, e], z_r.at[k, slot], dev(e, rank_to)))

    def relay(k, dest, owned=None, gate=None):
        for b in range(n):
            here = b == me if owned is None else both(b == me, owned)
            away = jnp.logical_not(here)
            arrived(away if gate is None else both(away, gate), dest.at[b, ten], z_r.at[k, b])
            for j in range(n_t):
                begin(
                    j != ten if gate is None else both(j != ten, gate),
                    rcopy(dest.at[b, ten], dest.at[b, ten], t_s.at[k, b, j], t_r.at[k, b, ten], dev(me, j)),
                )

    def collect(k, dest):
        for b in range(n):
            for j in range(n_t):
                arrived(j != ten, dest.at[b, j], t_r.at[k, b, j])

    def spread_block(k, source, dest, gate=None):
        for e in range(n):
            cond = both(jnp.logical_or(e != me, secondary), jnp.logical_or(half == e // 2, near == e))
            if gate is not None:
                cond = both(cond, gate)
            begin(cond, rcopy(source, dest.at[block], b_s.at[k, e], b_r.at[k, block], dev(e, group)))

    def hand_on(k, dest, gate=None):
        for b in range(n):
            cond = both(middle, half != b // 2)
            if gate is not None:
                cond = both(cond, gate)
            arrived(cond, dest.at[b], b_r.at[k, b])
            begin(cond, rcopy(dest.at[b], dest.at[b], bh_s.at[k, b], b_r.at[k, b], dev(mate, ten)))

    def collect_block(k, dest):
        for b in range(n):
            handed = both(middle, half != b // 2)
            cond = both(jnp.logical_or(b != me, secondary), jnp.logical_not(handed))
            arrived(cond, dest.at[b], b_r.at[k, b])

    spread_dp(0, lambda j: own_v, sm_v)
    sm_v[me] = own_v[...]
    begin(primary, rcopy(saved_ref, xs_v, x_s.at[0], x_r.at[0], dev(mate, ten)))
    my_quarter = wl_ref.at[pl.ds(pl.multiple_of(ten * quarter, quarter), quarter)]
    for i, level in enumerate((near, mate)):
        begin(me >= 0, rcopy(my_quarter, wl_v.at[me, ten], wz_s.at[i], wz_r.at[me], dev(level, ten)))
    weights = ((wq_ref, wq_v), (we_ref, we_v), (wo_ref, wo_v))

    def give(k):
        ref, store = weights[k]
        for i in range(n // 2):
            level = 2 * i + core
            begin(level != me, rcopy(ref, store.at[me], w_s.at[k, i], w_r.at[k, me], dev(level, ten)))
        begin(primary, rcopy(ref, store.at[me], f_s.at[k, me], f_r.at[k, me], dev(me, partner)))

    give(0)
    um_cols = lambda e: um_v.at[:, pl.ds(e * wcol, wcol)]
    for j in range(n_t):
        wl_v[me, j] = wl_ref[j * quarter : (j + 1) * quarter]

    @pl.when(primary)
    def _():
        for ref, store in weights:
            store[me] = ref[...]

        by_share(x_store, saved_ref)

    collect_dp(0, sm_v)
    gain = jnp.concatenate([sm_v[d][0:1, :wcol] for d in range(n)], axis=1)
    lgain = jnp.concatenate([sm_v[d][0:1, wcol : wcol + ccol] for d in range(n)], axis=1)
    x_my = mine(saved_ref).astype(F32)
    r_my = lax.rsqrt(jnp.mean(x_my * x_my, axis=1, keepdims=True) + EPS)
    nm_v[...] = (x_my * r_my * gain).astype(BF)
    spread_z(0, lambda e: nm_v.at[:, pl.ds(e * wcol, wcol)], nc_v, me, ten)
    for j in range(n):
        @pl.when(j == me)
        def _():
            nc_v[j, ten] = nm_v[:, cols(j, wcol)]

    def to_ten(b, valid):
        for j in range(n_t):
            begin(
                both(valid, j != ten),
                rcopy(wl_v.at[b, ten], wl_v.at[b, ten], wt_s.at[b, j], wt_r.at[b, ten], dev(me, j)),
            )

    for b in range(n):
        arrived(b != me, wl_v.at[b, ten], wz_r.at[b])
        begin(
            both(middle, half != b // 2),
            rcopy(wl_v.at[b, ten], wl_v.at[b, ten], wh_s.at[b], wz_r.at[b], dev(mate, ten)),
        )
        to_ten(b, b != me)
    give(1)
    give(2)
    for s in range(n_t):
        begin(both(last, primary), rcopy(u_v.at[s], u_v.at[s], uf_s.at[s], uf_r.at[s], dev(mate, ten)))
    spread_z(2, um_cols, uc_v, me, ten, gate=last)

    @pl.when(secondary)
    def _():
        rcopy(xs_v, xs_v, x_s.at[0], x_r.at[0], dev(me, partner)).wait_recv()
        by_share(x_store, xs_v)

    x32 = x_v[...].astype(F32)
    r = lax.rsqrt(jnp.mean(x32 * x32, axis=1, keepdims=True) + EPS)
    nb = (x32 * r * gain).astype(BF)

    def take(k):
        store = weights[k][1]
        for d in range(n):
            cond = both(primary, d != me)
            arrived(cond, store.at[d], w_r.at[k, d])
            begin(cond, rcopy(store.at[d], store.at[d], f_s.at[k, d], f_r.at[k, d], dev(me, partner)))
        for d in range(n):
            arrived(secondary, store.at[d], f_r.at[k, d])

    take(0)
    for d in range(n):
        for j in range(n_t):
            arrived(both(d != me, j != ten), wl_v.at[d, j], wt_r.at[d, j])

    wq = wq_v[...].reshape(width, wq_v.shape[2])
    wl = [wl_v[d].reshape(n_t * quarter, wcol) for d in range(n)]
    q = mm(nb, wq)
    lat = jnp.zeros((rows, n_t * quarter), F32)
    for d in range(n):
        lat = lat + mm_nt(nb[:, cols(d, wcol)], wl[d])
    l32 = lat[:, :rank]
    rl = lax.rsqrt(jnp.mean(l32 * l32, axis=1, keepdims=True) + EPS)
    cb = (l32 * rl * lgain).astype(BF)
    cb_v[...] = cb
    my_rows = pl.ds(pl.multiple_of(group * share, share), share)
    spread_z(1, lambda e: cb_v.at[my_rows, pl.ds(e * ccol, ccol)], cc_v, block, group)
    for j in range(n):
        @pl.when(both(j == me, primary))
        def _():
            cc_v[j, ten] = cb_v[my_rows, cols(j, ccol)]

    cosine, sine = cos_ref[...], sin_ref[...]
    lr = lat[:, rank:]
    lr2 = jnp.concatenate([lr, lr], axis=1)
    rk = (lr2 * cosine + half_swap(lr2) * sine).astype(BF)
    ro_v[...] = rk
    spread_z(4, lambda e: ro_v.at[my_rows], rk_v, block, group)

    @pl.when(primary)
    def _():
        rk_v[me, ten] = ro_v[my_rows]

    relay(0, nc_v)
    lane = lax.broadcasted_iota(jnp.int32, (rows, 2 * ROPE), 1)
    low = lane < ROPE
    q1, q2 = q[:, NOPE : 2 * NOPE], q[:, 2 * NOPE :]
    nope = (q[:, :NOPE], pltpu.roll(jnp.where(low, q2, q1), ROPE, 1))
    qr_all = jnp.where(low, q1, q2)
    qr = qr_all * cosine + half_swap(qr_all) * sine
    row = lax.broadcasted_iota(jnp.int32, (rows, rows), 0)
    col = lax.broadcasted_iota(jnp.int32, (rows, rows), 1)

    def place(i):
        return (i // share) * chunk + lax.rem(i, chunk)

    same = lax.rem(row, share) // chunk == lax.rem(col, share) // chunk
    keep = jnp.logical_and(same, place(row) >= place(col))
    picks = [jnp.where(place(row) + h * seq == col, 1.0, 0.0).astype(BF) for h in range(2)]
    scale = (NOPE + ROPE) ** (-0.5)
    masks = (low, jnp.logical_not(low))
    take(1)
    we = we_v[...].reshape(n * ccol, we_v.shape[2])
    ex = mm(cb, we)
    heads = []
    for h in range(2):
        qn = nope[h].astype(BF)
        kn = ex[:, h * (NOPE + VDIM) : h * (NOPE + VDIM) + NOPE].astype(BF)
        vv = ex[:, h * (NOPE + VDIM) + NOPE : (h + 1) * (NOPE + VDIM)].astype(BF)
        qh = jnp.where(masks[h], qr, 0.0).astype(BF)
        scores = (mm_nt(qn, kn) + mm_nt(qh, rk)) * scale
        scores = jnp.where(keep, scores, -1e30)
        e = jnp.exp(scores - jnp.max(scores, axis=1, keepdims=True))
        w32 = e / jnp.sum(e, axis=1, keepdims=True)
        wb = w32.astype(BF)
        fo_v[:, cols(h, NOPE)] = qn
        fo_v[:, cols(2 + h, NOPE)] = kn
        fo_v[:, cols(4 + h, VDIM)] = mm(wb, vv).astype(BF)
        heads.append((qn, kn, vv, qh, w32, wb))

    @pl.when(primary)
    def _():
        fw_v[me] = fo_v[...]

    spread_block(0, fo_v, fw_v, gate=lower)
    take(2)
    relay(1, cc_v, owned=primary, gate=lower)
    relay(4, rk_v, owned=primary, gate=lower)
    hand_on(0, fw_v, gate=lower)

    for s in range(n_t):
        cond = both(lower, primary)
        arrived(cond, u_v.at[s], u_r.at[s])
        begin(cond, rcopy(u_v.at[s], u_v.at[s], uf_s.at[s], uf_r.at[s], dev(mate, ten)))

    @pl.when(both(lower, primary))
    def _():
        um_v[...] = u_v[ten]

    arrived(both(lower, secondary), um_v, um_r.at[0])
    spread_z(2, um_cols, uc_v, me, ten, gate=lower)
    for j in range(n):
        @pl.when(j == me)
        def _():
            uc_v[j, ten] = um_v[:, cols(j, wcol)]

    for s in range(n_t):
        arrived(secondary, u_v.at[s], uf_r.at[s])

    ub = u_v[...].reshape(rows, width)
    dm = jnp.zeros((rows, wo_v.shape[1]), F32)
    for j in range(n):
        dm = dm + mm_nt(ub[:, cols(j, wcol)], wo_v[j])
    dm = dm.astype(BF)

    def query_grad(slope, kn0, kn1, rk_b):
        dqr = jnp.where(low, mm(slope[0], rk_b), mm(slope[1], rk_b))
        dqr = dqr * cosine - half_swap(dqr) * sine
        turned = pltpu.roll(mm(slope[1], kn1), ROPE, 1)
        return jnp.concatenate(
            [
                mm(slope[0], kn0).astype(BF),
                jnp.where(low, dqr, turned).astype(BF),
                jnp.where(low, turned, dqr).astype(BF),
            ],
            axis=1,
        )

    drk = jnp.zeros((rows, 2 * ROPE), F32)
    slopes, pieces = [], []
    for h, (qn, kn, vv, qh, w32, wb) in enumerate(heads):
        dmh = dm[:, cols(h, VDIM)]
        dw = mm_nt(dmh, vv).astype(BF).astype(F32)
        ds = (w32 * (dw - jnp.sum(dw * w32, axis=1, keepdims=True)) * scale).astype(BF)
        drk = drk + mm_tn(ds, qh)
        slopes.append(ds)
        pieces += [mm_tn(ds, qn).astype(BF), mm_tn(wb, dmh).astype(BF)]
    drk = drk * cosine - half_swap(drk) * sine
    drk = drk + pltpu.roll(drk, ROPE, 1)
    so_v[:, cols(0, NOPE)] = (mm(slopes[0], picks[0]) + mm(slopes[1], picks[1])).astype(BF)
    so_v[:, cols(1, VDIM)] = pieces[1]
    so_v[:, cols(2, VDIM)] = pieces[3]
    dc = mm_nt(jnp.concatenate(pieces, axis=1), we)
    dlg = jnp.sum(dc * l32 * rl, axis=0, keepdims=True)
    dcg = dc * lgain
    dl = rl * dcg - l32 * (rl * rl * rl) * jnp.mean(l32 * dcg, axis=1, keepdims=True)
    dlat = jnp.concatenate([dl.astype(BF), drk[:, :ROPE].astype(BF)], axis=1)
    dq = query_grad(slopes, heads[0][1], heads[1][1], rk)
    dn = mm_nt(dq, wq) + jnp.concatenate([mm(dlat, wl[d]) for d in range(n)], axis=1)
    part_v[...] = dn.astype(BF).reshape(n_t, share, width)
    lp_v[...] = dlat.reshape(n_t, share, dlat.shape[1])
    for k, (source, dest) in enumerate(((part_v, rs_v), (lp_v, ls_v))):
        for s in range(n_t):
            begin(
                jnp.logical_or(s != ten, secondary),
                rcopy(source.at[s], dest.at[group], rs_s.at[k, s], rs_r.at[k, group], dev(block, s)),
            )

    @pl.when(primary)
    def _():
        rs_v[group] = part_v[ten]
        ls_v[group] = lp_v[ten]
        sv_v[me] = so_v[...]

    spread_block(1, so_v, sv_v, gate=lower)

    def collect_shares(k, dest):
        for g in range(n_t):
            arrived(jnp.logical_or(g != ten, secondary), dest.at[g], rs_r.at[k, g])

    collect_shares(0, rs_v)
    dns = jnp.sum(rs_v[...].astype(F32), axis=0)
    dng = dns * gain
    u_my = um_v[...].astype(F32)
    dx = u_my + r_my * dng - x_my * (r_my * r_my * r_my) * jnp.mean(x_my * dng, axis=1, keepdims=True)
    dx_v[...] = dx.astype(BF)
    below = jnp.maximum(sec - 1, 0)
    for i in range(n_t // 2):
        begin(sec > 0, rcopy(dx_v, u_v.at[ten], p_s.at[i], u_r.at[ten], (below, me, 2 * i + par)))
    begin(both(sec > 0, secondary), rcopy(dx_v, um_v, p_s.at[n_t // 2], um_r.at[0], (below, me, ten)))
    collect_shares(1, ls_v)
    dl_v[me, ten] = jnp.sum(ls_v[...].astype(F32), axis=0).astype(BF)
    spread_z(3, lambda e: dl_v.at[me, ten], dl_v, me, ten)
    dgain = jnp.sum(dns * x_my * r_my, axis=0, keepdims=True)
    for j in range(n):
        piece = jnp.concatenate([dgain[:, cols(j, wcol)], dlg[:, cols(j, ccol)]], axis=1)
        sg_v[j] = jnp.broadcast_to(piece, sg_v.shape[1:])
    spread_dp(1, lambda j: sg_v.at[j], sr_v)
    sr_v[me] = sg_v[me]
    spread_block(1, so_v, sv_v, gate=last)
    spread_block(0, fo_v, fw_v, gate=last)
    for m in range(micros):
        ig_ref[m] = dx[m * chunk : (m + 1) * chunk].astype(BF)
    relay(1, cc_v, owned=primary, gate=last)
    relay(4, rk_v, owned=primary, gate=last)
    relay(2, uc_v)
    hand_on(1, sv_v)
    relay(3, dl_v)
    hand_on(0, fw_v, gate=last)
    collect_dp(1, sr_v)
    st_v[ten] = jnp.sum(sr_v[...], axis=0)
    for j in range(n_t):
        begin(j != ten, rcopy(st_v.at[ten], st_v.at[ten], st_s.at[j], st_r.at[ten], dev(me, j)))
    collect_block(0, fw_v)
    collect_block(1, sv_v)
    collect(4, rk_v)
    for b in range(n):
        few = sv_v[b, :, :NOPE]
        ds = [jnp.where(same, mm_nt(few, picks[h]), 0.0).astype(BF) for h in range(2)]
        part = lambda i: fw_v[b, :, cols(i, NOPE)]
        dq_v[b] = query_grad(ds, part(2), part(3), rk_v[b].reshape(rows, 2 * ROPE))
        for h in range(2):
            de_v[b, :, cols(2 * h, NOPE)] = mm_tn(ds[h], part(h)).astype(BF)
            de_v[b, :, cols(2 * h + 1, NOPE)] = sv_v[b, :, cols(1 + h, VDIM)]
    collect(0, nc_v)
    collect(1, cc_v)
    gq_ref[...] = mm_tn(nc_v[...].reshape(n * rows, wcol), dq_v[...].reshape(n * rows, dq_v.shape[2]))
    ge_ref[...] = mm_tn(cc_v[...].reshape(n * rows, ccol), de_v[...].reshape(n * rows, de_v.shape[2]))
    collect(2, uc_v)
    mixed = fw_v[:, :, 4 * NOPE :].reshape(n * rows, 2 * VDIM)
    go_ref[...] = mm_tn(mixed, uc_v[...].reshape(n * rows, wcol))
    collect(3, dl_v)
    gl_ref[...] = mm_tn(dl_v[...].reshape(n * rows, dl_v.shape[3]), nc_v[...].reshape(n * rows, wcol))
    for j in range(n_t):
        arrived(j != ten, st_v.at[j], st_r.at[j])
    summed = jnp.sum(st_v[...], axis=0)
    gg_ref[...] = summed[0:1, :wcol]
    glg_ref[...] = summed[0:1, wcol:]
    for cond, copy in drains:
        @pl.when(cond)
        def _(copy=copy):
            copy.wait_send()


def hand_over(*refs):
    for source, dest in zip(refs[:7], refs[7:]):
        dest[...] = source[...]


def section_step(saved, top_grad, gain, w_query, w_latent, compressed_gain, expand_weight, w_output):
    n_pipe, n, n_t = (lax.axis_size(a) for a in ("pipe", "dp", "tensor"))
    micros, seq, width = saved.shape[1:]
    wcol, ccol = gain.shape[1], compressed_gain.shape[1]
    rows, share = micros * seq, micros * seq // n_t
    qcols, lcols = w_query.shape[2], w_latent.shape[2]
    ecols, orows = expand_weight.shape[2], w_output.shape[1]
    order = np.arange(rows)
    place = (order // share) * (seq // n_t) + order % (seq // n_t)
    pair = np.arange(2 * ROPE) % (ROPE // 2)
    angle = place[:, None] * np.exp(-np.log(10000.0) * pair / (ROPE // 2))[None, :]
    sign = np.where(np.arange(2 * ROPE) % ROPE < ROPE // 2, -1.0, 1.0)
    cosine = jnp.asarray(np.cos(angle), F32)
    sine = jnp.asarray(np.sin(angle) * sign, F32)
    vm = pl.BlockSpec(memory_space=pltpu.VMEM)
    shape = jax.ShapeDtypeStruct
    kept = pltpu.VMEM
    sem = lambda *dims: pltpu.SemaphoreType.DMA(dims)
    small = wcol + ccol
    ig, gg, gq, gl, glg, ge, go = pl.pallas_call(
        lambda *refs: section_kernel((n_pipe, n, n_t, micros, seq), *refs),
        name="section_step",
        out_shape=(
            kept((micros, seq // n_t, width), BF),
            kept((1, wcol), F32),
            kept((wcol, qcols), F32),
            kept((lcols, wcol), F32),
            kept((1, ccol), F32),
            kept((ccol, ecols), F32),
            kept((orows, wcol), F32),
        ),
        in_specs=[vm] * 10,
        out_specs=(vm,) * 7,
        scratch_shapes=[
            pltpu.VMEM((rows, width), BF),
            pltpu.VMEM((micros, seq, width), BF),
            pltpu.VMEM((8, small), F32),
            pltpu.VMEM((n, 8, small), F32),
            pltpu.VMEM((share, width), BF),
            pltpu.VMEM((n_t, share, width), BF),
            pltpu.VMEM((share, width), BF),
            pltpu.VMEM((rows, n * ccol), BF),
            pltpu.VMEM((n, wcol, qcols), BF),
            pltpu.VMEM((n, n_t, lcols // n_t, wcol), BF),
            pltpu.VMEM((n, ccol, ecols), BF),
            pltpu.VMEM((n, orows, wcol), BF),
            pltpu.VMEM((n, n_t, share, wcol), BF),
            pltpu.VMEM((n, n_t, share, ccol), BF),
            pltpu.VMEM((n, n_t, share, wcol), BF),
            pltpu.VMEM((n, n_t, share, lcols), BF),
            pltpu.VMEM((n, n_t, share, 2 * ROPE), BF),
            pltpu.VMEM((rows, 2 * ROPE), BF),
            pltpu.VMEM((rows, 4 * NOPE + orows), BF),
            pltpu.VMEM((n, rows, 4 * NOPE + orows), BF),
            pltpu.VMEM((rows, NOPE + orows), BF),
            pltpu.VMEM((n, rows, NOPE + orows), BF),
            pltpu.VMEM((n_t, share, width), BF),
            pltpu.VMEM((n_t, share, width), BF),
            pltpu.VMEM((n_t, share, lcols), BF),
            pltpu.VMEM((n_t, share, lcols), BF),
            pltpu.VMEM((share, width), BF),
            pltpu.VMEM((n, 8, small), F32),
            pltpu.VMEM((n, 8, small), F32),
            pltpu.VMEM((n_t, 8, small), F32),
            pltpu.VMEM((n, rows, qcols), BF),
            pltpu.VMEM((n, rows, ecols), BF),
            sem(2, n), sem(2, n), sem(1), sem(1), sem(2), sem(n), sem(n), sem(n, n_t), sem(n, n_t),
            sem(3, n // 2), sem(3, n), sem(3, n), sem(3, n), sem(5, n), sem(5, n), sem(5, n, n_t), sem(5, n, n_t),
            sem(2, n), sem(2, n), sem(2, n), sem(2, n_t), sem(2, n_t), sem(n_t // 2 + 1), sem(n_t), sem(1), sem(n_t), sem(n_t),
            sem(n_t), sem(n_t),
        ],
        compiler_params=pltpu.CompilerParams(
            collective_id=0, has_side_effects=True, vmem_limit_bytes=60 * 1024 * 1024
        ),
    )(
        saved[0], top_grad, gain, compressed_gain, w_query[0], w_latent[0].T,
        expand_weight[0], w_output[0], cosine, sine,
    )
    parts = [pltpu.with_memory_space_constraint(p, pltpu.VMEM) for p in (ig, gg, gq, gl, glg, ge, go)]
    ig, gg, gq, gl, glg, ge, go = pl.pallas_call(
        hand_over,
        name="hand_over",
        out_shape=tuple(shape(p.shape, p.dtype) for p in parts),
        in_specs=[vm] * 7,
        out_specs=(vm,) * 7,
    )(*parts)
    return ig[None], gg, gq[None], gl.T[None], glg, ge[None], go[None]


def choose(saved, top_grad, gain, w_query, w_latent, compressed_gain, expand_weight, w_output):
    arrays = (saved, top_grad, gain, w_query, w_latent, compressed_gain, expand_weight, w_output)
    n, n_t = lax.axis_size("dp"), lax.axis_size("tensor")
    fits = (
        n == 4
        and n_t == 4
        and saved.shape[1] == 2
        and saved.shape[2] == ROPE
        and w_query.shape[2] == 2 * (NOPE + ROPE)
        and w_output.shape[1] == 2 * VDIM
        and gain.shape[1] % 128 == 0
        and compressed_gain.shape[1] % 128 == 0
        and n * compressed_gain.shape[1] + ROPE == w_latent.shape[2]
        and w_latent.shape[2] % (16 * n_t) == 0
    )
    return section_step(*arrays) if fits else shards(*arrays)


def solution(mesh):
    in_specs = (
        P("pipe", None, "dp", None),
        P(None, "dp", None),
        P("pipe", "dp"),
        P("pipe", "dp", "tensor"),
        P("pipe", "dp", None),
        P("pipe", "dp"),
        P("pipe", "dp", "tensor"),
        P("pipe", "tensor", "dp"),
    )
    out_specs = (
        P("pipe", None, ("dp", "tensor"), None),
        P("pipe", "dp"),
        P("pipe", "dp", "tensor"),
        P("pipe", "dp", None),
        P("pipe", "dp"),
        P("pipe", "dp", "tensor"),
        P("pipe", "tensor", "dp"),
    )
    return jax.shard_map(choose, mesh=mesh, in_specs=in_specs, out_specs=out_specs, check_vma=False)
```

```python
import jax
import jax.numpy as jnp
from jax import lax
import numpy as np
from jax.experimental import pallas as pl
from jax.experimental.pallas import tpu as pltpu
from jax.sharding import PartitionSpec as P

NOPE = 128
ROPE = 64
VDIM = 128
COMPRESSED_RANK = 512


EPS = 1e-06


def passed_along(value, axis, steps):
    count = lax.axis_size(axis)
    first, last = (max(0, -steps), min(count, count - steps))
    return lax.ppermute(value, axis, [(source, source + steps) for source in range(first, last)])


def root_mean_scale(values, scale):
    return values * lax.rsqrt(jnp.mean(values * values, axis=-1, keepdims=True) + EPS) * scale


def rotary_angles(values):
    length = values.shape[0]
    half = values.shape[-1] // 2
    freq = jnp.exp(-jnp.log(10000.0) * jnp.arange(half, dtype=jnp.float32) / half)
    angle = jnp.arange(length, dtype=jnp.float32)[:, None] * freq[None, :]
    cosine = jnp.cos(angle)[:, None, :]
    sine = jnp.sin(angle)[:, None, :]
    first = values[..., :half]
    second = values[..., half:]
    return jnp.concatenate(
        [first * cosine - second * sine, second * cosine + first * sine], axis=-1
    )


def branch(normed, w_q, w_lat, latent_norm_gain, w_exp, w_out):
    length = normed.shape[0]
    heads = w_q.shape[1] // (NOPE + ROPE)
    rounded = normed.astype(jnp.bfloat16)
    query = jnp.dot(rounded, w_q, preferred_element_type=jnp.float32).reshape(
        length, heads, NOPE + ROPE
    )
    latent_state = jnp.dot(rounded, w_lat, preferred_element_type=jnp.float32)
    compressed_state = root_mean_scale(latent_state[:, :COMPRESSED_RANK], latent_norm_gain).astype(
        jnp.bfloat16
    )
    rotary_key_part = rotary_angles(latent_state[:, None, COMPRESSED_RANK:])[:, 0, :]
    expanded = jnp.dot(compressed_state, w_exp, preferred_element_type=jnp.float32).reshape(
        length, heads, NOPE + VDIM
    )
    key_nope = expanded[:, :, :NOPE]
    values = expanded[:, :, NOPE:].astype(jnp.bfloat16)
    query_rope = rotary_angles(query[:, :, NOPE:])
    scores = jnp.einsum("qhd,khd->hqk", query[:, :, :NOPE], key_nope) + jnp.einsum(
        "qhd,kd->hqk", query_rope, rotary_key_part
    )
    scores = scores * (NOPE + ROPE) ** (-0.5)
    causal = jnp.arange(length)[:, None] >= jnp.arange(length)[None, :]
    scores = jnp.where(causal[None], scores, -1e30)
    weights = jax.nn.softmax(scores, axis=-1).astype(jnp.bfloat16)
    mixed = jnp.einsum("hqk,khd->qhd", weights.astype(jnp.float32), values.astype(jnp.float32))
    mixed = mixed.astype(jnp.bfloat16).reshape(length, heads * VDIM)
    return jnp.dot(mixed, w_out, preferred_element_type=jnp.float32)


def shards(saved, top_grad, gain, w_query, w_latent, compressed_gain, expand_weight, w_output):
    gathered = (
        lax.all_gather(gain, "dp", axis=1, tiled=True),
        lax.all_gather(w_query, "dp", axis=1, tiled=True),
        lax.all_gather(w_latent, "dp", axis=1, tiled=True),
        lax.all_gather(compressed_gain, "dp", axis=1, tiled=True),
        lax.all_gather(expand_weight, "dp", axis=1, tiled=True),
        lax.all_gather(w_output, "dp", axis=2, tiled=True),
    )
    gain32 = gathered[0][0].astype(jnp.float32)
    query_all = gathered[1][0]
    latent_all = gathered[2][0]
    lgain32 = gathered[3][0].astype(jnp.float32)
    expand_all = gathered[4][0]
    output_all = gathered[5][0]
    sections = lax.axis_size("pipe")
    section_index = lax.axis_index("pipe")
    tensor_count = lax.axis_size("tensor")
    tensor_rank = lax.axis_index("tensor")
    micro_count = saved.shape[1]
    length = saved.shape[2]
    width = saved.shape[3]
    share = length // tensor_count

    def compute(normed, upstream):
        unused, pull = jax.vjp(
            lambda value: branch(value, query_all, latent_all, lgain32, expand_all, output_all),
            normed,
        )
        return pull(upstream.astype(jnp.float32))[0]

    def skip(normed, upstream):
        return jnp.zeros_like(normed)

    gain_total = jnp.zeros((width,), jnp.float32)
    results = jnp.zeros((micro_count, share, width), jnp.bfloat16)
    stored = jnp.zeros((micro_count, length, width), jnp.bfloat16)
    received = jnp.zeros((length, width), jnp.bfloat16)
    for tick in range(sections + micro_count - 1):
        micro = tick - (sections - 1 - section_index)
        active = jnp.logical_and(micro >= 0, micro < micro_count)
        picked = jnp.clip(micro, 0, micro_count - 1)
        x_rows = lax.dynamic_index_in_dim(saved[0], picked, 0, keepdims=False)
        top_rows = lax.dynamic_index_in_dim(top_grad, picked, 0, keepdims=False)
        arrived = received
        upstream = jnp.where(section_index == sections - 1, top_rows, arrived)
        x_float = x_rows.astype(jnp.float32)
        normed, norm_pull = jax.vjp(root_mean_scale, x_float, gain32)
        branch_grad = lax.cond(active, compute, skip, normed, upstream)
        d_normed = lax.psum(branch_grad.astype(jnp.bfloat16), "tensor").astype(jnp.float32)
        dx_norm, d_gain = norm_pull(d_normed)
        dx = (upstream.astype(jnp.float32) + dx_norm).astype(jnp.bfloat16)
        gain_total = gain_total + jnp.where(active, d_gain, 0.0)
        mine = lax.dynamic_slice_in_dim(dx, tensor_rank * share, share, 0)
        chosen = (jnp.arange(micro_count) == micro)[:, None, None]
        results = jnp.where(chosen, mine[None], results)
        stored = jnp.where(chosen, upstream[None], stored)
        received = passed_along(dx, "pipe", -1)
    totals = (
        jnp.zeros(query_all.shape, jnp.float32),
        jnp.zeros(latent_all.shape, jnp.float32),
        jnp.zeros(lgain32.shape, jnp.float32),
        jnp.zeros(expand_all.shape, jnp.float32),
        jnp.zeros(output_all.shape, jnp.float32),
    )
    for micro_index in range(micro_count):
        normed_again = root_mean_scale(saved[0, micro_index].astype(jnp.float32), gain32)
        unused, weight_pull = jax.vjp(
            lambda w_q, w_lat, lat_gain, w_exp, w_out: branch(
                normed_again, w_q, w_lat, lat_gain, w_exp, w_out
            ),
            query_all,
            latent_all,
            lgain32,
            expand_all,
            output_all,
        )
        cotangents = weight_pull(stored[micro_index].astype(jnp.float32))
        totals = tuple(
            (total + piece.astype(jnp.float32) for total, piece in zip(totals, cotangents))
        )
    gain_part = jnp.where(tensor_rank == 0, gain_total, 0.0)
    grad_q, grad_lat, grad_lg, grad_e, grad_o = totals
    out_q, part_lat, part_lg, out_e, out_o, part_gain = (
        lax.psum_scatter(grad_q.astype(jnp.bfloat16), "dp", scatter_dimension=0, tiled=True).astype(
            jnp.float32
        ),
        lax.psum_scatter(
            grad_lat.astype(jnp.bfloat16), "dp", scatter_dimension=0, tiled=True
        ).astype(jnp.float32),
        lax.psum_scatter(
            grad_lg.astype(jnp.bfloat16), "dp", scatter_dimension=0, tiled=True
        ).astype(jnp.float32),
        lax.psum_scatter(grad_e.astype(jnp.bfloat16), "dp", scatter_dimension=0, tiled=True).astype(
            jnp.float32
        ),
        lax.psum_scatter(grad_o.astype(jnp.bfloat16), "dp", scatter_dimension=1, tiled=True).astype(
            jnp.float32
        ),
        lax.psum_scatter(
            gain_part.astype(jnp.bfloat16), "dp", scatter_dimension=0, tiled=True
        ).astype(jnp.float32),
    )
    out_lat, out_lg, out_gain = (
        lax.psum(part_lat.astype(jnp.bfloat16), "tensor").astype(jnp.float32),
        lax.psum(part_lg.astype(jnp.bfloat16), "tensor").astype(jnp.float32),
        lax.psum(part_gain.astype(jnp.bfloat16), "tensor").astype(jnp.float32),
    )
    return (
        results[None],
        out_gain[None],
        out_q[None],
        out_lat[None],
        out_lg[None],
        out_e[None],
        out_o[None],
    )


MESH = pl.DeviceIdType.MESH
BF = jnp.bfloat16
F32 = jnp.float32


def mm(a, b):
    return lax.dot_general(a, b, (((1,), (0,)), ((), ())), preferred_element_type=F32)


def mm_nt(a, b):
    return lax.dot_general(a, b, (((1,), (1,)), ((), ())), preferred_element_type=F32)


def mm_tn(a, b):
    return lax.dot_general(a, b, (((0,), (0,)), ((), ())), preferred_element_type=F32)


def half_swap(v):
    lane = lax.broadcasted_iota(jnp.int32, v.shape, 1)
    ahead = pltpu.roll(v, v.shape[1] - ROPE // 2, 1)
    behind = pltpu.roll(v, ROPE // 2, 1)
    return jnp.where(lax.rem(lane, ROPE) < ROPE // 2, ahead, behind)


def section_kernel(
    dims,
    saved_ref, top_ref, gain_ref, lgain_ref, wq_ref, wl_ref, we_ref, wo_ref, cos_ref, sin_ref,
    ig_ref, gg_ref, gq_ref, gl_ref, glg_ref, ge_ref, go_ref,
    x_v, xs_v, own_v, sm_v, nm_v, u_v, um_v, cb_v, wq_v, wl_v, we_v, wo_v,
    nc_v, cc_v, uc_v, dl_v, rk_v, ro_v, fo_v, fw_v, so_v, sv_v, part_v, rs_v, lp_v, ls_v, dx_v, sg_v, sr_v,
    dq_v, de_v,
    dp_s, dp_r, x_s, x_r, wz_s, wz_r, wh_s, wt_s, wt_r, w_s, w_r, f_s, f_r, z_s, z_r, zl_r, t_s, ta_r, tb_r,
    b_s, b_r, bh_s, rs_s, rs_r, p_s, u_r, um_r, uf_s, uf_r, sg_s, sg_r,
):
    n_pipe, n, n_t, micros, seq = dims
    sec, me, ten = lax.axis_index("pipe"), lax.axis_index("dp"), lax.axis_index("tensor")
    rows = micros * seq
    chunk = seq // n_t
    share = micros * chunk
    width = x_v.shape[1]
    wcol, ccol = wq_v.shape[1], we_v.shape[1]
    rank = n * ccol
    quarter = wl_v.shape[2]
    core = lax.rem(ten, 2)
    partner = ten + 1 - 2 * core
    opposite = lax.rem(ten + 2, n_t)
    par = lax.rem(me, 2)
    mate = me + 1 - 2 * par
    group = ten - core + par
    block = me - par + core
    primary = core == par
    secondary = jnp.logical_not(primary)
    half = me // 2
    near = 2 - half
    middle = jnp.logical_or(me == 1, me == 2)
    last = sec == n_pipe - 1
    lower = jnp.logical_not(last)
    both = jnp.logical_and
    drains = []

    def rcopy(a, b, ss, rs, dev):
        return pltpu.make_async_remote_copy(
            src_ref=a, dst_ref=b, send_sem=ss, recv_sem=rs, device_id=dev, device_id_type=MESH
        )

    def begin(cond, copy, sent=False):
        @pl.when(cond)
        def _():
            copy.start()

        if not sent:
            drains.append((cond, copy))

    def settle(cond, ref, ss):
        drains.append((cond, rcopy(ref, ref, ss, x_r.at[0], dev(me, partner))))

    def arrived(cond, ref, rs):
        @pl.when(cond)
        def _():
            rcopy(ref, ref, x_s.at[0], rs, dev(me, partner)).wait_recv()

    def dev(d, t):
        return (sec, d, t)

    def cols(j, size):
        return slice(j * size, (j + 1) * size)

    def mine(ref):
        at = pl.ds(pl.multiple_of(ten * chunk, chunk), chunk)
        return jnp.concatenate([ref[m, at] for m in range(micros)], axis=0)

    def by_share(store, ref):
        for j in range(n_t):
            for m in range(micros):
                store(j, m, ref[m, j * chunk : (j + 1) * chunk])

    def x_store(j, m, value):
        x_v[j * share + m * chunk : j * share + (m + 1) * chunk] = value

    def u_store(j, m, value):
        u_v[j, m * chunk : (m + 1) * chunk] = value

    own_v[:, :wcol] = jnp.broadcast_to(gain_ref[...].astype(F32), (8, wcol))
    own_v[:, wcol:] = jnp.broadcast_to(lgain_ref[...].astype(F32), (8, ccol))

    @pl.when(last)
    def _():
        um_v[...] = mine(top_ref)

    @pl.when(both(last, primary))
    def _():
        by_share(u_store, top_ref)

    barrier = pltpu.get_barrier_semaphore()
    for j in range(n_t):
        for d in range(n):
            @pl.when(jnp.logical_or(d != me, j != ten))
            def _():
                pl.semaphore_signal(barrier, inc=1, device_id=dev(d, j), device_id_type=MESH)

        @pl.when(sec > 0)
        def _():
            pl.semaphore_signal(barrier, inc=1, device_id=(sec - 1, me, j), device_id_type=MESH)

        @pl.when(lower)
        def _():
            pl.semaphore_signal(barrier, inc=1, device_id=(sec + 1, me, j), device_id_type=MESH)

    neighbours = jnp.minimum(sec, 1) + jnp.minimum(n_pipe - 1 - sec, 1)
    pl.semaphore_wait(barrier, n * n_t - 1 + neighbours * n_t)

    def spread_dp(k, source, dest):
        for j in range(n):
            begin(j != me, rcopy(source(j), dest.at[me], dp_s.at[k], dp_r.at[k], dev(j, ten)), sent=True)
        settle(me >= 0, dest.at[pl.ds(0, n - 1)], dp_s.at[k])

    def collect_dp(k, dest):
        arrived(me >= 0, dest.at[pl.ds(0, n - 1)], dp_r.at[k])

    def spread_z(k, source, dest, slot, rank_to, gate=None):
        for e in range(n):
            cond = jnp.logical_or(e != me, rank_to != ten)
            if gate is not None:
                cond = both(cond, gate)
            rs = zl_r.at[slot] if k == 3 else z_r.at[k]
            begin(cond, rcopy(source(e), dest.at[slot, rank_to], z_s.at[k], rs, dev(e, rank_to)), sent=True)
        on = me >= 0 if gate is None else gate
        if k in (1, 4):
            settle(both(on, primary), dest.at[0, pl.ds(0, n - 1)], z_s.at[k])
            settle(both(on, secondary), dest.at[0, pl.ds(0, n)], z_s.at[k])
        else:
            settle(on, dest.at[0, pl.ds(0, n - 1)], z_s.at[k])

    def relay(k, dest, gate):
        def share_slot(b):
            for to, rs in ((opposite, ta_r), (partner, tb_r)):
                copy = rcopy(dest.at[b, ten], dest.at[b, ten], t_s.at[k], rs.at[k], dev(me, to))
                begin(gate, copy, sent=True)

        if k == 3:
            for b in range(n):
                arrived(both(b != me, gate), dest.at[b, ten], zl_r.at[b])
                share_slot(b)
        else:
            few, every = dest.at[pl.ds(0, n - 1), ten], dest.at[pl.ds(0, n), ten]
            if k in (1, 4):
                arrived(both(gate, primary), few, z_r.at[k])
                arrived(both(gate, secondary), every, z_r.at[k])
            else:
                arrived(gate, few, z_r.at[k])
            for b in range(n):
                share_slot(b)

    def pass_on(k, dest):
        arrived(me >= 0, dest.at[pl.ds(0, n), opposite], ta_r.at[k])
        for b in range(n):
            at = dest.at[b, opposite]
            begin(me >= 0, rcopy(at, at, t_s.at[k], tb_r.at[k], dev(me, partner)), sent=True)
        settle(me >= 0, dest.at[pl.ds(0, n - 1)], t_s.at[k])

    def collect(k, dest):
        arrived(me >= 0, dest.at[pl.ds(0, 2)], tb_r.at[k])

    def landing(k, b):
        return sv_v.at[b] if k == 3 else fw_v.at[b, k]

    def spread_block(k, gate, across):
        source = so_v if k == 3 else fo_v.at[k]
        for e in range(n):
            wanted = near == e if across else both(half == e // 2, jnp.logical_or(e != me, secondary))
            copy = rcopy(source, landing(k, block), b_s.at[k], b_r.at[k, block], dev(e, group))
            begin(both(wanted, gate), copy, sent=True)
        if across:
            several = lambda c: sv_v.at[pl.ds(0, c)] if k == 3 else fw_v.at[pl.ds(0, c), k]
            settle(both(gate, primary), several(2), b_s.at[k])
            settle(both(gate, secondary), several(3), b_s.at[k])

    def hand_on(k, gate):
        for b in range(n):
            cond = both(both(middle, half != b // 2), gate)
            at = landing(k, b)
            arrived(cond, at, b_r.at[k, b])
            begin(cond, rcopy(at, at, bh_s.at[k], b_r.at[k, b], dev(mate, ten)), sent=True)
        two = sv_v.at[pl.ds(0, 2)] if k == 3 else fw_v.at[pl.ds(0, 2), k]
        settle(both(middle, gate), two, bh_s.at[k])

    def collect_block(k):
        for b in range(n):
            handed = both(middle, half != b // 2)
            cond = both(jnp.logical_or(b != me, secondary), jnp.logical_not(handed))
            arrived(cond, landing(k, b), b_r.at[k, b])

    spread_dp(0, lambda j: own_v, sm_v)
    sm_v[me] = own_v[...]
    my_quarter = wl_ref.at[pl.ds(pl.multiple_of(ten * quarter, quarter), quarter)]
    for level in (near, mate):
        begin(me >= 0, rcopy(my_quarter, wl_v.at[me, ten], wz_s.at[0], wz_r.at[me], dev(level, ten)), sent=True)
    settle(me >= 0, wl_v.at[0, pl.ds(0, 2)], wz_s.at[0])
    weights = ((wq_ref, wq_v), (we_ref, we_v), (wo_ref, wo_v))

    begin(primary, rcopy(saved_ref, xs_v, x_s.at[0], x_r.at[0], dev(mate, ten)))

    def give(k, gate=True):
        ref, store = weights[k]
        for i in range(n // 2):
            level = 2 * i + core
            copy = rcopy(ref, store.at[me], w_s.at[k], w_r.at[k, me], dev(level, ten))
            begin(both(level != me, gate), copy, sent=True)
        settle(both(primary, gate), store.at[pl.ds(0, n // 2 - 1)], w_s.at[k])
        settle(both(secondary, gate), store.at[pl.ds(0, n // 2)], w_s.at[k])
        copy = rcopy(ref, store.at[me], f_s.at[k], f_r.at[k], dev(me, partner))
        begin(both(primary, gate), copy, sent=True)

    def give_rest(gate):
        give(1, gate)
        for s in range(n_t):
            copy = rcopy(u_v.at[s], u_v.at[s], uf_s.at[0], uf_r.at[0], dev(mate, ten))
            begin(both(both(last, primary), gate), copy, sent=True)
        give(2, gate)
        spread_z(2, um_cols, uc_v, me, ten, gate=both(last, gate))

    um_cols = lambda e: um_v.at[:, pl.ds(e * wcol, wcol)]
    give(0)
    give_rest(jnp.logical_not(middle))

    for j in range(n_t):
        wl_v[me, j] = wl_ref[j * quarter : (j + 1) * quarter]

    @pl.when(primary)
    def _():
        for ref, store in weights:
            store[me] = ref[...]

        by_share(x_store, saved_ref)

    def to_ten(b, valid):
        for j in range(n_t):
            begin(
                both(valid, j != ten),
                rcopy(wl_v.at[b, ten], wl_v.at[b, ten], wt_s.at[0], wt_r.at[0], dev(me, j)),
                sent=True,
            )

    for b in range(n):
        arrived(b != me, wl_v.at[b, ten], wz_r.at[b])
        begin(
            both(middle, half != b // 2),
            rcopy(wl_v.at[b, ten], wl_v.at[b, ten], wh_s.at[0], wz_r.at[b], dev(mate, ten)),
            sent=True,
        )
        to_ten(b, b != me)
    settle(middle, wl_v.at[0, pl.ds(0, 2)], wh_s.at[0])
    wl_peers = wl_v.at[pl.ds(0, n - 1), pl.ds(0, n_t - 1)]
    settle(me >= 0, wl_peers, wt_s.at[0])
    give_rest(middle)

    collect_dp(0, sm_v)
    gain = jnp.concatenate([sm_v[d][0:1, :wcol] for d in range(n)], axis=1)
    lgain = jnp.concatenate([sm_v[d][0:1, wcol : wcol + ccol] for d in range(n)], axis=1)
    x_my = mine(saved_ref).astype(F32)
    r_my = lax.rsqrt(jnp.mean(x_my * x_my, axis=1, keepdims=True) + EPS)
    nm_v[...] = (x_my * r_my * gain).astype(BF)
    spread_z(0, lambda e: nm_v.at[:, pl.ds(e * wcol, wcol)], nc_v, me, ten)
    for j in range(n):
        @pl.when(j == me)
        def _():
            nc_v[j, ten] = nm_v[:, cols(j, wcol)]

    @pl.when(secondary)
    def _():
        rcopy(xs_v, xs_v, x_s.at[0], x_r.at[0], dev(me, partner)).wait_recv()
        by_share(x_store, xs_v)

    x32 = x_v[...].astype(F32)
    r = lax.rsqrt(jnp.mean(x32 * x32, axis=1, keepdims=True) + EPS)
    nb = (x32 * r * gain).astype(BF)

    def take(k):
        store = weights[k][1]
        for d in range(n):
            cond = both(primary, d != me)
            arrived(cond, store.at[d], w_r.at[k, d])
            begin(cond, rcopy(store.at[d], store.at[d], f_s.at[k], f_r.at[k], dev(me, partner)), sent=True)
        settle(primary, store, f_s.at[k])
        arrived(secondary, store, f_r.at[k])

    take(0)
    arrived(me >= 0, wl_peers, wt_r.at[0])

    wq = wq_v[...].reshape(width, wq_v.shape[2])
    wl = [wl_v[d].reshape(n_t * quarter, wcol) for d in range(n)]
    q = mm(nb, wq)
    lat = jnp.zeros((rows, n_t * quarter), F32)
    for d in range(n):
        lat = lat + mm_nt(nb[:, cols(d, wcol)], wl[d])
    l32 = lat[:, :rank]
    rl = lax.rsqrt(jnp.mean(l32 * l32, axis=1, keepdims=True) + EPS)
    cb = (l32 * rl * lgain).astype(BF)
    cb_v[...] = cb
    my_rows = pl.ds(pl.multiple_of(group * share, share), share)
    spread_z(1, lambda e: cb_v.at[my_rows, pl.ds(e * ccol, ccol)], cc_v, block, group)
    for j in range(n):
        @pl.when(both(j == me, primary))
        def _():
            cc_v[j, ten] = cb_v[my_rows, cols(j, ccol)]

    cosine, sine = cos_ref[...], sin_ref[...]
    lr = lat[:, rank:]
    lr2 = jnp.concatenate([lr, lr], axis=1)
    rk = (lr2 * cosine + half_swap(lr2) * sine).astype(BF)
    ro_v[...] = rk
    spread_z(4, lambda e: ro_v.at[my_rows], rk_v, block, group)

    @pl.when(primary)
    def _():
        rk_v[me, ten] = ro_v[my_rows]

    lane = lax.broadcasted_iota(jnp.int32, (rows, 2 * ROPE), 1)
    low = lane < ROPE
    q1, q2 = q[:, NOPE : 2 * NOPE], q[:, 2 * NOPE :]
    nope = (q[:, :NOPE], pltpu.roll(jnp.where(low, q2, q1), ROPE, 1))
    for h in range(2):
        fo_v[0, :, cols(h, NOPE)] = nope[h].astype(BF)
    spread_block(0, lower, True)
    spread_block(0, lower, False)
    qr_all = jnp.where(low, q1, q2)
    qr = qr_all * cosine + half_swap(qr_all) * sine
    row = lax.broadcasted_iota(jnp.int32, (rows, rows), 0)
    col = lax.broadcasted_iota(jnp.int32, (rows, rows), 1)

    def place(i):
        return (i // share) * chunk + lax.rem(i, chunk)

    same = lax.rem(row, share) // chunk == lax.rem(col, share) // chunk
    keep = jnp.logical_and(same, place(row) >= place(col))
    picks = [jnp.where(place(row) + h * seq == col, 1.0, 0.0).astype(BF) for h in range(2)]
    scale = (NOPE + ROPE) ** (-0.5)
    masks = (low, jnp.logical_not(low))
    take(1)
    we = we_v[...].reshape(n * ccol, we_v.shape[2])
    ex = mm(cb, we)
    for h in range(2):
        fo_v[1, :, cols(h, NOPE)] = ex[:, cols(2 * h, NOPE)].astype(BF)
    spread_block(1, lower, True)
    spread_block(1, lower, False)
    heads = []
    for h in range(2):
        qn = nope[h].astype(BF)
        kn = ex[:, h * (NOPE + VDIM) : h * (NOPE + VDIM) + NOPE].astype(BF)
        vv = ex[:, h * (NOPE + VDIM) + NOPE : (h + 1) * (NOPE + VDIM)].astype(BF)
        qh = jnp.where(masks[h], qr, 0.0).astype(BF)
        scores = (mm_nt(qn, kn) + mm_nt(qh, rk)) * scale
        scores = jnp.where(keep, scores, -1e30)
        e = jnp.exp(scores - jnp.max(scores, axis=1, keepdims=True))
        w32 = e / jnp.sum(e, axis=1, keepdims=True)
        wb = w32.astype(BF)
        fo_v[2, :, cols(h, VDIM)] = mm(wb, vv).astype(BF)
        heads.append((qn, kn, vv, qh, w32, wb))

    @pl.when(primary)
    def _():
        fw_v[me] = fo_v[...]

    spread_block(2, lower, True)
    spread_block(2, lower, False)
    take(2)
    relay(0, nc_v, gate=lower)
    relay(1, cc_v, gate=lower)
    relay(4, rk_v, gate=lower)
    for k in range(3):
        hand_on(k, lower)

    for s in range(n_t):
        cond = both(lower, primary)
        arrived(cond, u_v.at[s], u_r.at[s])
        begin(cond, rcopy(u_v.at[s], u_v.at[s], uf_s.at[0], uf_r.at[0], dev(mate, ten)), sent=True)
    settle(primary, u_v, uf_s.at[0])

    @pl.when(both(lower, primary))
    def _():
        um_v[...] = u_v[ten]

    arrived(both(lower, secondary), um_v, um_r.at[0])
    spread_z(2, um_cols, uc_v, me, ten, gate=lower)
    for j in range(n):
        @pl.when(j == me)
        def _():
            uc_v[j, ten] = um_v[:, cols(j, wcol)]

    arrived(secondary, u_v, uf_r.at[0])

    ub = u_v[...].reshape(rows, width)
    dm = jnp.zeros((rows, wo_v.shape[1]), F32)
    for j in range(n):
        dm = dm + mm_nt(ub[:, cols(j, wcol)], wo_v[j])
    dm = dm.astype(BF)

    def query_grad(slope, kn0, kn1, rk_b):
        dqr = jnp.where(low, mm(slope[0], rk_b), mm(slope[1], rk_b))
        dqr = dqr * cosine - half_swap(dqr) * sine
        turned = pltpu.roll(mm(slope[1], kn1), ROPE, 1)
        return jnp.concatenate(
            [
                mm(slope[0], kn0).astype(BF),
                jnp.where(low, dqr, turned).astype(BF),
                jnp.where(low, turned, dqr).astype(BF),
            ],
            axis=1,
        )

    drk = jnp.zeros((rows, 2 * ROPE), F32)
    slopes, pieces = [], []
    for h, (qn, kn, vv, qh, w32, wb) in enumerate(heads):
        dmh = dm[:, cols(h, VDIM)]
        dw = mm_nt(dmh, vv).astype(BF).astype(F32)
        ds = (w32 * (dw - jnp.sum(dw * w32, axis=1, keepdims=True)) * scale).astype(BF)
        drk = drk + mm_tn(ds, qh)
        slopes.append(ds)
        pieces += [mm_tn(ds, qn).astype(BF), mm_tn(wb, dmh).astype(BF)]
    drk = drk * cosine - half_swap(drk) * sine
    drk = drk + pltpu.roll(drk, ROPE, 1)
    so_v[:, cols(0, NOPE)] = (mm(slopes[0], picks[0]) + mm(slopes[1], picks[1])).astype(BF)
    so_v[:, cols(1, VDIM)] = pieces[1]
    so_v[:, cols(2, VDIM)] = pieces[3]
    dc = mm_nt(jnp.concatenate(pieces, axis=1), we)
    dlg = jnp.sum(dc * l32 * rl, axis=0, keepdims=True)
    dcg = dc * lgain
    dl = rl * dcg - l32 * (rl * rl * rl) * jnp.mean(l32 * dcg, axis=1, keepdims=True)
    dlat = jnp.concatenate([dl.astype(BF), drk[:, :ROPE].astype(BF)], axis=1)
    lp_v[...] = dlat.reshape(n_t, share, dlat.shape[1])

    @pl.when(primary)
    def _():
        ls_v[group] = lp_v[ten]

    shared = ((part_v, rs_v), (lp_v, ls_v))

    def share_out(k, gate):
        source, dest = shared[k]
        for s in range(n_t):
            copy = rcopy(source.at[s], dest.at[group], rs_s.at[k], rs_r.at[k], dev(block, s))
            begin(both(jnp.logical_or(s != ten, secondary), gate), copy, sent=True)
        settle(both(primary, gate), dest.at[pl.ds(0, n_t - 1)], rs_s.at[k])
        settle(both(secondary, gate), dest, rs_s.at[k])

    share_out(1, lower)
    dq = query_grad(slopes, heads[0][1], heads[1][1], rk)
    dn = mm_nt(dq, wq) + jnp.concatenate([mm(dlat, wl[d]) for d in range(n)], axis=1)
    part_v[...] = dn.astype(BF).reshape(n_t, share, width)

    @pl.when(primary)
    def _():
        rs_v[group] = part_v[ten]
        sv_v[me] = so_v[...]

    share_out(0, last)
    share_out(1, last)
    spread_block(3, lower, True)
    spread_block(3, lower, False)
    share_out(0, lower)

    def collect_shares(k, gate=True):
        dest = shared[k][1]
        arrived(both(primary, gate), dest.at[pl.ds(0, n_t - 1)], rs_r.at[k])
        arrived(both(secondary, gate), dest, rs_r.at[k])

    def sum_latent(gate):
        collect_shares(1, gate)

        @pl.when(gate)
        def _():
            dl_v[me, ten] = jnp.sum(ls_v[...].astype(F32), axis=0).astype(BF)

        spread_z(3, lambda e: dl_v.at[me, ten], dl_v, me, ten, gate=gate)

    sum_latent(lower)
    relay(2, uc_v, gate=lower)
    hand_on(3, lower)
    relay(3, dl_v, gate=lower)
    lanes = 128
    below = jnp.maximum(sec - 1, 0)

    def finish(gate):
        collect_shares(0, gate)

        @pl.when(gate)
        def _():
            dns = jnp.sum(rs_v[...].astype(F32), axis=0)
            dng = dns * gain
            u_my = um_v[...].astype(F32)
            dx = u_my + r_my * dng - x_my * (r_my * r_my * r_my) * jnp.mean(x_my * dng, axis=1, keepdims=True)
            dx_v[...] = dx.astype(BF)

        for i in range(n_t // 2):
            copy = rcopy(dx_v, u_v.at[ten], p_s.at[i], u_r.at[ten], (below, me, 2 * i + par))
            begin(both(sec > 0, gate), copy)
        copy = rcopy(dx_v, um_v, p_s.at[n_t // 2], um_r.at[0], (below, me, ten))
        begin(both(both(sec > 0, secondary), gate), copy)

        @pl.when(gate)
        def _():
            dgain = jnp.sum(jnp.sum(rs_v[...].astype(F32), axis=0) * x_my * r_my, axis=0, keepdims=True)
            for j in range(n):
                piece = jnp.concatenate([dgain[:, cols(j, wcol)], dlg[:, cols(j, ccol)]], axis=1)
                for i in range(piece.shape[1] // lanes):
                    sg_v[j, i : i + 1] = piece[:, cols(i, lanes)]
            sr_v[me * n_t + ten] = sg_v[me]
            for m in range(micros):
                ig_ref[m] = dx_v[m * chunk : (m + 1) * chunk]

        for j in range(n):
            for t in range(n_t):
                copy = rcopy(sg_v.at[j], sr_v.at[me * n_t + ten], sg_s.at[0], sg_r.at[0], dev(j, t))
                begin(both(jnp.logical_or(j != me, t != ten), gate), copy, sent=True)
        settle(gate, sr_v.at[pl.ds(0, n * n_t - 1)], sg_s.at[0])

    finish(lower)
    finish(last)
    for across in (True, False):
        for k in range(4):
            spread_block(k, last, across)
    sum_latent(last)
    relay(0, nc_v, gate=last)
    relay(1, cc_v, gate=last)
    relay(4, rk_v, gate=last)
    relay(2, uc_v, gate=last)
    for k in range(4):
        hand_on(k, last)
    relay(3, dl_v, gate=last)
    for k in range(4):
        collect_block(k)
    for k, dest in ((0, nc_v), (1, cc_v), (2, uc_v), (4, rk_v)):
        pass_on(k, dest)
    collect(4, rk_v)
    for b in range(n):
        few = sv_v[b, :, :NOPE]
        ds = [jnp.where(same, mm_nt(few, picks[h]), 0.0).astype(BF) for h in range(2)]
        part = lambda i: fw_v[b, i // 2, :, cols(i % 2, NOPE)]
        dq_v[b] = query_grad(ds, part(2), part(3), rk_v[b].reshape(rows, 2 * ROPE))
        for h in range(2):
            de_v[b, :, cols(2 * h, NOPE)] = mm_tn(ds[h], part(h)).astype(BF)
            de_v[b, :, cols(2 * h + 1, NOPE)] = sv_v[b, :, cols(1 + h, VDIM)]
    collect(0, nc_v)
    collect(1, cc_v)
    gq_ref[...] = mm_tn(nc_v[...].reshape(n * rows, wcol), dq_v[...].reshape(n * rows, dq_v.shape[2]))
    ge_ref[...] = mm_tn(cc_v[...].reshape(n * rows, ccol), de_v[...].reshape(n * rows, de_v.shape[2]))
    collect(2, uc_v)
    mixed = fw_v[:, 2].reshape(n * rows, 2 * VDIM)
    go_ref[...] = mm_tn(mixed, uc_v[...].reshape(n * rows, wcol))
    pass_on(3, dl_v)
    collect(3, dl_v)
    gl_ref[...] = mm_tn(dl_v[...].reshape(n * rows, dl_v.shape[3]), nc_v[...].reshape(n * rows, wcol))
    arrived(me >= 0, sr_v.at[pl.ds(0, n * n_t - 1)], sg_r.at[0])
    summed = jnp.sum(sr_v[...], axis=0)
    for i in range(wcol // lanes):
        gg_ref[:, cols(i, lanes)] = summed[i : i + 1]
    for i in range(ccol // lanes):
        glg_ref[:, cols(i, lanes)] = summed[wcol // lanes + i : wcol // lanes + i + 1]
    for cond, copy in drains:
        @pl.when(cond)
        def _(copy=copy):
            copy.wait_send()


def hand_over(*refs):
    for source, dest in zip(refs[:7], refs[7:]):
        dest[...] = source[...]


def section_step(saved, top_grad, gain, w_query, w_latent, compressed_gain, expand_weight, w_output):
    n_pipe, n, n_t = (lax.axis_size(a) for a in ("pipe", "dp", "tensor"))
    micros, seq, width = saved.shape[1:]
    wcol, ccol = gain.shape[1], compressed_gain.shape[1]
    rows, share = micros * seq, micros * seq // n_t
    qcols, lcols = w_query.shape[2], w_latent.shape[2]
    ecols, orows = expand_weight.shape[2], w_output.shape[1]
    order = np.arange(rows)
    place = (order // share) * (seq // n_t) + order % (seq // n_t)
    pair = np.arange(2 * ROPE) % (ROPE // 2)
    angle = place[:, None] * np.exp(-np.log(10000.0) * pair / (ROPE // 2))[None, :]
    sign = np.where(np.arange(2 * ROPE) % ROPE < ROPE // 2, -1.0, 1.0)
    cosine = jnp.asarray(np.cos(angle), F32)
    sine = jnp.asarray(np.sin(angle) * sign, F32)
    vm = pl.BlockSpec(memory_space=pltpu.VMEM)
    shape = jax.ShapeDtypeStruct
    kept = pltpu.VMEM
    sem = lambda *dims: pltpu.SemaphoreType.DMA(dims)
    small = wcol + ccol
    ig, gg, gq, gl, glg, ge, go = pl.pallas_call(
        lambda *refs: section_kernel((n_pipe, n, n_t, micros, seq), *refs),
        name="section_step",
        out_shape=(
            kept((micros, seq // n_t, width), BF),
            kept((1, wcol), F32),
            kept((wcol, qcols), F32),
            kept((lcols, wcol), F32),
            kept((1, ccol), F32),
            kept((ccol, ecols), F32),
            kept((orows, wcol), F32),
        ),
        in_specs=[vm] * 10,
        out_specs=(vm,) * 7,
        scratch_shapes=[
            pltpu.VMEM((rows, width), BF),
            pltpu.VMEM((micros, seq, width), BF),
            pltpu.VMEM((8, small), F32),
            pltpu.VMEM((n, 8, small), F32),
            pltpu.VMEM((share, width), BF),
            pltpu.VMEM((n_t, share, width), BF),
            pltpu.VMEM((share, width), BF),
            pltpu.VMEM((rows, n * ccol), BF),
            pltpu.VMEM((n, wcol, qcols), BF),
            pltpu.VMEM((n, n_t, lcols // n_t, wcol), BF),
            pltpu.VMEM((n, ccol, ecols), BF),
            pltpu.VMEM((n, orows, wcol), BF),
            pltpu.VMEM((n, n_t, share, wcol), BF),
            pltpu.VMEM((n, n_t, share, ccol), BF),
            pltpu.VMEM((n, n_t, share, wcol), BF),
            pltpu.VMEM((n, n_t, share, lcols), BF),
            pltpu.VMEM((n, n_t, share, 2 * ROPE), BF),
            pltpu.VMEM((rows, 2 * ROPE), BF),
            pltpu.VMEM((3, rows, orows), BF),
            pltpu.VMEM((n, 3, rows, orows), BF),
            pltpu.VMEM((rows, NOPE + orows), BF),
            pltpu.VMEM((n, rows, NOPE + orows), BF),
            pltpu.VMEM((n_t, share, width), BF),
            pltpu.VMEM((n_t, share, width), BF),
            pltpu.VMEM((n_t, share, lcols), BF),
            pltpu.VMEM((n_t, share, lcols), BF),
            pltpu.VMEM((share, width), BF),
            pltpu.VMEM((n, 8 * -(-small // 1024), 128), F32),
            pltpu.VMEM((n * n_t, 8 * -(-small // 1024), 128), F32),
            pltpu.VMEM((n, rows, qcols), BF),
            pltpu.VMEM((n, rows, ecols), BF),
            sem(1), sem(1), sem(1), sem(1), sem(1), sem(n), sem(1), sem(1), sem(1),
            sem(3), sem(3, n), sem(3), sem(3), sem(5), sem(5), sem(n), sem(5), sem(5), sem(5),
            sem(4), sem(4, n), sem(4), sem(2), sem(2), sem(n_t // 2 + 1), sem(n_t), sem(1), sem(1), sem(1),
            sem(1), sem(1),
        ],
        compiler_params=pltpu.CompilerParams(
            collective_id=0, has_side_effects=True, vmem_limit_bytes=60 * 1024 * 1024
        ),
    )(
        saved[0], top_grad, gain, compressed_gain, w_query[0], w_latent[0].T,
        expand_weight[0], w_output[0], cosine, sine,
    )
    parts = [pltpu.with_memory_space_constraint(p, pltpu.VMEM) for p in (ig, gg, gq, gl, glg, ge, go)]
    ig, gg, gq, gl, glg, ge, go = pl.pallas_call(
        hand_over,
        name="hand_over",
        out_shape=tuple(shape(p.shape, p.dtype) for p in parts),
        in_specs=[vm] * 7,
        out_specs=(vm,) * 7,
    )(*parts)
    return ig[None], gg, gq[None], gl.T[None], glg, ge[None], go[None]


def choose(saved, top_grad, gain, w_query, w_latent, compressed_gain, expand_weight, w_output):
    arrays = (saved, top_grad, gain, w_query, w_latent, compressed_gain, expand_weight, w_output)
    n, n_t = lax.axis_size("dp"), lax.axis_size("tensor")
    fits = (
        n == 4
        and n_t == 4
        and saved.shape[1] == 2
        and saved.shape[2] == ROPE
        and w_query.shape[2] == 2 * (NOPE + ROPE)
        and w_output.shape[1] == 2 * VDIM
        and gain.shape[1] % 128 == 0
        and compressed_gain.shape[1] % 128 == 0
        and n * compressed_gain.shape[1] + ROPE == w_latent.shape[2]
        and w_latent.shape[2] % (16 * n_t) == 0
    )
    return section_step(*arrays) if fits else shards(*arrays)


def solution(mesh):
    in_specs = (
        P("pipe", None, "dp", None),
        P(None, "dp", None),
        P("pipe", "dp"),
        P("pipe", "dp", "tensor"),
        P("pipe", "dp", None),
        P("pipe", "dp"),
        P("pipe", "dp", "tensor"),
        P("pipe", "tensor", "dp"),
    )
    out_specs = (
        P("pipe", None, ("dp", "tensor"), None),
        P("pipe", "dp"),
        P("pipe", "dp", "tensor"),
        P("pipe", "dp", None),
        P("pipe", "dp"),
        P("pipe", "dp", "tensor"),
        P("pipe", "tensor", "dp"),
    )
    return jax.shard_map(choose, mesh=mesh, in_specs=in_specs, out_specs=out_specs, check_vma=False)
```

```python
import jax
import jax.numpy as jnp
from jax import lax
import numpy as np
from jax.experimental import pallas as pl
from jax.experimental.pallas import tpu as pltpu
from jax.sharding import PartitionSpec as P

NOPE = 128
ROPE = 64
VDIM = 128
COMPRESSED_RANK = 512


EPS = 1e-06


def passed_along(value, axis, steps):
    count = lax.axis_size(axis)
    first, last = (max(0, -steps), min(count, count - steps))
    return lax.ppermute(value, axis, [(source, source + steps) for source in range(first, last)])


def root_mean_scale(values, scale):
    return values * lax.rsqrt(jnp.mean(values * values, axis=-1, keepdims=True) + EPS) * scale


def rotary_angles(values):
    length = values.shape[0]
    half = values.shape[-1] // 2
    freq = jnp.exp(-jnp.log(10000.0) * jnp.arange(half, dtype=jnp.float32) / half)
    angle = jnp.arange(length, dtype=jnp.float32)[:, None] * freq[None, :]
    cosine = jnp.cos(angle)[:, None, :]
    sine = jnp.sin(angle)[:, None, :]
    first = values[..., :half]
    second = values[..., half:]
    return jnp.concatenate(
        [first * cosine - second * sine, second * cosine + first * sine], axis=-1
    )


def branch(normed, w_q, w_lat, latent_norm_gain, w_exp, w_out):
    length = normed.shape[0]
    heads = w_q.shape[1] // (NOPE + ROPE)
    rounded = normed.astype(jnp.bfloat16)
    query = jnp.dot(rounded, w_q, preferred_element_type=jnp.float32).reshape(
        length, heads, NOPE + ROPE
    )
    latent_state = jnp.dot(rounded, w_lat, preferred_element_type=jnp.float32)
    compressed_state = root_mean_scale(latent_state[:, :COMPRESSED_RANK], latent_norm_gain).astype(
        jnp.bfloat16
    )
    rotary_key_part = rotary_angles(latent_state[:, None, COMPRESSED_RANK:])[:, 0, :]
    expanded = jnp.dot(compressed_state, w_exp, preferred_element_type=jnp.float32).reshape(
        length, heads, NOPE + VDIM
    )
    key_nope = expanded[:, :, :NOPE]
    values = expanded[:, :, NOPE:].astype(jnp.bfloat16)
    query_rope = rotary_angles(query[:, :, NOPE:])
    scores = jnp.einsum("qhd,khd->hqk", query[:, :, :NOPE], key_nope) + jnp.einsum(
        "qhd,kd->hqk", query_rope, rotary_key_part
    )
    scores = scores * (NOPE + ROPE) ** (-0.5)
    causal = jnp.arange(length)[:, None] >= jnp.arange(length)[None, :]
    scores = jnp.where(causal[None], scores, -1e30)
    weights = jax.nn.softmax(scores, axis=-1).astype(jnp.bfloat16)
    mixed = jnp.einsum("hqk,khd->qhd", weights.astype(jnp.float32), values.astype(jnp.float32))
    mixed = mixed.astype(jnp.bfloat16).reshape(length, heads * VDIM)
    return jnp.dot(mixed, w_out, preferred_element_type=jnp.float32)


def shards(saved, top_grad, gain, w_query, w_latent, compressed_gain, expand_weight, w_output):
    gathered = (
        lax.all_gather(gain, "dp", axis=1, tiled=True),
        lax.all_gather(w_query, "dp", axis=1, tiled=True),
        lax.all_gather(w_latent, "dp", axis=1, tiled=True),
        lax.all_gather(compressed_gain, "dp", axis=1, tiled=True),
        lax.all_gather(expand_weight, "dp", axis=1, tiled=True),
        lax.all_gather(w_output, "dp", axis=2, tiled=True),
    )
    gain32 = gathered[0][0].astype(jnp.float32)
    query_all = gathered[1][0]
    latent_all = gathered[2][0]
    lgain32 = gathered[3][0].astype(jnp.float32)
    expand_all = gathered[4][0]
    output_all = gathered[5][0]
    sections = lax.axis_size("pipe")
    section_index = lax.axis_index("pipe")
    tensor_count = lax.axis_size("tensor")
    tensor_rank = lax.axis_index("tensor")
    micro_count = saved.shape[1]
    length = saved.shape[2]
    width = saved.shape[3]
    share = length // tensor_count

    def compute(normed, upstream):
        unused, pull = jax.vjp(
            lambda value: branch(value, query_all, latent_all, lgain32, expand_all, output_all),
            normed,
        )
        return pull(upstream.astype(jnp.float32))[0]

    def skip(normed, upstream):
        return jnp.zeros_like(normed)

    gain_total = jnp.zeros((width,), jnp.float32)
    results = jnp.zeros((micro_count, share, width), jnp.bfloat16)
    stored = jnp.zeros((micro_count, length, width), jnp.bfloat16)
    received = jnp.zeros((length, width), jnp.bfloat16)
    for tick in range(sections + micro_count - 1):
        micro = tick - (sections - 1 - section_index)
        active = jnp.logical_and(micro >= 0, micro < micro_count)
        picked = jnp.clip(micro, 0, micro_count - 1)
        x_rows = lax.dynamic_index_in_dim(saved[0], picked, 0, keepdims=False)
        top_rows = lax.dynamic_index_in_dim(top_grad, picked, 0, keepdims=False)
        arrived = received
        upstream = jnp.where(section_index == sections - 1, top_rows, arrived)
        x_float = x_rows.astype(jnp.float32)
        normed, norm_pull = jax.vjp(root_mean_scale, x_float, gain32)
        branch_grad = lax.cond(active, compute, skip, normed, upstream)
        d_normed = lax.psum(branch_grad.astype(jnp.bfloat16), "tensor").astype(jnp.float32)
        dx_norm, d_gain = norm_pull(d_normed)
        dx = (upstream.astype(jnp.float32) + dx_norm).astype(jnp.bfloat16)
        gain_total = gain_total + jnp.where(active, d_gain, 0.0)
        mine = lax.dynamic_slice_in_dim(dx, tensor_rank * share, share, 0)
        chosen = (jnp.arange(micro_count) == micro)[:, None, None]
        results = jnp.where(chosen, mine[None], results)
        stored = jnp.where(chosen, upstream[None], stored)
        received = passed_along(dx, "pipe", -1)
    totals = (
        jnp.zeros(query_all.shape, jnp.float32),
        jnp.zeros(latent_all.shape, jnp.float32),
        jnp.zeros(lgain32.shape, jnp.float32),
        jnp.zeros(expand_all.shape, jnp.float32),
        jnp.zeros(output_all.shape, jnp.float32),
    )
    for micro_index in range(micro_count):
        normed_again = root_mean_scale(saved[0, micro_index].astype(jnp.float32), gain32)
        unused, weight_pull = jax.vjp(
            lambda w_q, w_lat, lat_gain, w_exp, w_out: branch(
                normed_again, w_q, w_lat, lat_gain, w_exp, w_out
            ),
            query_all,
            latent_all,
            lgain32,
            expand_all,
            output_all,
        )
        cotangents = weight_pull(stored[micro_index].astype(jnp.float32))
        totals = tuple(
            (total + piece.astype(jnp.float32) for total, piece in zip(totals, cotangents))
        )
    gain_part = jnp.where(tensor_rank == 0, gain_total, 0.0)
    grad_q, grad_lat, grad_lg, grad_e, grad_o = totals
    out_q, part_lat, part_lg, out_e, out_o, part_gain = (
        lax.psum_scatter(grad_q.astype(jnp.bfloat16), "dp", scatter_dimension=0, tiled=True).astype(
            jnp.float32
        ),
        lax.psum_scatter(
            grad_lat.astype(jnp.bfloat16), "dp", scatter_dimension=0, tiled=True
        ).astype(jnp.float32),
        lax.psum_scatter(
            grad_lg.astype(jnp.bfloat16), "dp", scatter_dimension=0, tiled=True
        ).astype(jnp.float32),
        lax.psum_scatter(grad_e.astype(jnp.bfloat16), "dp", scatter_dimension=0, tiled=True).astype(
            jnp.float32
        ),
        lax.psum_scatter(grad_o.astype(jnp.bfloat16), "dp", scatter_dimension=1, tiled=True).astype(
            jnp.float32
        ),
        lax.psum_scatter(
            gain_part.astype(jnp.bfloat16), "dp", scatter_dimension=0, tiled=True
        ).astype(jnp.float32),
    )
    out_lat, out_lg, out_gain = (
        lax.psum(part_lat.astype(jnp.bfloat16), "tensor").astype(jnp.float32),
        lax.psum(part_lg.astype(jnp.bfloat16), "tensor").astype(jnp.float32),
        lax.psum(part_gain.astype(jnp.bfloat16), "tensor").astype(jnp.float32),
    )
    return (
        results[None],
        out_gain[None],
        out_q[None],
        out_lat[None],
        out_lg[None],
        out_e[None],
        out_o[None],
    )


MESH = pl.DeviceIdType.MESH
BF = jnp.bfloat16
F32 = jnp.float32


def mm(a, b):
    return lax.dot_general(a, b, (((1,), (0,)), ((), ())), preferred_element_type=F32)


def mm_nt(a, b):
    return lax.dot_general(a, b, (((1,), (1,)), ((), ())), preferred_element_type=F32)


def mm_tn(a, b):
    return lax.dot_general(a, b, (((0,), (0,)), ((), ())), preferred_element_type=F32)


def half_swap(v):
    lane = lax.broadcasted_iota(jnp.int32, v.shape, 1)
    ahead = pltpu.roll(v, v.shape[1] - ROPE // 2, 1)
    behind = pltpu.roll(v, ROPE // 2, 1)
    return jnp.where(lax.rem(lane, ROPE) < ROPE // 2, ahead, behind)


def section_kernel(
    dims,
    saved_in, top_in, gain_in, lgain_in, wq_in, wl_in, we_in, wo_in, cos_in, sin_in,
    ig_ref, gg_ref, gq_ref, gl_ref, glg_ref, ge_ref, go_ref,
    saved_ref, top_ref, gain_ref, lgain_ref, wq_ref, wl_ref, we_ref, wo_ref, cos_ref, sin_ref,
    x_v, xs_v, own_v, sm_v, nm_v, u_v, um_v, cb_v, wq_v, wl_v, we_v, wo_v,
    nc_v, cc_v, uc_v, dl_v, rk_v, ro_v, fo_v, fw_v, so_v, sv_v, part_v, rs_v, lp_v, ls_v, dx_v, sg_v, sr_v,
    dq_v, de_v,
    dp_s, dp_r, x_s, x_r, wz_s, wz_r, wh_s, wt_s, wt_r, w_s, w_r, f_s, f_r, z_s, z_r, zl_r, t_s, ta_r, tb_r,
    b_s, b_r, bh_s, rs_s, rs_r, p_s, u_r, um_r, uf_s, uf_r, sg_s, sg_r, in_s,
):
    n_pipe, n, n_t, micros, seq = dims
    sec, me, ten = lax.axis_index("pipe"), lax.axis_index("dp"), lax.axis_index("tensor")
    rows = micros * seq
    chunk = seq // n_t
    share = micros * chunk
    width = x_v.shape[1]
    wcol, ccol = wq_v.shape[1], we_v.shape[1]
    rank = n * ccol
    quarter = wl_v.shape[2]
    core = lax.rem(ten, 2)
    partner = ten + 1 - 2 * core
    opposite = lax.rem(ten + 2, n_t)
    par = lax.rem(me, 2)
    mate = me + 1 - 2 * par
    group = ten - core + par
    block = me - par + core
    primary = core == par
    secondary = jnp.logical_not(primary)
    half = me // 2
    near = 2 - half
    middle = jnp.logical_or(me == 1, me == 2)
    last = sec == n_pipe - 1
    lower = jnp.logical_not(last)
    both = jnp.logical_and
    drains = []

    def rcopy(a, b, ss, rs, dev):
        return pltpu.make_async_remote_copy(
            src_ref=a, dst_ref=b, send_sem=ss, recv_sem=rs, device_id=dev, device_id_type=MESH
        )

    def begin(cond, copy, sent=False):
        @pl.when(cond)
        def _():
            copy.start()

        if not sent:
            drains.append((cond, copy))

    def settle(cond, ref, ss):
        drains.append((cond, rcopy(ref, ref, ss, x_r.at[0], dev(me, partner))))

    def arrived(cond, ref, rs):
        @pl.when(cond)
        def _():
            rcopy(ref, ref, x_s.at[0], rs, dev(me, partner)).wait_recv()

    def dev(d, t):
        return (sec, d, t)

    def cols(j, size):
        return slice(j * size, (j + 1) * size)

    def mine(ref):
        at = pl.ds(pl.multiple_of(ten * chunk, chunk), chunk)
        return jnp.concatenate([ref[m, at] for m in range(micros)], axis=0)

    def by_share(store, ref):
        for j in range(n_t):
            for m in range(micros):
                store(j, m, ref[m, j * chunk : (j + 1) * chunk])

    def x_store(j, m, value):
        x_v[j * share + m * chunk : j * share + (m + 1) * chunk] = value

    def u_store(j, m, value):
        u_v[j, m * chunk : (m + 1) * chunk] = value

    inputs = (saved_in, top_in, gain_in, lgain_in, wq_in, wl_in, we_in, wo_in, cos_in, sin_in)
    places = (saved_ref, top_ref, gain_ref, lgain_ref, wq_ref, wl_ref, we_ref, wo_ref, cos_ref, sin_ref)
    fetches = [pltpu.make_async_copy(a, b, in_s.at[i]) for i, (a, b) in enumerate(zip(inputs, places))]
    for copy in fetches:
        copy.start()

    barrier = pltpu.get_barrier_semaphore()
    for j in range(n_t):
        for d in range(n):
            @pl.when(jnp.logical_or(d != me, j != ten))
            def _():
                pl.semaphore_signal(barrier, inc=1, device_id=dev(d, j), device_id_type=MESH)

        @pl.when(sec > 0)
        def _():
            pl.semaphore_signal(barrier, inc=1, device_id=(sec - 1, me, j), device_id_type=MESH)

        @pl.when(lower)
        def _():
            pl.semaphore_signal(barrier, inc=1, device_id=(sec + 1, me, j), device_id_type=MESH)

    for copy in fetches:
        copy.wait()

    own_v[:, :wcol] = jnp.broadcast_to(gain_ref[...].astype(F32), (8, wcol))
    own_v[:, wcol:] = jnp.broadcast_to(lgain_ref[...].astype(F32), (8, ccol))

    @pl.when(last)
    def _():
        um_v[...] = mine(top_ref)

    @pl.when(both(last, primary))
    def _():
        by_share(u_store, top_ref)

    neighbours = jnp.minimum(sec, 1) + jnp.minimum(n_pipe - 1 - sec, 1)
    pl.semaphore_wait(barrier, n * n_t - 1 + neighbours * n_t)

    def spread_dp(k, source, dest):
        for j in range(n):
            begin(j != me, rcopy(source(j), dest.at[me], dp_s.at[k], dp_r.at[k], dev(j, ten)), sent=True)
        settle(me >= 0, dest.at[pl.ds(0, n - 1)], dp_s.at[k])

    def collect_dp(k, dest):
        arrived(me >= 0, dest.at[pl.ds(0, n - 1)], dp_r.at[k])

    def spread_z(k, source, dest, slot, rank_to, gate=None):
        for e in range(n):
            cond = jnp.logical_or(e != me, rank_to != ten)
            if gate is not None:
                cond = both(cond, gate)
            rs = zl_r.at[slot] if k == 3 else z_r.at[k]
            begin(cond, rcopy(source(e), dest.at[slot, rank_to], z_s.at[k], rs, dev(e, rank_to)), sent=True)
        on = me >= 0 if gate is None else gate
        if k in (1, 4):
            settle(both(on, primary), dest.at[0, pl.ds(0, n - 1)], z_s.at[k])
            settle(both(on, secondary), dest.at[0, pl.ds(0, n)], z_s.at[k])
        else:
            settle(on, dest.at[0, pl.ds(0, n - 1)], z_s.at[k])

    def relay(k, dest, gate):
        def share_slot(b):
            for to, rs in ((opposite, ta_r), (partner, tb_r)):
                copy = rcopy(dest.at[b, ten], dest.at[b, ten], t_s.at[k], rs.at[k], dev(me, to))
                begin(gate, copy, sent=True)

        if k == 3:
            for b in range(n):
                arrived(both(b != me, gate), dest.at[b, ten], zl_r.at[b])
                share_slot(b)
        else:
            few, every = dest.at[pl.ds(0, n - 1), ten], dest.at[pl.ds(0, n), ten]
            if k in (1, 4):
                arrived(both(gate, primary), few, z_r.at[k])
                arrived(both(gate, secondary), every, z_r.at[k])
            else:
                arrived(gate, few, z_r.at[k])
            for b in range(n):
                share_slot(b)

    def pass_on(k, dest, gate=True):
        gate = both(me >= 0, gate)
        arrived(gate, dest.at[pl.ds(0, n), opposite], ta_r.at[k])
        for b in range(n):
            at = dest.at[b, opposite]
            begin(gate, rcopy(at, at, t_s.at[k], tb_r.at[k], dev(me, partner)), sent=True)
        settle(gate, dest.at[pl.ds(0, n - 1)], t_s.at[k])

    def collect(k, dest):
        arrived(me >= 0, dest.at[pl.ds(0, 2)], tb_r.at[k])

    def landing(k, b):
        return sv_v.at[b] if k == 3 else fw_v.at[b, k]

    def spread_block(k, gate, across):
        source = so_v if k == 3 else fo_v.at[k]
        for e in range(n):
            wanted = near == e if across else both(half == e // 2, jnp.logical_or(e != me, secondary))
            copy = rcopy(source, landing(k, block), b_s.at[k], b_r.at[k, block], dev(e, group))
            begin(both(wanted, gate), copy, sent=True)
        if across:
            several = lambda c: sv_v.at[pl.ds(0, c)] if k == 3 else fw_v.at[pl.ds(0, c), k]
            settle(both(gate, primary), several(2), b_s.at[k])
            settle(both(gate, secondary), several(3), b_s.at[k])

    def hand_on(k, gate):
        for b in range(n):
            cond = both(both(middle, half != b // 2), gate)
            at = landing(k, b)
            arrived(cond, at, b_r.at[k, b])
            begin(cond, rcopy(at, at, bh_s.at[k], b_r.at[k, b], dev(mate, ten)), sent=True)
        two = sv_v.at[pl.ds(0, 2)] if k == 3 else fw_v.at[pl.ds(0, 2), k]
        settle(both(middle, gate), two, bh_s.at[k])

    def collect_block(k):
        for b in range(n):
            handed = both(middle, half != b // 2)
            cond = both(jnp.logical_or(b != me, secondary), jnp.logical_not(handed))
            arrived(cond, landing(k, b), b_r.at[k, b])

    spread_dp(0, lambda j: own_v, sm_v)
    sm_v[me] = own_v[...]
    my_quarter = wl_ref.at[pl.ds(pl.multiple_of(ten * quarter, quarter), quarter)]
    for level in (near, mate):
        begin(me >= 0, rcopy(my_quarter, wl_v.at[me, ten], wz_s.at[0], wz_r.at[me], dev(level, ten)), sent=True)
    settle(me >= 0, wl_v.at[0, pl.ds(0, 2)], wz_s.at[0])
    weights = ((wq_ref, wq_v), (we_ref, we_v), (wo_ref, wo_v))

    begin(primary, rcopy(saved_ref, xs_v, x_s.at[0], x_r.at[0], dev(mate, ten)))

    def give(k, gate=True):
        ref, store = weights[k]
        for i in range(n // 2):
            level = 2 * i + core
            copy = rcopy(ref, store.at[me], w_s.at[k], w_r.at[k, me], dev(level, ten))
            begin(both(level != me, gate), copy, sent=True)
        settle(both(primary, gate), store.at[pl.ds(0, n // 2 - 1)], w_s.at[k])
        settle(both(secondary, gate), store.at[pl.ds(0, n // 2)], w_s.at[k])
        copy = rcopy(ref, store.at[me], f_s.at[k], f_r.at[k], dev(me, partner))
        begin(both(primary, gate), copy, sent=True)

    def give_rest(gate):
        give(1, gate)
        for s in range(n_t):
            copy = rcopy(u_v.at[s], u_v.at[s], uf_s.at[0], uf_r.at[0], dev(mate, ten))
            begin(both(both(last, primary), gate), copy, sent=True)
        give(2, gate)
        spread_z(2, um_cols, uc_v, me, ten, gate=both(last, gate))

    um_cols = lambda e: um_v.at[:, pl.ds(e * wcol, wcol)]
    give(0)
    give_rest(jnp.logical_not(middle))

    for j in range(n_t):
        wl_v[me, j] = wl_ref[j * quarter : (j + 1) * quarter]

    @pl.when(primary)
    def _():
        for ref, store in weights:
            store[me] = ref[...]

        by_share(x_store, saved_ref)

    def to_ten(b, valid):
        for j in range(n_t):
            begin(
                both(valid, j != ten),
                rcopy(wl_v.at[b, ten], wl_v.at[b, ten], wt_s.at[0], wt_r.at[0], dev(me, j)),
                sent=True,
            )

    for b in range(n):
        arrived(b != me, wl_v.at[b, ten], wz_r.at[b])
        begin(
            both(middle, half != b // 2),
            rcopy(wl_v.at[b, ten], wl_v.at[b, ten], wh_s.at[0], wz_r.at[b], dev(mate, ten)),
            sent=True,
        )
        to_ten(b, b != me)
    settle(middle, wl_v.at[0, pl.ds(0, 2)], wh_s.at[0])
    wl_peers = wl_v.at[pl.ds(0, n - 1), pl.ds(0, n_t - 1)]
    settle(me >= 0, wl_peers, wt_s.at[0])
    give_rest(middle)

    collect_dp(0, sm_v)
    gain = jnp.concatenate([sm_v[d][0:1, :wcol] for d in range(n)], axis=1)
    lgain = jnp.concatenate([sm_v[d][0:1, wcol : wcol + ccol] for d in range(n)], axis=1)
    x_my = mine(saved_ref).astype(F32)
    r_my = lax.rsqrt(jnp.mean(x_my * x_my, axis=1, keepdims=True) + EPS)
    nm_v[...] = (x_my * r_my * gain).astype(BF)
    spread_z(0, lambda e: nm_v.at[:, pl.ds(e * wcol, wcol)], nc_v, me, ten)
    for j in range(n):
        @pl.when(j == me)
        def _():
            nc_v[j, ten] = nm_v[:, cols(j, wcol)]

    @pl.when(secondary)
    def _():
        rcopy(xs_v, xs_v, x_s.at[0], x_r.at[0], dev(me, partner)).wait_recv()
        by_share(x_store, xs_v)

    x32 = x_v[...].astype(F32)
    r = lax.rsqrt(jnp.mean(x32 * x32, axis=1, keepdims=True) + EPS)
    nb = (x32 * r * gain).astype(BF)

    def take(k):
        store = weights[k][1]
        for d in range(n):
            cond = both(primary, d != me)
            arrived(cond, store.at[d], w_r.at[k, d])
            begin(cond, rcopy(store.at[d], store.at[d], f_s.at[k], f_r.at[k], dev(me, partner)), sent=True)
        settle(primary, store, f_s.at[k])
        arrived(secondary, store, f_r.at[k])

    take(0)
    arrived(me >= 0, wl_peers, wt_r.at[0])

    wq = wq_v[...].reshape(width, wq_v.shape[2])
    wl = [wl_v[d].reshape(n_t * quarter, wcol) for d in range(n)]
    q = mm(nb, wq)
    lat = jnp.zeros((rows, n_t * quarter), F32)
    for d in range(n):
        lat = lat + mm_nt(nb[:, cols(d, wcol)], wl[d])
    l32 = lat[:, :rank]
    rl = lax.rsqrt(jnp.mean(l32 * l32, axis=1, keepdims=True) + EPS)
    cb = (l32 * rl * lgain).astype(BF)
    cb_v[...] = cb
    my_rows = pl.ds(pl.multiple_of(group * share, share), share)
    spread_z(1, lambda e: cb_v.at[my_rows, pl.ds(e * ccol, ccol)], cc_v, block, group)
    for j in range(n):
        @pl.when(both(j == me, primary))
        def _():
            cc_v[j, ten] = cb_v[my_rows, cols(j, ccol)]

    cosine, sine = cos_ref[...], sin_ref[...]
    lr = lat[:, rank:]
    lr2 = jnp.concatenate([lr, lr], axis=1)
    rk = (lr2 * cosine + half_swap(lr2) * sine).astype(BF)
    ro_v[...] = rk
    spread_z(4, lambda e: ro_v.at[my_rows], rk_v, block, group)

    @pl.when(primary)
    def _():
        rk_v[me, ten] = ro_v[my_rows]

    lane = lax.broadcasted_iota(jnp.int32, (rows, 2 * ROPE), 1)
    low = lane < ROPE
    q1, q2 = q[:, NOPE : 2 * NOPE], q[:, 2 * NOPE :]
    nope = (q[:, :NOPE], pltpu.roll(jnp.where(low, q2, q1), ROPE, 1))
    for h in range(2):
        fo_v[0, :, cols(h, NOPE)] = nope[h].astype(BF)
    spread_block(0, lower, True)
    spread_block(0, lower, False)
    qr_all = jnp.where(low, q1, q2)
    qr = qr_all * cosine + half_swap(qr_all) * sine
    row = lax.broadcasted_iota(jnp.int32, (rows, rows), 0)
    col = lax.broadcasted_iota(jnp.int32, (rows, rows), 1)

    def place(i):
        return (i // share) * chunk + lax.rem(i, chunk)

    same = lax.rem(row, share) // chunk == lax.rem(col, share) // chunk
    keep = jnp.logical_and(same, place(row) >= place(col))
    picks = [jnp.where(place(row) + h * seq == col, 1.0, 0.0).astype(BF) for h in range(2)]
    scale = (NOPE + ROPE) ** (-0.5)
    masks = (low, jnp.logical_not(low))
    take(1)
    we = we_v[...].reshape(n * ccol, we_v.shape[2])
    ex = mm(cb, we)
    for h in range(2):
        fo_v[1, :, cols(h, NOPE)] = ex[:, cols(2 * h, NOPE)].astype(BF)
    spread_block(1, lower, True)
    spread_block(1, lower, False)
    heads = []
    for h in range(2):
        qn = nope[h].astype(BF)
        kn = ex[:, h * (NOPE + VDIM) : h * (NOPE + VDIM) + NOPE].astype(BF)
        vv = ex[:, h * (NOPE + VDIM) + NOPE : (h + 1) * (NOPE + VDIM)].astype(BF)
        qh = jnp.where(masks[h], qr, 0.0).astype(BF)
        scores = (mm_nt(qn, kn) + mm_nt(qh, rk)) * scale
        scores = jnp.where(keep, scores, -1e30)
        e = jnp.exp(scores - jnp.max(scores, axis=1, keepdims=True))
        w32 = e / jnp.sum(e, axis=1, keepdims=True)
        wb = w32.astype(BF)
        fo_v[2, :, cols(h, VDIM)] = mm(wb, vv).astype(BF)
        heads.append((qn, kn, vv, qh, w32, wb))

    @pl.when(primary)
    def _():
        fw_v[me] = fo_v[...]

    spread_block(2, lower, True)
    spread_block(2, lower, False)
    take(2)
    relay(0, nc_v, gate=lower)
    relay(1, cc_v, gate=lower)
    relay(4, rk_v, gate=lower)
    for k in range(3):
        hand_on(k, lower)

    for s in range(n_t):
        cond = both(lower, primary)
        arrived(cond, u_v.at[s], u_r.at[s])
        begin(cond, rcopy(u_v.at[s], u_v.at[s], uf_s.at[0], uf_r.at[0], dev(mate, ten)), sent=True)
    settle(primary, u_v, uf_s.at[0])

    @pl.when(both(lower, primary))
    def _():
        um_v[...] = u_v[ten]

    arrived(both(lower, secondary), um_v, um_r.at[0])
    spread_z(2, um_cols, uc_v, me, ten, gate=lower)
    for j in range(n):
        @pl.when(j == me)
        def _():
            uc_v[j, ten] = um_v[:, cols(j, wcol)]

    arrived(secondary, u_v, uf_r.at[0])

    ub = u_v[...].reshape(rows, width)
    dm = jnp.zeros((rows, wo_v.shape[1]), F32)
    for j in range(n):
        dm = dm + mm_nt(ub[:, cols(j, wcol)], wo_v[j])
    dm = dm.astype(BF)

    def query_grad(slope, kn0, kn1, rk_b):
        dqr = jnp.where(low, mm(slope[0], rk_b), mm(slope[1], rk_b))
        dqr = dqr * cosine - half_swap(dqr) * sine
        turned = pltpu.roll(mm(slope[1], kn1), ROPE, 1)
        return jnp.concatenate(
            [
                mm(slope[0], kn0).astype(BF),
                jnp.where(low, dqr, turned).astype(BF),
                jnp.where(low, turned, dqr).astype(BF),
            ],
            axis=1,
        )

    drk = jnp.zeros((rows, 2 * ROPE), F32)
    slopes, pieces = [], []
    for h, (qn, kn, vv, qh, w32, wb) in enumerate(heads):
        dmh = dm[:, cols(h, VDIM)]
        dw = mm_nt(dmh, vv).astype(BF).astype(F32)
        ds = (w32 * (dw - jnp.sum(dw * w32, axis=1, keepdims=True)) * scale).astype(BF)
        drk = drk + mm_tn(ds, qh)
        slopes.append(ds)
        pieces += [mm_tn(ds, qn).astype(BF), mm_tn(wb, dmh).astype(BF)]
    drk = drk * cosine - half_swap(drk) * sine
    drk = drk + pltpu.roll(drk, ROPE, 1)
    so_v[:, cols(0, NOPE)] = (mm(slopes[0], picks[0]) + mm(slopes[1], picks[1])).astype(BF)
    so_v[:, cols(1, VDIM)] = pieces[1]
    so_v[:, cols(2, VDIM)] = pieces[3]
    dc = mm_nt(jnp.concatenate(pieces, axis=1), we)
    dlg = jnp.sum(dc * l32 * rl, axis=0, keepdims=True)
    dcg = dc * lgain
    dl = rl * dcg - l32 * (rl * rl * rl) * jnp.mean(l32 * dcg, axis=1, keepdims=True)
    dlat = jnp.concatenate([dl.astype(BF), drk[:, :ROPE].astype(BF)], axis=1)
    lp_v[...] = dlat.reshape(n_t, share, dlat.shape[1])

    @pl.when(primary)
    def _():
        ls_v[group] = lp_v[ten]

    shared = ((part_v, rs_v), (lp_v, ls_v))

    def share_out(k, gate):
        source, dest = shared[k]
        for i in range(n_t):
            s = lax.rem(ten - core + 2 + i, n_t)
            copy = rcopy(source.at[s], dest.at[group], rs_s.at[k], rs_r.at[k], dev(block, s))
            begin(both(jnp.logical_or(s != ten, secondary), gate), copy, sent=True)
        settle(both(primary, gate), dest.at[pl.ds(0, n_t - 1)], rs_s.at[k])
        settle(both(secondary, gate), dest, rs_s.at[k])

    share_out(1, lower)
    dq = query_grad(slopes, heads[0][1], heads[1][1], rk)
    dn = mm_nt(dq, wq) + jnp.concatenate([mm(dlat, wl[d]) for d in range(n)], axis=1)
    part_v[...] = dn.astype(BF).reshape(n_t, share, width)

    @pl.when(primary)
    def _():
        rs_v[group] = part_v[ten]
        sv_v[me] = so_v[...]

    share_out(0, last)
    share_out(1, last)
    spread_block(3, lower, False)
    spread_block(3, lower, True)
    share_out(0, lower)

    def collect_shares(k, gate=True):
        dest = shared[k][1]
        arrived(both(primary, gate), dest.at[pl.ds(0, n_t - 1)], rs_r.at[k])
        arrived(both(secondary, gate), dest, rs_r.at[k])

    def sum_latent(gate):
        collect_shares(1, gate)

        @pl.when(gate)
        def _():
            dl_v[me, ten] = jnp.sum(ls_v[...].astype(F32), axis=0).astype(BF)

        spread_z(3, lambda e: dl_v.at[me, ten], dl_v, me, ten, gate=gate)

    for k, dest in ((0, nc_v), (1, cc_v), (4, rk_v)):
        pass_on(k, dest, lower)
    sum_latent(lower)
    relay(2, uc_v, gate=lower)
    hand_on(3, lower)
    relay(3, dl_v, gate=lower)
    lanes = 128
    below = jnp.maximum(sec - 1, 0)

    def finish(gate):
        collect_shares(0, gate)

        @pl.when(gate)
        def _():
            dns = jnp.sum(rs_v[...].astype(F32), axis=0)
            dng = dns * gain
            u_my = um_v[...].astype(F32)
            dx = u_my + r_my * dng - x_my * (r_my * r_my * r_my) * jnp.mean(x_my * dng, axis=1, keepdims=True)
            dx_v[...] = dx.astype(BF)

        for i in range(n_t // 2):
            to = lax.rem(ten - core + 2 + 2 * i, n_t) + par
            copy = rcopy(dx_v, u_v.at[ten], p_s.at[i], u_r.at[ten], (below, me, to))
            begin(both(sec > 0, gate), copy)
        copy = rcopy(dx_v, um_v, p_s.at[n_t // 2], um_r.at[0], (below, me, ten))
        begin(both(both(sec > 0, secondary), gate), copy)

        @pl.when(gate)
        def _():
            dgain = jnp.sum(jnp.sum(rs_v[...].astype(F32), axis=0) * x_my * r_my, axis=0, keepdims=True)
            for j in range(n):
                piece = jnp.concatenate([dgain[:, cols(j, wcol)], dlg[:, cols(j, ccol)]], axis=1)
                for i in range(piece.shape[1] // lanes):
                    sg_v[j, i : i + 1] = piece[:, cols(i, lanes)]
            sr_v[me * n_t + ten] = sg_v[me]
            for m in range(micros):
                ig_ref[m] = dx_v[m * chunk : (m + 1) * chunk]

        for j in range(n):
            for t in range(n_t):
                copy = rcopy(sg_v.at[j], sr_v.at[me * n_t + ten], sg_s.at[0], sg_r.at[0], dev(j, t))
                begin(both(jnp.logical_or(j != me, t != ten), gate), copy, sent=True)
        settle(gate, sr_v.at[pl.ds(0, n * n_t - 1)], sg_s.at[0])

    finish(lower)
    finish(last)
    for across in (True, False):
        for k in range(4):
            spread_block(k, last, across)
    sum_latent(last)
    relay(0, nc_v, gate=last)
    relay(1, cc_v, gate=last)
    relay(4, rk_v, gate=last)
    relay(2, uc_v, gate=last)
    for k, dest in ((0, nc_v), (1, cc_v), (4, rk_v)):
        pass_on(k, dest, last)
    for k in range(4):
        hand_on(k, last)
    relay(3, dl_v, gate=last)
    for k in range(4):
        collect_block(k)
    pass_on(2, uc_v)
    collect(4, rk_v)
    for b in range(n):
        few = sv_v[b, :, :NOPE]
        ds = [jnp.where(same, mm_nt(few, picks[h]), 0.0).astype(BF) for h in range(2)]
        part = lambda i: fw_v[b, i // 2, :, cols(i % 2, NOPE)]
        dq_v[b] = query_grad(ds, part(2), part(3), rk_v[b].reshape(rows, 2 * ROPE))
        for h in range(2):
            de_v[b, :, cols(2 * h, NOPE)] = mm_tn(ds[h], part(h)).astype(BF)
            de_v[b, :, cols(2 * h + 1, NOPE)] = sv_v[b, :, cols(1 + h, VDIM)]
    collect(0, nc_v)
    collect(1, cc_v)
    gq_ref[...] = mm_tn(nc_v[...].reshape(n * rows, wcol), dq_v[...].reshape(n * rows, dq_v.shape[2]))
    ge_ref[...] = mm_tn(cc_v[...].reshape(n * rows, ccol), de_v[...].reshape(n * rows, de_v.shape[2]))
    collect(2, uc_v)
    mixed = fw_v[:, 2].reshape(n * rows, 2 * VDIM)
    go_ref[...] = mm_tn(mixed, uc_v[...].reshape(n * rows, wcol))
    pass_on(3, dl_v)
    collect(3, dl_v)
    gl_ref[...] = mm_tn(dl_v[...].reshape(n * rows, dl_v.shape[3]), nc_v[...].reshape(n * rows, wcol))
    arrived(me >= 0, sr_v.at[pl.ds(0, n * n_t - 1)], sg_r.at[0])
    summed = jnp.sum(sr_v[...], axis=0)
    for i in range(wcol // lanes):
        gg_ref[:, cols(i, lanes)] = summed[i : i + 1]
    for i in range(ccol // lanes):
        glg_ref[:, cols(i, lanes)] = summed[wcol // lanes + i : wcol // lanes + i + 1]
    for cond, copy in drains:
        @pl.when(cond)
        def _(copy=copy):
            copy.wait_send()


def hand_over(*refs):
    for source, dest in zip(refs[:7], refs[7:]):
        dest[...] = source[...]


def section_step(saved, top_grad, gain, w_query, w_latent, compressed_gain, expand_weight, w_output):
    n_pipe, n, n_t = (lax.axis_size(a) for a in ("pipe", "dp", "tensor"))
    micros, seq, width = saved.shape[1:]
    wcol, ccol = gain.shape[1], compressed_gain.shape[1]
    rows, share = micros * seq, micros * seq // n_t
    qcols, lcols = w_query.shape[2], w_latent.shape[2]
    ecols, orows = expand_weight.shape[2], w_output.shape[1]
    order = np.arange(rows)
    place = (order // share) * (seq // n_t) + order % (seq // n_t)
    pair = np.arange(2 * ROPE) % (ROPE // 2)
    angle = place[:, None] * np.exp(-np.log(10000.0) * pair / (ROPE // 2))[None, :]
    sign = np.where(np.arange(2 * ROPE) % ROPE < ROPE // 2, -1.0, 1.0)
    cosine = jnp.asarray(np.cos(angle), F32)
    sine = jnp.asarray(np.sin(angle) * sign, F32)
    operands = (
        saved[0], top_grad, gain, compressed_gain, w_query[0], w_latent[0].T,
        expand_weight[0], w_output[0], cosine, sine,
    )
    vm = pl.BlockSpec(memory_space=pltpu.VMEM)
    shape = jax.ShapeDtypeStruct
    kept = pltpu.VMEM
    sem = lambda *dims: pltpu.SemaphoreType.DMA(dims)
    small = wcol + ccol
    ig, gg, gq, gl, glg, ge, go = pl.pallas_call(
        lambda *refs: section_kernel((n_pipe, n, n_t, micros, seq), *refs),
        name="section_step",
        out_shape=(
            kept((micros, seq // n_t, width), BF),
            kept((1, wcol), F32),
            kept((wcol, qcols), F32),
            kept((lcols, wcol), F32),
            kept((1, ccol), F32),
            kept((ccol, ecols), F32),
            kept((orows, wcol), F32),
        ),
        in_specs=[pl.BlockSpec(memory_space=pl.ANY)] * 10,
        out_specs=(vm,) * 7,
        scratch_shapes=[
            *(pltpu.VMEM(a.shape, a.dtype) for a in operands),
            pltpu.VMEM((rows, width), BF),
            pltpu.VMEM((micros, seq, width), BF),
            pltpu.VMEM((8, small), F32),
            pltpu.VMEM((n, 8, small), F32),
            pltpu.VMEM((share, width), BF),
            pltpu.VMEM((n_t, share, width), BF),
            pltpu.VMEM((share, width), BF),
            pltpu.VMEM((rows, n * ccol), BF),
            pltpu.VMEM((n, wcol, qcols), BF),
            pltpu.VMEM((n, n_t, lcols // n_t, wcol), BF),
            pltpu.VMEM((n, ccol, ecols), BF),
            pltpu.VMEM((n, orows, wcol), BF),
            pltpu.VMEM((n, n_t, share, wcol), BF),
            pltpu.VMEM((n, n_t, share, ccol), BF),
            pltpu.VMEM((n, n_t, share, wcol), BF),
            pltpu.VMEM((n, n_t, share, lcols), BF),
            pltpu.VMEM((n, n_t, share, 2 * ROPE), BF),
            pltpu.VMEM((rows, 2 * ROPE), BF),
            pltpu.VMEM((3, rows, orows), BF),
            pltpu.VMEM((n, 3, rows, orows), BF),
            pltpu.VMEM((rows, NOPE + orows), BF),
            pltpu.VMEM((n, rows, NOPE + orows), BF),
            pltpu.VMEM((n_t, share, width), BF),
            pltpu.VMEM((n_t, share, width), BF),
            pltpu.VMEM((n_t, share, lcols), BF),
            pltpu.VMEM((n_t, share, lcols), BF),
            pltpu.VMEM((share, width), BF),
            pltpu.VMEM((n, 8 * -(-small // 1024), 128), F32),
            pltpu.VMEM((n * n_t, 8 * -(-small // 1024), 128), F32),
            pltpu.VMEM((n, rows, qcols), BF),
            pltpu.VMEM((n, rows, ecols), BF),
            sem(1), sem(1), sem(1), sem(1), sem(1), sem(n), sem(1), sem(1), sem(1),
            sem(3), sem(3, n), sem(3), sem(3), sem(5), sem(5), sem(n), sem(5), sem(5), sem(5),
            sem(4), sem(4, n), sem(4), sem(2), sem(2), sem(n_t // 2 + 1), sem(n_t), sem(1), sem(1), sem(1),
            sem(1), sem(1), sem(len(operands)),
        ],
        compiler_params=pltpu.CompilerParams(
            collective_id=0, has_side_effects=True, vmem_limit_bytes=60 * 1024 * 1024
        ),
    )(*operands)
    parts = [pltpu.with_memory_space_constraint(p, pltpu.VMEM) for p in (ig, gg, gq, gl, glg, ge, go)]
    ig, gg, gq, gl, glg, ge, go = pl.pallas_call(
        hand_over,
        name="hand_over",
        out_shape=tuple(shape(p.shape, p.dtype) for p in parts),
        in_specs=[vm] * 7,
        out_specs=(vm,) * 7,
    )(*parts)
    return ig[None], gg, gq[None], gl.T[None], glg, ge[None], go[None]


def choose(saved, top_grad, gain, w_query, w_latent, compressed_gain, expand_weight, w_output):
    arrays = (saved, top_grad, gain, w_query, w_latent, compressed_gain, expand_weight, w_output)
    n, n_t = lax.axis_size("dp"), lax.axis_size("tensor")
    fits = (
        n == 4
        and n_t == 4
        and saved.shape[1] == 2
        and saved.shape[2] == ROPE
        and w_query.shape[2] == 2 * (NOPE + ROPE)
        and w_output.shape[1] == 2 * VDIM
        and gain.shape[1] % 128 == 0
        and compressed_gain.shape[1] % 128 == 0
        and n * compressed_gain.shape[1] + ROPE == w_latent.shape[2]
        and w_latent.shape[2] % (16 * n_t) == 0
    )
    return section_step(*arrays) if fits else shards(*arrays)


def solution(mesh):
    in_specs = (
        P("pipe", None, "dp", None),
        P(None, "dp", None),
        P("pipe", "dp"),
        P("pipe", "dp", "tensor"),
        P("pipe", "dp", None),
        P("pipe", "dp"),
        P("pipe", "dp", "tensor"),
        P("pipe", "tensor", "dp"),
    )
    out_specs = (
        P("pipe", None, ("dp", "tensor"), None),
        P("pipe", "dp"),
        P("pipe", "dp", "tensor"),
        P("pipe", "dp", None),
        P("pipe", "dp"),
        P("pipe", "dp", "tensor"),
        P("pipe", "tensor", "dp"),
    )
    return jax.shard_map(choose, mesh=mesh, in_specs=in_specs, out_specs=out_specs, check_vma=False)
```

```python
import jax
import jax.numpy as jnp
from jax import lax
import numpy as np
from jax.experimental import pallas as pl
from jax.experimental.pallas import tpu as pltpu
from jax.sharding import PartitionSpec as P

NOPE = 128
ROPE = 64
VDIM = 128
COMPRESSED_RANK = 512


EPS = 1e-06


def passed_along(value, axis, steps):
    count = lax.axis_size(axis)
    first, last = (max(0, -steps), min(count, count - steps))
    return lax.ppermute(value, axis, [(source, source + steps) for source in range(first, last)])


def root_mean_scale(values, scale):
    return values * lax.rsqrt(jnp.mean(values * values, axis=-1, keepdims=True) + EPS) * scale


def rotary_angles(values):
    length = values.shape[0]
    half = values.shape[-1] // 2
    freq = jnp.exp(-jnp.log(10000.0) * jnp.arange(half, dtype=jnp.float32) / half)
    angle = jnp.arange(length, dtype=jnp.float32)[:, None] * freq[None, :]
    cosine = jnp.cos(angle)[:, None, :]
    sine = jnp.sin(angle)[:, None, :]
    first = values[..., :half]
    second = values[..., half:]
    return jnp.concatenate(
        [first * cosine - second * sine, second * cosine + first * sine], axis=-1
    )


def branch(normed, w_q, w_lat, latent_norm_gain, w_exp, w_out):
    length = normed.shape[0]
    heads = w_q.shape[1] // (NOPE + ROPE)
    rounded = normed.astype(jnp.bfloat16)
    query = jnp.dot(rounded, w_q, preferred_element_type=jnp.float32).reshape(
        length, heads, NOPE + ROPE
    )
    latent_state = jnp.dot(rounded, w_lat, preferred_element_type=jnp.float32)
    compressed_state = root_mean_scale(latent_state[:, :COMPRESSED_RANK], latent_norm_gain).astype(
        jnp.bfloat16
    )
    rotary_key_part = rotary_angles(latent_state[:, None, COMPRESSED_RANK:])[:, 0, :]
    expanded = jnp.dot(compressed_state, w_exp, preferred_element_type=jnp.float32).reshape(
        length, heads, NOPE + VDIM
    )
    key_nope = expanded[:, :, :NOPE]
    values = expanded[:, :, NOPE:].astype(jnp.bfloat16)
    query_rope = rotary_angles(query[:, :, NOPE:])
    scores = jnp.einsum("qhd,khd->hqk", query[:, :, :NOPE], key_nope) + jnp.einsum(
        "qhd,kd->hqk", query_rope, rotary_key_part
    )
    scores = scores * (NOPE + ROPE) ** (-0.5)
    causal = jnp.arange(length)[:, None] >= jnp.arange(length)[None, :]
    scores = jnp.where(causal[None], scores, -1e30)
    weights = jax.nn.softmax(scores, axis=-1).astype(jnp.bfloat16)
    mixed = jnp.einsum("hqk,khd->qhd", weights.astype(jnp.float32), values.astype(jnp.float32))
    mixed = mixed.astype(jnp.bfloat16).reshape(length, heads * VDIM)
    return jnp.dot(mixed, w_out, preferred_element_type=jnp.float32)


def shards(saved, top_grad, gain, w_query, w_latent, compressed_gain, expand_weight, w_output):
    gathered = (
        lax.all_gather(gain, "dp", axis=1, tiled=True),
        lax.all_gather(w_query, "dp", axis=1, tiled=True),
        lax.all_gather(w_latent, "dp", axis=1, tiled=True),
        lax.all_gather(compressed_gain, "dp", axis=1, tiled=True),
        lax.all_gather(expand_weight, "dp", axis=1, tiled=True),
        lax.all_gather(w_output, "dp", axis=2, tiled=True),
    )
    gain32 = gathered[0][0].astype(jnp.float32)
    query_all = gathered[1][0]
    latent_all = gathered[2][0]
    lgain32 = gathered[3][0].astype(jnp.float32)
    expand_all = gathered[4][0]
    output_all = gathered[5][0]
    sections = lax.axis_size("pipe")
    section_index = lax.axis_index("pipe")
    tensor_count = lax.axis_size("tensor")
    tensor_rank = lax.axis_index("tensor")
    micro_count = saved.shape[1]
    length = saved.shape[2]
    width = saved.shape[3]
    share = length // tensor_count

    def compute(normed, upstream):
        unused, pull = jax.vjp(
            lambda value: branch(value, query_all, latent_all, lgain32, expand_all, output_all),
            normed,
        )
        return pull(upstream.astype(jnp.float32))[0]

    def skip(normed, upstream):
        return jnp.zeros_like(normed)

    gain_total = jnp.zeros((width,), jnp.float32)
    results = jnp.zeros((micro_count, share, width), jnp.bfloat16)
    stored = jnp.zeros((micro_count, length, width), jnp.bfloat16)
    received = jnp.zeros((length, width), jnp.bfloat16)
    for tick in range(sections + micro_count - 1):
        micro = tick - (sections - 1 - section_index)
        active = jnp.logical_and(micro >= 0, micro < micro_count)
        picked = jnp.clip(micro, 0, micro_count - 1)
        x_rows = lax.dynamic_index_in_dim(saved[0], picked, 0, keepdims=False)
        top_rows = lax.dynamic_index_in_dim(top_grad, picked, 0, keepdims=False)
        arrived = received
        upstream = jnp.where(section_index == sections - 1, top_rows, arrived)
        x_float = x_rows.astype(jnp.float32)
        normed, norm_pull = jax.vjp(root_mean_scale, x_float, gain32)
        branch_grad = lax.cond(active, compute, skip, normed, upstream)
        d_normed = lax.psum(branch_grad.astype(jnp.bfloat16), "tensor").astype(jnp.float32)
        dx_norm, d_gain = norm_pull(d_normed)
        dx = (upstream.astype(jnp.float32) + dx_norm).astype(jnp.bfloat16)
        gain_total = gain_total + jnp.where(active, d_gain, 0.0)
        mine = lax.dynamic_slice_in_dim(dx, tensor_rank * share, share, 0)
        chosen = (jnp.arange(micro_count) == micro)[:, None, None]
        results = jnp.where(chosen, mine[None], results)
        stored = jnp.where(chosen, upstream[None], stored)
        received = passed_along(dx, "pipe", -1)
    totals = (
        jnp.zeros(query_all.shape, jnp.float32),
        jnp.zeros(latent_all.shape, jnp.float32),
        jnp.zeros(lgain32.shape, jnp.float32),
        jnp.zeros(expand_all.shape, jnp.float32),
        jnp.zeros(output_all.shape, jnp.float32),
    )
    for micro_index in range(micro_count):
        normed_again = root_mean_scale(saved[0, micro_index].astype(jnp.float32), gain32)
        unused, weight_pull = jax.vjp(
            lambda w_q, w_lat, lat_gain, w_exp, w_out: branch(
                normed_again, w_q, w_lat, lat_gain, w_exp, w_out
            ),
            query_all,
            latent_all,
            lgain32,
            expand_all,
            output_all,
        )
        cotangents = weight_pull(stored[micro_index].astype(jnp.float32))
        totals = tuple(
            (total + piece.astype(jnp.float32) for total, piece in zip(totals, cotangents))
        )
    gain_part = jnp.where(tensor_rank == 0, gain_total, 0.0)
    grad_q, grad_lat, grad_lg, grad_e, grad_o = totals
    out_q, part_lat, part_lg, out_e, out_o, part_gain = (
        lax.psum_scatter(grad_q.astype(jnp.bfloat16), "dp", scatter_dimension=0, tiled=True).astype(
            jnp.float32
        ),
        lax.psum_scatter(
            grad_lat.astype(jnp.bfloat16), "dp", scatter_dimension=0, tiled=True
        ).astype(jnp.float32),
        lax.psum_scatter(
            grad_lg.astype(jnp.bfloat16), "dp", scatter_dimension=0, tiled=True
        ).astype(jnp.float32),
        lax.psum_scatter(grad_e.astype(jnp.bfloat16), "dp", scatter_dimension=0, tiled=True).astype(
            jnp.float32
        ),
        lax.psum_scatter(grad_o.astype(jnp.bfloat16), "dp", scatter_dimension=1, tiled=True).astype(
            jnp.float32
        ),
        lax.psum_scatter(
            gain_part.astype(jnp.bfloat16), "dp", scatter_dimension=0, tiled=True
        ).astype(jnp.float32),
    )
    out_lat, out_lg, out_gain = (
        lax.psum(part_lat.astype(jnp.bfloat16), "tensor").astype(jnp.float32),
        lax.psum(part_lg.astype(jnp.bfloat16), "tensor").astype(jnp.float32),
        lax.psum(part_gain.astype(jnp.bfloat16), "tensor").astype(jnp.float32),
    )
    return (
        results[None],
        out_gain[None],
        out_q[None],
        out_lat[None],
        out_lg[None],
        out_e[None],
        out_o[None],
    )


MESH = pl.DeviceIdType.MESH
BF = jnp.bfloat16
F32 = jnp.float32


def mm(a, b):
    return lax.dot_general(a, b, (((1,), (0,)), ((), ())), preferred_element_type=F32)


def mm_nt(a, b):
    return lax.dot_general(a, b, (((1,), (1,)), ((), ())), preferred_element_type=F32)


def mm_tn(a, b):
    return lax.dot_general(a, b, (((0,), (0,)), ((), ())), preferred_element_type=F32)


def half_swap(v):
    lane = lax.broadcasted_iota(jnp.int32, v.shape, 1)
    ahead = pltpu.roll(v, v.shape[1] - ROPE // 2, 1)
    behind = pltpu.roll(v, ROPE // 2, 1)
    return jnp.where(lax.rem(lane, ROPE) < ROPE // 2, ahead, behind)


def section_kernel(
    dims,
    saved_in, top_in, gain_in, lgain_in, wq_in, wl_in, we_in, wo_in, cos_in, sin_in,
    ig_ref, gg_ref, gq_ref, gl_ref, glg_ref, ge_ref, go_ref,
    saved_ref, top_ref, gain_ref, lgain_ref, wq_ref, wl_ref, we_ref, wo_ref, cos_ref, sin_ref,
    x_v, xs_v, own_v, sm_v, nm_v, u_v, um_v, cb_v, wq_v, wl_v, we_v, wo_v,
    nc_v, cc_v, uc_v, dl_v, rk_v, ro_v, fo_v, fw_v, so_v, sv_v, part_v, rs_v, lp_v, ls_v, dx_v, sg_v, sr_v,
    dq_v, de_v,
    dp_s, dp_r, x_s, x_r, wz_s, wz_r, wh_s, wt_s, wt_r, w_s, w_r, f_s, f_r, z_s, z_r, zl_r, t_s, ta_r, tb_r,
    b_s, b_r, bh_s, rs_s, rs_r, p_s, u_r, um_r, uf_s, uf_r, sg_s, sg_r, in_s,
):
    n_pipe, n, n_t, micros, seq = dims
    sec, me, ten = lax.axis_index("pipe"), lax.axis_index("dp"), lax.axis_index("tensor")
    rows = micros * seq
    chunk = seq // n_t
    share = micros * chunk
    width = x_v.shape[1]
    wcol, ccol = wq_v.shape[1], we_v.shape[1]
    rank = n * ccol
    quarter = wl_v.shape[2]
    core = lax.rem(ten, 2)
    partner = ten + 1 - 2 * core
    opposite = lax.rem(ten + 2, n_t)
    par = lax.rem(me, 2)
    mate = me + 1 - 2 * par
    group = ten - core + par
    block = me - par + core
    primary = core == par
    secondary = jnp.logical_not(primary)
    half = me // 2
    near = 2 - half
    middle = jnp.logical_or(me == 1, me == 2)
    last = sec == n_pipe - 1
    lower = jnp.logical_not(last)
    both = jnp.logical_and
    drains = []

    def rcopy(a, b, ss, rs, dev):
        return pltpu.make_async_remote_copy(
            src_ref=a, dst_ref=b, send_sem=ss, recv_sem=rs, device_id=dev, device_id_type=MESH
        )

    def begin(cond, copy, sent=False):
        @pl.when(cond)
        def _():
            copy.start()

        if not sent:
            drains.append((cond, copy))

    def settle(cond, ref, ss):
        drains.append((cond, rcopy(ref, ref, ss, x_r.at[0], dev(me, partner))))

    def arrived(cond, ref, rs):
        @pl.when(cond)
        def _():
            rcopy(ref, ref, x_s.at[0], rs, dev(me, partner)).wait_recv()

    def dev(d, t):
        return (sec, d, t)

    def cols(j, size):
        return slice(j * size, (j + 1) * size)

    def mine(ref):
        at = pl.ds(pl.multiple_of(ten * chunk, chunk), chunk)
        return jnp.concatenate([ref[m, at] for m in range(micros)], axis=0)

    def by_share(store, ref):
        for j in range(n_t):
            for m in range(micros):
                store(j, m, ref[m, j * chunk : (j + 1) * chunk])

    def x_store(j, m, value):
        x_v[j * share + m * chunk : j * share + (m + 1) * chunk] = value

    def u_store(j, m, value):
        u_v[j, m * chunk : (m + 1) * chunk] = value

    inputs = (saved_in, top_in, gain_in, lgain_in, wq_in, wl_in, we_in, wo_in, cos_in, sin_in)
    places = (saved_ref, top_ref, gain_ref, lgain_ref, wq_ref, wl_ref, we_ref, wo_ref, cos_ref, sin_ref)
    fetches = [pltpu.make_async_copy(a, b, in_s.at[i]) for i, (a, b) in enumerate(zip(inputs, places))]
    for copy in fetches:
        copy.start()

    barrier = pltpu.get_barrier_semaphore()
    for j in range(n_t):
        for d in range(n):
            @pl.when(jnp.logical_or(d != me, j != ten))
            def _():
                pl.semaphore_signal(barrier, inc=1, device_id=dev(d, j), device_id_type=MESH)

        @pl.when(sec > 0)
        def _():
            pl.semaphore_signal(barrier, inc=1, device_id=(sec - 1, me, j), device_id_type=MESH)

        @pl.when(lower)
        def _():
            pl.semaphore_signal(barrier, inc=1, device_id=(sec + 1, me, j), device_id_type=MESH)

    for copy in fetches:
        copy.wait()

    own_v[:, :wcol] = jnp.broadcast_to(gain_ref[...].astype(F32), (8, wcol))
    own_v[:, wcol:] = jnp.broadcast_to(lgain_ref[...].astype(F32), (8, ccol))

    @pl.when(last)
    def _():
        um_v[...] = mine(top_ref)

    @pl.when(both(last, primary))
    def _():
        by_share(u_store, top_ref)

    neighbours = jnp.minimum(sec, 1) + jnp.minimum(n_pipe - 1 - sec, 1)
    pl.semaphore_wait(barrier, n * n_t - 1 + neighbours * n_t)

    def spread_dp(k, source, dest):
        for j in range(n):
            begin(j != me, rcopy(source(j), dest.at[me], dp_s.at[k], dp_r.at[k], dev(j, ten)), sent=True)
        settle(me >= 0, dest.at[pl.ds(0, n - 1)], dp_s.at[k])

    def collect_dp(k, dest):
        arrived(me >= 0, dest.at[pl.ds(0, n - 1)], dp_r.at[k])

    def spread_z(k, source, dest, slot, rank_to, gate=None):
        for e in range(n):
            cond = jnp.logical_or(e != me, rank_to != ten)
            if gate is not None:
                cond = both(cond, gate)
            rs = zl_r.at[slot] if k == 3 else z_r.at[k]
            begin(cond, rcopy(source(e), dest.at[slot, rank_to], z_s.at[k], rs, dev(e, rank_to)), sent=True)
        on = me >= 0 if gate is None else gate
        if k in (1, 4):
            settle(both(on, primary), dest.at[0, pl.ds(0, n - 1)], z_s.at[k])
            settle(both(on, secondary), dest.at[0, pl.ds(0, n)], z_s.at[k])
        else:
            settle(on, dest.at[0, pl.ds(0, n - 1)], z_s.at[k])

    def relay(k, dest, gate):
        def share_slot(b):
            for to, rs in ((opposite, ta_r), (partner, tb_r)):
                copy = rcopy(dest.at[b, ten], dest.at[b, ten], t_s.at[k], rs.at[k], dev(me, to))
                begin(gate, copy, sent=True)

        if k == 3:
            for b in range(n):
                arrived(both(b != me, gate), dest.at[b, ten], zl_r.at[b])
                share_slot(b)
        else:
            few, every = dest.at[pl.ds(0, n - 1), ten], dest.at[pl.ds(0, n), ten]
            if k in (1, 4):
                arrived(both(gate, primary), few, z_r.at[k])
                arrived(both(gate, secondary), every, z_r.at[k])
            else:
                arrived(gate, few, z_r.at[k])
            for b in range(n):
                share_slot(b)

    def pass_on(k, dest, gate=True):
        gate = both(me >= 0, gate)
        arrived(gate, dest.at[pl.ds(0, n), opposite], ta_r.at[k])
        for b in range(n):
            at = dest.at[b, opposite]
            begin(gate, rcopy(at, at, t_s.at[k], tb_r.at[k], dev(me, partner)), sent=True)
        settle(gate, dest.at[pl.ds(0, n - 1)], t_s.at[k])

    def collect(k, dest):
        arrived(me >= 0, dest.at[pl.ds(0, 2)], tb_r.at[k])

    def landing(k, b):
        return sv_v.at[b] if k == 3 else fw_v.at[b, k]

    def spread_block(k, gate, across):
        source = so_v if k == 3 else fo_v.at[k]
        for e in range(n):
            wanted = near == e if across else both(half == e // 2, jnp.logical_or(e != me, secondary))
            copy = rcopy(source, landing(k, block), b_s.at[k], b_r.at[k, block], dev(e, group))
            begin(both(wanted, gate), copy, sent=True)
        if across:
            several = lambda c: sv_v.at[pl.ds(0, c)] if k == 3 else fw_v.at[pl.ds(0, c), k]
            settle(both(gate, primary), several(2), b_s.at[k])
            settle(both(gate, secondary), several(3), b_s.at[k])

    def hand_on(k, gate, early=None):
        for b in range(n):
            cond = both(both(middle, half != b // 2), gate)
            if early is not None:
                cond = both(cond, core == b % 2 if early else core != b % 2)
            at = landing(k, b)
            arrived(cond, at, b_r.at[k, b])
            begin(cond, rcopy(at, at, bh_s.at[k], b_r.at[k, b], dev(mate, ten)), sent=True)
        two = sv_v.at[pl.ds(0, 2)] if k == 3 else fw_v.at[pl.ds(0, 2), k]
        if not early:
            settle(both(middle, gate), two, bh_s.at[k])

    def collect_block(k):
        for b in range(n):
            handed = both(middle, half != b // 2)
            cond = both(jnp.logical_or(b != me, secondary), jnp.logical_not(handed))
            arrived(cond, landing(k, b), b_r.at[k, b])

    spread_dp(0, lambda j: own_v, sm_v)
    sm_v[me] = own_v[...]
    my_quarter = wl_ref.at[pl.ds(pl.multiple_of(ten * quarter, quarter), quarter)]
    for level in (near, mate):
        begin(me >= 0, rcopy(my_quarter, wl_v.at[me, ten], wz_s.at[0], wz_r.at[me], dev(level, ten)), sent=True)
    settle(me >= 0, wl_v.at[0, pl.ds(0, 2)], wz_s.at[0])
    weights = ((wq_ref, wq_v), (we_ref, we_v), (wo_ref, wo_v))

    begin(primary, rcopy(saved_ref, xs_v, x_s.at[0], x_r.at[0], dev(mate, ten)))

    def give(k, gate=True):
        ref, store = weights[k]
        for i in range(n // 2):
            level = 2 * i + core
            copy = rcopy(ref, store.at[me], w_s.at[k], w_r.at[k, me], dev(level, ten))
            begin(both(level != me, gate), copy, sent=True)
        settle(both(primary, gate), store.at[pl.ds(0, n // 2 - 1)], w_s.at[k])
        settle(both(secondary, gate), store.at[pl.ds(0, n // 2)], w_s.at[k])
        copy = rcopy(ref, store.at[me], f_s.at[k], f_r.at[k], dev(me, partner))
        begin(both(primary, gate), copy, sent=True)

    def give_rest(gate):
        give(1, gate)
        for s in range(n_t):
            copy = rcopy(u_v.at[s], u_v.at[s], uf_s.at[0], uf_r.at[0], dev(mate, ten))
            begin(both(both(last, primary), gate), copy, sent=True)
        give(2, gate)
        spread_z(2, um_cols, uc_v, me, ten, gate=both(last, gate))

    um_cols = lambda e: um_v.at[:, pl.ds(e * wcol, wcol)]
    give(0)
    give_rest(jnp.logical_not(middle))

    for j in range(n_t):
        wl_v[me, j] = wl_ref[j * quarter : (j + 1) * quarter]

    @pl.when(primary)
    def _():
        for ref, store in weights:
            store[me] = ref[...]

        by_share(x_store, saved_ref)

    def to_ten(b, valid):
        for j in range(n_t):
            begin(
                both(valid, j != ten),
                rcopy(wl_v.at[b, ten], wl_v.at[b, ten], wt_s.at[0], wt_r.at[0], dev(me, j)),
                sent=True,
            )

    for b in range(n):
        arrived(b != me, wl_v.at[b, ten], wz_r.at[b])
        begin(
            both(middle, half != b // 2),
            rcopy(wl_v.at[b, ten], wl_v.at[b, ten], wh_s.at[0], wz_r.at[b], dev(mate, ten)),
            sent=True,
        )
        to_ten(b, b != me)
    settle(middle, wl_v.at[0, pl.ds(0, 2)], wh_s.at[0])
    wl_peers = wl_v.at[pl.ds(0, n - 1), pl.ds(0, n_t - 1)]
    settle(me >= 0, wl_peers, wt_s.at[0])
    give_rest(middle)

    collect_dp(0, sm_v)
    gain = jnp.concatenate([sm_v[d][0:1, :wcol] for d in range(n)], axis=1)
    lgain = jnp.concatenate([sm_v[d][0:1, wcol : wcol + ccol] for d in range(n)], axis=1)
    x_my = mine(saved_ref).astype(F32)
    r_my = lax.rsqrt(jnp.mean(x_my * x_my, axis=1, keepdims=True) + EPS)
    nm_v[...] = (x_my * r_my * gain).astype(BF)
    spread_z(0, lambda e: nm_v.at[:, pl.ds(e * wcol, wcol)], nc_v, me, ten)
    for j in range(n):
        @pl.when(j == me)
        def _():
            nc_v[j, ten] = nm_v[:, cols(j, wcol)]

    @pl.when(secondary)
    def _():
        rcopy(xs_v, xs_v, x_s.at[0], x_r.at[0], dev(me, partner)).wait_recv()
        by_share(x_store, xs_v)

    x32 = x_v[...].astype(F32)
    r = lax.rsqrt(jnp.mean(x32 * x32, axis=1, keepdims=True) + EPS)
    nb = (x32 * r * gain).astype(BF)

    def take(k):
        store = weights[k][1]
        for d in range(n):
            cond = both(primary, d != me)
            arrived(cond, store.at[d], w_r.at[k, d])
            begin(cond, rcopy(store.at[d], store.at[d], f_s.at[k], f_r.at[k], dev(me, partner)), sent=True)
        settle(primary, store, f_s.at[k])
        arrived(secondary, store, f_r.at[k])

    take(0)
    arrived(me >= 0, wl_peers, wt_r.at[0])

    wq = wq_v[...].reshape(width, wq_v.shape[2])
    wl = [wl_v[d].reshape(n_t * quarter, wcol) for d in range(n)]
    q = mm(nb, wq)
    lat = jnp.zeros((rows, n_t * quarter), F32)
    for d in range(n):
        lat = lat + mm_nt(nb[:, cols(d, wcol)], wl[d])
    l32 = lat[:, :rank]
    rl = lax.rsqrt(jnp.mean(l32 * l32, axis=1, keepdims=True) + EPS)
    cb = (l32 * rl * lgain).astype(BF)
    cb_v[...] = cb
    my_rows = pl.ds(pl.multiple_of(group * share, share), share)
    spread_z(1, lambda e: cb_v.at[my_rows, pl.ds(e * ccol, ccol)], cc_v, block, group)
    for j in range(n):
        @pl.when(both(j == me, primary))
        def _():
            cc_v[j, ten] = cb_v[my_rows, cols(j, ccol)]

    cosine, sine = cos_ref[...], sin_ref[...]
    lr = lat[:, rank:]
    lr2 = jnp.concatenate([lr, lr], axis=1)
    rk = (lr2 * cosine + half_swap(lr2) * sine).astype(BF)
    ro_v[...] = rk
    spread_z(4, lambda e: ro_v.at[my_rows], rk_v, block, group)

    @pl.when(primary)
    def _():
        rk_v[me, ten] = ro_v[my_rows]

    lane = lax.broadcasted_iota(jnp.int32, (rows, 2 * ROPE), 1)
    low = lane < ROPE
    q1, q2 = q[:, NOPE : 2 * NOPE], q[:, 2 * NOPE :]
    nope = (q[:, :NOPE], pltpu.roll(jnp.where(low, q2, q1), ROPE, 1))
    for h in range(2):
        fo_v[0, :, cols(h, NOPE)] = nope[h].astype(BF)
    spread_block(0, lower, True)
    spread_block(0, lower, False)
    qr_all = jnp.where(low, q1, q2)
    qr = qr_all * cosine + half_swap(qr_all) * sine
    row = lax.broadcasted_iota(jnp.int32, (rows, rows), 0)
    col = lax.broadcasted_iota(jnp.int32, (rows, rows), 1)

    def place(i):
        return (i // share) * chunk + lax.rem(i, chunk)

    same = lax.rem(row, share) // chunk == lax.rem(col, share) // chunk
    keep = jnp.logical_and(same, place(row) >= place(col))
    picks = [jnp.where(place(row) + h * seq == col, 1.0, 0.0).astype(BF) for h in range(2)]
    scale = (NOPE + ROPE) ** (-0.5)
    masks = (low, jnp.logical_not(low))
    take(1)
    we = we_v[...].reshape(n * ccol, we_v.shape[2])
    ex = mm(cb, we)
    for h in range(2):
        fo_v[1, :, cols(h, NOPE)] = ex[:, cols(2 * h, NOPE)].astype(BF)
    spread_block(1, lower, True)
    spread_block(1, lower, False)
    heads = []
    for h in range(2):
        qn = nope[h].astype(BF)
        kn = ex[:, h * (NOPE + VDIM) : h * (NOPE + VDIM) + NOPE].astype(BF)
        vv = ex[:, h * (NOPE + VDIM) + NOPE : (h + 1) * (NOPE + VDIM)].astype(BF)
        qh = jnp.where(masks[h], qr, 0.0).astype(BF)
        scores = (mm_nt(qn, kn) + mm_nt(qh, rk)) * scale
        scores = jnp.where(keep, scores, -1e30)
        e = jnp.exp(scores - jnp.max(scores, axis=1, keepdims=True))
        w32 = e / jnp.sum(e, axis=1, keepdims=True)
        wb = w32.astype(BF)
        fo_v[2, :, cols(h, VDIM)] = mm(wb, vv).astype(BF)
        heads.append((qn, kn, vv, qh, w32, wb))

    @pl.when(primary)
    def _():
        fw_v[me] = fo_v[...]

    spread_block(2, lower, True)
    spread_block(2, lower, False)
    take(2)
    relay(0, nc_v, gate=lower)
    relay(1, cc_v, gate=lower)
    relay(4, rk_v, gate=lower)
    for k in range(3):
        hand_on(k, lower)

    for s in range(n_t):
        cond = both(lower, primary)
        arrived(cond, u_v.at[s], u_r.at[s])
        begin(cond, rcopy(u_v.at[s], u_v.at[s], uf_s.at[0], uf_r.at[0], dev(mate, ten)), sent=True)
    settle(primary, u_v, uf_s.at[0])

    @pl.when(both(lower, primary))
    def _():
        um_v[...] = u_v[ten]

    arrived(both(lower, secondary), um_v, um_r.at[0])
    spread_z(2, um_cols, uc_v, me, ten, gate=lower)
    for j in range(n):
        @pl.when(j == me)
        def _():
            uc_v[j, ten] = um_v[:, cols(j, wcol)]

    arrived(secondary, u_v, uf_r.at[0])

    ub = u_v[...].reshape(rows, width)
    dm = jnp.zeros((rows, wo_v.shape[1]), F32)
    for j in range(n):
        dm = dm + mm_nt(ub[:, cols(j, wcol)], wo_v[j])
    dm = dm.astype(BF)

    def query_grad(slope, kn0, kn1, rk_b):
        dqr = jnp.where(low, mm(slope[0], rk_b), mm(slope[1], rk_b))
        dqr = dqr * cosine - half_swap(dqr) * sine
        turned = pltpu.roll(mm(slope[1], kn1), ROPE, 1)
        return jnp.concatenate(
            [
                mm(slope[0], kn0).astype(BF),
                jnp.where(low, dqr, turned).astype(BF),
                jnp.where(low, turned, dqr).astype(BF),
            ],
            axis=1,
        )

    drk = jnp.zeros((rows, 2 * ROPE), F32)
    slopes, pieces = [], []
    for h, (qn, kn, vv, qh, w32, wb) in enumerate(heads):
        dmh = dm[:, cols(h, VDIM)]
        dw = mm_nt(dmh, vv).astype(BF).astype(F32)
        ds = (w32 * (dw - jnp.sum(dw * w32, axis=1, keepdims=True)) * scale).astype(BF)
        drk = drk + mm_tn(ds, qh)
        slopes.append(ds)
        pieces += [mm_tn(ds, qn).astype(BF), mm_tn(wb, dmh).astype(BF)]
    drk = drk * cosine - half_swap(drk) * sine
    drk = drk + pltpu.roll(drk, ROPE, 1)
    so_v[:, cols(0, NOPE)] = (mm(slopes[0], picks[0]) + mm(slopes[1], picks[1])).astype(BF)
    so_v[:, cols(1, VDIM)] = pieces[1]
    so_v[:, cols(2, VDIM)] = pieces[3]
    dc = mm_nt(jnp.concatenate(pieces, axis=1), we)
    dlg = jnp.sum(dc * l32 * rl, axis=0, keepdims=True)
    dcg = dc * lgain
    dl = rl * dcg - l32 * (rl * rl * rl) * jnp.mean(l32 * dcg, axis=1, keepdims=True)
    dlat = jnp.concatenate([dl.astype(BF), drk[:, :ROPE].astype(BF)], axis=1)
    lp_v[...] = dlat.reshape(n_t, share, dlat.shape[1])

    @pl.when(primary)
    def _():
        ls_v[group] = lp_v[ten]

    shared = ((part_v, rs_v), (lp_v, ls_v))

    def share_out(k, gate):
        source, dest = shared[k]
        for i in range(n_t):
            s = lax.rem(ten - core + 2 + i, n_t)
            copy = rcopy(source.at[s], dest.at[group], rs_s.at[k], rs_r.at[k], dev(block, s))
            begin(both(jnp.logical_or(s != ten, secondary), gate), copy, sent=True)
        settle(both(primary, gate), dest.at[pl.ds(0, n_t - 1)], rs_s.at[k])
        settle(both(secondary, gate), dest, rs_s.at[k])

    share_out(1, lower)
    dq = query_grad(slopes, heads[0][1], heads[1][1], rk)
    dn = mm_nt(dq, wq) + jnp.concatenate([mm(dlat, wl[d]) for d in range(n)], axis=1)
    part_v[...] = dn.astype(BF).reshape(n_t, share, width)

    @pl.when(primary)
    def _():
        rs_v[group] = part_v[ten]
        sv_v[me] = so_v[...]

    share_out(0, last)
    share_out(1, last)
    spread_block(3, lower, False)
    spread_block(3, lower, True)

    def collect_shares(k, gate=True):
        dest = shared[k][1]
        arrived(both(primary, gate), dest.at[pl.ds(0, n_t - 1)], rs_r.at[k])
        arrived(both(secondary, gate), dest, rs_r.at[k])

    def sum_latent(gate):
        collect_shares(1, gate)

        @pl.when(gate)
        def _():
            dl_v[me, ten] = jnp.sum(ls_v[...].astype(F32), axis=0).astype(BF)

        spread_z(3, lambda e: dl_v.at[me, ten], dl_v, me, ten, gate=gate)

    for k, dest in ((0, nc_v), (1, cc_v), (4, rk_v)):
        pass_on(k, dest, lower)
    hand_on(3, lower, early=True)
    sum_latent(lower)
    share_out(0, lower)
    relay(2, uc_v, gate=lower)
    hand_on(3, lower, early=False)
    relay(3, dl_v, gate=lower)
    lanes = 128
    below = jnp.maximum(sec - 1, 0)

    def finish(gate):
        collect_shares(0, gate)

        @pl.when(gate)
        def _():
            dns = jnp.sum(rs_v[...].astype(F32), axis=0)
            dng = dns * gain
            u_my = um_v[...].astype(F32)
            dx = u_my + r_my * dng - x_my * (r_my * r_my * r_my) * jnp.mean(x_my * dng, axis=1, keepdims=True)
            dx_v[...] = dx.astype(BF)

        for i in range(n_t // 2):
            to = lax.rem(ten - core + 2 + 2 * i, n_t) + par
            copy = rcopy(dx_v, u_v.at[ten], p_s.at[i], u_r.at[ten], (below, me, to))
            begin(both(sec > 0, gate), copy)
        copy = rcopy(dx_v, um_v, p_s.at[n_t // 2], um_r.at[0], (below, me, ten))
        begin(both(both(sec > 0, secondary), gate), copy)

        @pl.when(gate)
        def _():
            dgain = jnp.sum(jnp.sum(rs_v[...].astype(F32), axis=0) * x_my * r_my, axis=0, keepdims=True)
            for j in range(n):
                piece = jnp.concatenate([dgain[:, cols(j, wcol)], dlg[:, cols(j, ccol)]], axis=1)
                for i in range(piece.shape[1] // lanes):
                    sg_v[j, i : i + 1] = piece[:, cols(i, lanes)]
            sr_v[me * n_t + ten] = sg_v[me]
            for m in range(micros):
                ig_ref[m] = dx_v[m * chunk : (m + 1) * chunk]

        for j in range(n):
            for t in range(n_t):
                copy = rcopy(sg_v.at[j], sr_v.at[me * n_t + ten], sg_s.at[0], sg_r.at[0], dev(j, t))
                begin(both(jnp.logical_or(j != me, t != ten), gate), copy, sent=True)
        settle(gate, sr_v.at[pl.ds(0, n * n_t - 1)], sg_s.at[0])

    finish(lower)
    finish(last)
    for across in (True, False):
        for k in range(4):
            spread_block(k, last, across)
    sum_latent(last)
    relay(0, nc_v, gate=last)
    relay(1, cc_v, gate=last)
    relay(4, rk_v, gate=last)
    relay(2, uc_v, gate=last)
    for k, dest in ((0, nc_v), (1, cc_v), (4, rk_v)):
        pass_on(k, dest, last)
    for k in range(4):
        hand_on(k, last)
    relay(3, dl_v, gate=last)
    for k in range(4):
        collect_block(k)
    pass_on(2, uc_v)
    collect(4, rk_v)
    for b in range(n):
        few = sv_v[b, :, :NOPE]
        ds = [jnp.where(same, mm_nt(few, picks[h]), 0.0).astype(BF) for h in range(2)]
        part = lambda i: fw_v[b, i // 2, :, cols(i % 2, NOPE)]
        dq_v[b] = query_grad(ds, part(2), part(3), rk_v[b].reshape(rows, 2 * ROPE))
        for h in range(2):
            de_v[b, :, cols(2 * h, NOPE)] = mm_tn(ds[h], part(h)).astype(BF)
            de_v[b, :, cols(2 * h + 1, NOPE)] = sv_v[b, :, cols(1 + h, VDIM)]
    pass_on(3, dl_v)
    collect(0, nc_v)
    collect(1, cc_v)
    gq_ref[...] = mm_tn(nc_v[...].reshape(n * rows, wcol), dq_v[...].reshape(n * rows, dq_v.shape[2]))
    ge_ref[...] = mm_tn(cc_v[...].reshape(n * rows, ccol), de_v[...].reshape(n * rows, de_v.shape[2]))
    collect(2, uc_v)
    mixed = fw_v[:, 2].reshape(n * rows, 2 * VDIM)
    go_ref[...] = mm_tn(mixed, uc_v[...].reshape(n * rows, wcol))
    collect(3, dl_v)
    gl_ref[...] = mm_tn(dl_v[...].reshape(n * rows, dl_v.shape[3]), nc_v[...].reshape(n * rows, wcol))
    arrived(me >= 0, sr_v.at[pl.ds(0, n * n_t - 1)], sg_r.at[0])
    summed = jnp.sum(sr_v[...], axis=0)
    for i in range(wcol // lanes):
        gg_ref[:, cols(i, lanes)] = summed[i : i + 1]
    for i in range(ccol // lanes):
        glg_ref[:, cols(i, lanes)] = summed[wcol // lanes + i : wcol // lanes + i + 1]
    for cond, copy in drains:
        @pl.when(cond)
        def _(copy=copy):
            copy.wait_send()


def hand_over(*refs):
    for source, dest in zip(refs[:7], refs[7:]):
        dest[...] = source[...]


def section_step(saved, top_grad, gain, w_query, w_latent, compressed_gain, expand_weight, w_output):
    n_pipe, n, n_t = (lax.axis_size(a) for a in ("pipe", "dp", "tensor"))
    micros, seq, width = saved.shape[1:]
    wcol, ccol = gain.shape[1], compressed_gain.shape[1]
    rows, share = micros * seq, micros * seq // n_t
    qcols, lcols = w_query.shape[2], w_latent.shape[2]
    ecols, orows = expand_weight.shape[2], w_output.shape[1]
    order = np.arange(rows)
    place = (order // share) * (seq // n_t) + order % (seq // n_t)
    pair = np.arange(2 * ROPE) % (ROPE // 2)
    angle = place[:, None] * np.exp(-np.log(10000.0) * pair / (ROPE // 2))[None, :]
    sign = np.where(np.arange(2 * ROPE) % ROPE < ROPE // 2, -1.0, 1.0)
    cosine = jnp.asarray(np.cos(angle), F32)
    sine = jnp.asarray(np.sin(angle) * sign, F32)
    operands = (
        saved[0], top_grad, gain, compressed_gain, w_query[0], w_latent[0].T,
        expand_weight[0], w_output[0], cosine, sine,
    )
    vm = pl.BlockSpec(memory_space=pltpu.VMEM)
    shape = jax.ShapeDtypeStruct
    kept = pltpu.VMEM
    sem = lambda *dims: pltpu.SemaphoreType.DMA(dims)
    small = wcol + ccol
    ig, gg, gq, gl, glg, ge, go = pl.pallas_call(
        lambda *refs: section_kernel((n_pipe, n, n_t, micros, seq), *refs),
        name="section_step",
        out_shape=(
            kept((micros, seq // n_t, width), BF),
            kept((1, wcol), F32),
            kept((wcol, qcols), F32),
            kept((lcols, wcol), F32),
            kept((1, ccol), F32),
            kept((ccol, ecols), F32),
            kept((orows, wcol), F32),
        ),
        in_specs=[pl.BlockSpec(memory_space=pl.ANY)] * 10,
        out_specs=(vm,) * 7,
        scratch_shapes=[
            *(pltpu.VMEM(a.shape, a.dtype) for a in operands),
            pltpu.VMEM((rows, width), BF),
            pltpu.VMEM((micros, seq, width), BF),
            pltpu.VMEM((8, small), F32),
            pltpu.VMEM((n, 8, small), F32),
            pltpu.VMEM((share, width), BF),
            pltpu.VMEM((n_t, share, width), BF),
            pltpu.VMEM((share, width), BF),
            pltpu.VMEM((rows, n * ccol), BF),
            pltpu.VMEM((n, wcol, qcols), BF),
            pltpu.VMEM((n, n_t, lcols // n_t, wcol), BF),
            pltpu.VMEM((n, ccol, ecols), BF),
            pltpu.VMEM((n, orows, wcol), BF),
            pltpu.VMEM((n, n_t, share, wcol), BF),
            pltpu.VMEM((n, n_t, share, ccol), BF),
            pltpu.VMEM((n, n_t, share, wcol), BF),
            pltpu.VMEM((n, n_t, share, lcols), BF),
            pltpu.VMEM((n, n_t, share, 2 * ROPE), BF),
            pltpu.VMEM((rows, 2 * ROPE), BF),
            pltpu.VMEM((3, rows, orows), BF),
            pltpu.VMEM((n, 3, rows, orows), BF),
            pltpu.VMEM((rows, NOPE + orows), BF),
            pltpu.VMEM((n, rows, NOPE + orows), BF),
            pltpu.VMEM((n_t, share, width), BF),
            pltpu.VMEM((n_t, share, width), BF),
            pltpu.VMEM((n_t, share, lcols), BF),
            pltpu.VMEM((n_t, share, lcols), BF),
            pltpu.VMEM((share, width), BF),
            pltpu.VMEM((n, 8 * -(-small // 1024), 128), F32),
            pltpu.VMEM((n * n_t, 8 * -(-small // 1024), 128), F32),
            pltpu.VMEM((n, rows, qcols), BF),
            pltpu.VMEM((n, rows, ecols), BF),
            sem(1), sem(1), sem(1), sem(1), sem(1), sem(n), sem(1), sem(1), sem(1),
            sem(3), sem(3, n), sem(3), sem(3), sem(5), sem(5), sem(n), sem(5), sem(5), sem(5),
            sem(4), sem(4, n), sem(4), sem(2), sem(2), sem(n_t // 2 + 1), sem(n_t), sem(1), sem(1), sem(1),
            sem(1), sem(1), sem(len(operands)),
        ],
        compiler_params=pltpu.CompilerParams(
            collective_id=0, has_side_effects=True, vmem_limit_bytes=60 * 1024 * 1024
        ),
    )(*operands)
    parts = [pltpu.with_memory_space_constraint(p, pltpu.VMEM) for p in (ig, gg, gq, gl, glg, ge, go)]
    ig, gg, gq, gl, glg, ge, go = pl.pallas_call(
        hand_over,
        name="hand_over",
        out_shape=tuple(shape(p.shape, p.dtype) for p in parts),
        in_specs=[vm] * 7,
        out_specs=(vm,) * 7,
    )(*parts)
    return ig[None], gg, gq[None], gl.T[None], glg, ge[None], go[None]


def choose(saved, top_grad, gain, w_query, w_latent, compressed_gain, expand_weight, w_output):
    arrays = (saved, top_grad, gain, w_query, w_latent, compressed_gain, expand_weight, w_output)
    n, n_t = lax.axis_size("dp"), lax.axis_size("tensor")
    fits = (
        n == 4
        and n_t == 4
        and saved.shape[1] == 2
        and saved.shape[2] == ROPE
        and w_query.shape[2] == 2 * (NOPE + ROPE)
        and w_output.shape[1] == 2 * VDIM
        and gain.shape[1] % 128 == 0
        and compressed_gain.shape[1] % 128 == 0
        and n * compressed_gain.shape[1] + ROPE == w_latent.shape[2]
        and w_latent.shape[2] % (16 * n_t) == 0
    )
    return section_step(*arrays) if fits else shards(*arrays)


def solution(mesh):
    in_specs = (
        P("pipe", None, "dp", None),
        P(None, "dp", None),
        P("pipe", "dp"),
        P("pipe", "dp", "tensor"),
        P("pipe", "dp", None),
        P("pipe", "dp"),
        P("pipe", "dp", "tensor"),
        P("pipe", "tensor", "dp"),
    )
    out_specs = (
        P("pipe", None, ("dp", "tensor"), None),
        P("pipe", "dp"),
        P("pipe", "dp", "tensor"),
        P("pipe", "dp", None),
        P("pipe", "dp"),
        P("pipe", "dp", "tensor"),
        P("pipe", "tensor", "dp"),
    )
    return jax.shard_map(choose, mesh=mesh, in_specs=in_specs, out_specs=out_specs, check_vma=False)
```

```python
import jax
import jax.numpy as jnp
from jax import lax
import numpy as np
from jax.experimental import pallas as pl
from jax.experimental.pallas import tpu as pltpu
from jax.sharding import PartitionSpec as P

NOPE = 128
ROPE = 64
VDIM = 128
COMPRESSED_RANK = 512


EPS = 1e-06


def passed_along(value, axis, steps):
    count = lax.axis_size(axis)
    first, last = (max(0, -steps), min(count, count - steps))
    return lax.ppermute(value, axis, [(source, source + steps) for source in range(first, last)])


def root_mean_scale(values, scale):
    return values * lax.rsqrt(jnp.mean(values * values, axis=-1, keepdims=True) + EPS) * scale


def rotary_angles(values):
    length = values.shape[0]
    half = values.shape[-1] // 2
    freq = jnp.exp(-jnp.log(10000.0) * jnp.arange(half, dtype=jnp.float32) / half)
    angle = jnp.arange(length, dtype=jnp.float32)[:, None] * freq[None, :]
    cosine = jnp.cos(angle)[:, None, :]
    sine = jnp.sin(angle)[:, None, :]
    first = values[..., :half]
    second = values[..., half:]
    return jnp.concatenate(
        [first * cosine - second * sine, second * cosine + first * sine], axis=-1
    )


def branch(normed, w_q, w_lat, latent_norm_gain, w_exp, w_out):
    length = normed.shape[0]
    heads = w_q.shape[1] // (NOPE + ROPE)
    rounded = normed.astype(jnp.bfloat16)
    query = jnp.dot(rounded, w_q, preferred_element_type=jnp.float32).reshape(
        length, heads, NOPE + ROPE
    )
    latent_state = jnp.dot(rounded, w_lat, preferred_element_type=jnp.float32)
    compressed_state = root_mean_scale(latent_state[:, :COMPRESSED_RANK], latent_norm_gain).astype(
        jnp.bfloat16
    )
    rotary_key_part = rotary_angles(latent_state[:, None, COMPRESSED_RANK:])[:, 0, :]
    expanded = jnp.dot(compressed_state, w_exp, preferred_element_type=jnp.float32).reshape(
        length, heads, NOPE + VDIM
    )
    key_nope = expanded[:, :, :NOPE]
    values = expanded[:, :, NOPE:].astype(jnp.bfloat16)
    query_rope = rotary_angles(query[:, :, NOPE:])
    scores = jnp.einsum("qhd,khd->hqk", query[:, :, :NOPE], key_nope) + jnp.einsum(
        "qhd,kd->hqk", query_rope, rotary_key_part
    )
    scores = scores * (NOPE + ROPE) ** (-0.5)
    causal = jnp.arange(length)[:, None] >= jnp.arange(length)[None, :]
    scores = jnp.where(causal[None], scores, -1e30)
    weights = jax.nn.softmax(scores, axis=-1).astype(jnp.bfloat16)
    mixed = jnp.einsum("hqk,khd->qhd", weights.astype(jnp.float32), values.astype(jnp.float32))
    mixed = mixed.astype(jnp.bfloat16).reshape(length, heads * VDIM)
    return jnp.dot(mixed, w_out, preferred_element_type=jnp.float32)


def shards(saved, top_grad, gain, w_query, w_latent, compressed_gain, expand_weight, w_output):
    gathered = (
        lax.all_gather(gain, "dp", axis=1, tiled=True),
        lax.all_gather(w_query, "dp", axis=1, tiled=True),
        lax.all_gather(w_latent, "dp", axis=1, tiled=True),
        lax.all_gather(compressed_gain, "dp", axis=1, tiled=True),
        lax.all_gather(expand_weight, "dp", axis=1, tiled=True),
        lax.all_gather(w_output, "dp", axis=2, tiled=True),
    )
    gain32 = gathered[0][0].astype(jnp.float32)
    query_all = gathered[1][0]
    latent_all = gathered[2][0]
    lgain32 = gathered[3][0].astype(jnp.float32)
    expand_all = gathered[4][0]
    output_all = gathered[5][0]
    sections = lax.axis_size("pipe")
    section_index = lax.axis_index("pipe")
    tensor_count = lax.axis_size("tensor")
    tensor_rank = lax.axis_index("tensor")
    micro_count = saved.shape[1]
    length = saved.shape[2]
    width = saved.shape[3]
    share = length // tensor_count

    def compute(normed, upstream):
        unused, pull = jax.vjp(
            lambda value: branch(value, query_all, latent_all, lgain32, expand_all, output_all),
            normed,
        )
        return pull(upstream.astype(jnp.float32))[0]

    def skip(normed, upstream):
        return jnp.zeros_like(normed)

    gain_total = jnp.zeros((width,), jnp.float32)
    results = jnp.zeros((micro_count, share, width), jnp.bfloat16)
    stored = jnp.zeros((micro_count, length, width), jnp.bfloat16)
    received = jnp.zeros((length, width), jnp.bfloat16)
    for tick in range(sections + micro_count - 1):
        micro = tick - (sections - 1 - section_index)
        active = jnp.logical_and(micro >= 0, micro < micro_count)
        picked = jnp.clip(micro, 0, micro_count - 1)
        x_rows = lax.dynamic_index_in_dim(saved[0], picked, 0, keepdims=False)
        top_rows = lax.dynamic_index_in_dim(top_grad, picked, 0, keepdims=False)
        arrived = received
        upstream = jnp.where(section_index == sections - 1, top_rows, arrived)
        x_float = x_rows.astype(jnp.float32)
        normed, norm_pull = jax.vjp(root_mean_scale, x_float, gain32)
        branch_grad = lax.cond(active, compute, skip, normed, upstream)
        d_normed = lax.psum(branch_grad.astype(jnp.bfloat16), "tensor").astype(jnp.float32)
        dx_norm, d_gain = norm_pull(d_normed)
        dx = (upstream.astype(jnp.float32) + dx_norm).astype(jnp.bfloat16)
        gain_total = gain_total + jnp.where(active, d_gain, 0.0)
        mine = lax.dynamic_slice_in_dim(dx, tensor_rank * share, share, 0)
        chosen = (jnp.arange(micro_count) == micro)[:, None, None]
        results = jnp.where(chosen, mine[None], results)
        stored = jnp.where(chosen, upstream[None], stored)
        received = passed_along(dx, "pipe", -1)
    totals = (
        jnp.zeros(query_all.shape, jnp.float32),
        jnp.zeros(latent_all.shape, jnp.float32),
        jnp.zeros(lgain32.shape, jnp.float32),
        jnp.zeros(expand_all.shape, jnp.float32),
        jnp.zeros(output_all.shape, jnp.float32),
    )
    for micro_index in range(micro_count):
        normed_again = root_mean_scale(saved[0, micro_index].astype(jnp.float32), gain32)
        unused, weight_pull = jax.vjp(
            lambda w_q, w_lat, lat_gain, w_exp, w_out: branch(
                normed_again, w_q, w_lat, lat_gain, w_exp, w_out
            ),
            query_all,
            latent_all,
            lgain32,
            expand_all,
            output_all,
        )
        cotangents = weight_pull(stored[micro_index].astype(jnp.float32))
        totals = tuple(
            (total + piece.astype(jnp.float32) for total, piece in zip(totals, cotangents))
        )
    gain_part = jnp.where(tensor_rank == 0, gain_total, 0.0)
    grad_q, grad_lat, grad_lg, grad_e, grad_o = totals
    out_q, part_lat, part_lg, out_e, out_o, part_gain = (
        lax.psum_scatter(grad_q.astype(jnp.bfloat16), "dp", scatter_dimension=0, tiled=True).astype(
            jnp.float32
        ),
        lax.psum_scatter(
            grad_lat.astype(jnp.bfloat16), "dp", scatter_dimension=0, tiled=True
        ).astype(jnp.float32),
        lax.psum_scatter(
            grad_lg.astype(jnp.bfloat16), "dp", scatter_dimension=0, tiled=True
        ).astype(jnp.float32),
        lax.psum_scatter(grad_e.astype(jnp.bfloat16), "dp", scatter_dimension=0, tiled=True).astype(
            jnp.float32
        ),
        lax.psum_scatter(grad_o.astype(jnp.bfloat16), "dp", scatter_dimension=1, tiled=True).astype(
            jnp.float32
        ),
        lax.psum_scatter(
            gain_part.astype(jnp.bfloat16), "dp", scatter_dimension=0, tiled=True
        ).astype(jnp.float32),
    )
    out_lat, out_lg, out_gain = (
        lax.psum(part_lat.astype(jnp.bfloat16), "tensor").astype(jnp.float32),
        lax.psum(part_lg.astype(jnp.bfloat16), "tensor").astype(jnp.float32),
        lax.psum(part_gain.astype(jnp.bfloat16), "tensor").astype(jnp.float32),
    )
    return (
        results[None],
        out_gain[None],
        out_q[None],
        out_lat[None],
        out_lg[None],
        out_e[None],
        out_o[None],
    )


MESH = pl.DeviceIdType.MESH
BF = jnp.bfloat16
F32 = jnp.float32


def mm(a, b):
    return lax.dot_general(a, b, (((1,), (0,)), ((), ())), preferred_element_type=F32)


def mm_nt(a, b):
    return lax.dot_general(a, b, (((1,), (1,)), ((), ())), preferred_element_type=F32)


def mm_tn(a, b):
    return lax.dot_general(a, b, (((0,), (0,)), ((), ())), preferred_element_type=F32)


def half_swap(v):
    lane = lax.broadcasted_iota(jnp.int32, v.shape, 1)
    ahead = pltpu.roll(v, v.shape[1] - ROPE // 2, 1)
    behind = pltpu.roll(v, ROPE // 2, 1)
    return jnp.where(lax.rem(lane, ROPE) < ROPE // 2, ahead, behind)


def section_kernel(
    dims,
    saved_in, top_in, gain_in, lgain_in, wq_in, wl_in, we_in, wo_in, cos_in, sin_in,
    ig_ref, gg_ref, gq_ref, gl_ref, glg_ref, ge_ref, go_ref,
    saved_ref, top_ref, gain_ref, lgain_ref, wq_ref, wl_ref, we_ref, wo_ref, cos_ref, sin_ref,
    x_v, xs_v, own_v, sm_v, nm_v, u_v, um_v, cb_v, wq_v, wl_v, we_v, wo_v,
    nc_v, cc_v, uc_v, dl_v, rk_v, ro_v, fo_v, fw_v, so_v, sv_v, part_v, rs_v, lp_v, ls_v, dx_v, sg_v, sr_v,
    dq_v, de_v,
    dp_s, dp_r, x_s, x_r, wz_s, wz_r, wh_s, wt_s, wt_r, w_s, w_r, f_s, f_r, z_s, z_r, zl_r, t_s, ta_r, tb_r,
    b_s, b_r, bh_s, rs_s, rs_r, p_s, u_r, um_r, uf_s, uf_r, sg_s, sg_r, in_s,
):
    n_pipe, n, n_t, micros, seq = dims
    sec, me, ten = lax.axis_index("pipe"), lax.axis_index("dp"), lax.axis_index("tensor")
    rows = micros * seq
    chunk = seq // n_t
    share = micros * chunk
    width = x_v.shape[1]
    wcol, ccol = wq_v.shape[1], we_v.shape[1]
    rank = n * ccol
    quarter = wl_v.shape[2]
    core = lax.rem(ten, 2)
    partner = ten + 1 - 2 * core
    opposite = lax.rem(ten + 2, n_t)
    par = lax.rem(me, 2)
    mate = me + 1 - 2 * par
    group = ten - core + par
    block = me - par + core
    primary = core == par
    secondary = jnp.logical_not(primary)
    half = me // 2
    near = 2 - half
    middle = jnp.logical_or(me == 1, me == 2)
    last = sec == n_pipe - 1
    lower = jnp.logical_not(last)
    both = jnp.logical_and
    drains = []

    def rcopy(a, b, ss, rs, dev):
        return pltpu.make_async_remote_copy(
            src_ref=a, dst_ref=b, send_sem=ss, recv_sem=rs, device_id=dev, device_id_type=MESH
        )

    def begin(cond, copy, sent=False):
        @pl.when(cond)
        def _():
            copy.start()

        if not sent:
            drains.append((cond, copy))

    def settle(cond, ref, ss):
        drains.append((cond, rcopy(ref, ref, ss, x_r.at[0], dev(me, partner))))

    def arrived(cond, ref, rs):
        @pl.when(cond)
        def _():
            rcopy(ref, ref, x_s.at[0], rs, dev(me, partner)).wait_recv()

    def dev(d, t):
        return (sec, d, t)

    def cols(j, size):
        return slice(j * size, (j + 1) * size)

    def mine(ref):
        at = pl.ds(pl.multiple_of(ten * chunk, chunk), chunk)
        return jnp.concatenate([ref[m, at] for m in range(micros)], axis=0)

    def by_share(store, ref):
        for j in range(n_t):
            for m in range(micros):
                store(j, m, ref[m, j * chunk : (j + 1) * chunk])

    def x_store(j, m, value):
        x_v[j * share + m * chunk : j * share + (m + 1) * chunk] = value

    def u_store(j, m, value):
        u_v[j, m * chunk : (m + 1) * chunk] = value

    inputs = (saved_in, top_in, gain_in, lgain_in, wq_in, wl_in, we_in, wo_in, cos_in, sin_in)
    places = (saved_ref, top_ref, gain_ref, lgain_ref, wq_ref, wl_ref, we_ref, wo_ref, cos_ref, sin_ref)
    fetches = [pltpu.make_async_copy(a, b, in_s.at[i]) for i, (a, b) in enumerate(zip(inputs, places))]
    for copy in fetches:
        copy.start()

    barrier = pltpu.get_barrier_semaphore()
    for j in range(n_t):
        for d in range(n):
            @pl.when(jnp.logical_or(d != me, j != ten))
            def _():
                pl.semaphore_signal(barrier, inc=1, device_id=dev(d, j), device_id_type=MESH)

        @pl.when(sec > 0)
        def _():
            pl.semaphore_signal(barrier, inc=1, device_id=(sec - 1, me, j), device_id_type=MESH)

        @pl.when(lower)
        def _():
            pl.semaphore_signal(barrier, inc=1, device_id=(sec + 1, me, j), device_id_type=MESH)

    for copy in fetches:
        copy.wait()

    own_v[:, :wcol] = jnp.broadcast_to(gain_ref[...].astype(F32), (8, wcol))
    own_v[:, wcol:] = jnp.broadcast_to(lgain_ref[...].astype(F32), (8, ccol))

    @pl.when(last)
    def _():
        um_v[...] = mine(top_ref)

    @pl.when(both(last, primary))
    def _():
        by_share(u_store, top_ref)

    neighbours = jnp.minimum(sec, 1) + jnp.minimum(n_pipe - 1 - sec, 1)
    pl.semaphore_wait(barrier, n * n_t - 1 + neighbours * n_t)

    def spread_dp(k, source, dest):
        for j in range(n):
            begin(j != me, rcopy(source(j), dest.at[me], dp_s.at[k], dp_r.at[k], dev(j, ten)), sent=True)
        settle(me >= 0, dest.at[pl.ds(0, n - 1)], dp_s.at[k])

    def collect_dp(k, dest):
        arrived(me >= 0, dest.at[pl.ds(0, n - 1)], dp_r.at[k])

    def spread_z(k, source, dest, slot, rank_to, gate=None):
        for e in range(n):
            cond = jnp.logical_or(e != me, rank_to != ten)
            if gate is not None:
                cond = both(cond, gate)
            rs = zl_r.at[slot] if k == 3 else z_r.at[k]
            begin(cond, rcopy(source(e), dest.at[slot, rank_to], z_s.at[k], rs, dev(e, rank_to)), sent=True)
        on = me >= 0 if gate is None else gate
        if k in (1, 4):
            settle(both(on, primary), dest.at[0, pl.ds(0, n - 1)], z_s.at[k])
            settle(both(on, secondary), dest.at[0, pl.ds(0, n)], z_s.at[k])
        else:
            settle(on, dest.at[0, pl.ds(0, n - 1)], z_s.at[k])

    def relay(k, dest, gate):
        def share_slot(b):
            for to, rs in ((opposite, ta_r), (partner, tb_r)):
                copy = rcopy(dest.at[b, ten], dest.at[b, ten], t_s.at[k], rs.at[k], dev(me, to))
                begin(gate, copy, sent=True)

        if k == 3:
            for b in range(n):
                arrived(both(b != me, gate), dest.at[b, ten], zl_r.at[b])
                share_slot(b)
        else:
            few, every = dest.at[pl.ds(0, n - 1), ten], dest.at[pl.ds(0, n), ten]
            if k in (1, 4):
                arrived(both(gate, primary), few, z_r.at[k])
                arrived(both(gate, secondary), every, z_r.at[k])
            else:
                arrived(gate, few, z_r.at[k])
            for b in range(n):
                share_slot(b)

    def pass_on(k, dest, gate=True):
        gate = both(me >= 0, gate)
        arrived(gate, dest.at[pl.ds(0, n), opposite], ta_r.at[k])
        for b in range(n):
            at = dest.at[b, opposite]
            begin(gate, rcopy(at, at, t_s.at[k], tb_r.at[k], dev(me, partner)), sent=True)
        settle(gate, dest.at[pl.ds(0, n - 1)], t_s.at[k])

    def collect(k, dest):
        arrived(me >= 0, dest.at[pl.ds(0, 2)], tb_r.at[k])

    def landing(k, b):
        return sv_v.at[b] if k == 3 else fw_v.at[b, k]

    def spread_block(k, gate, across):
        source = so_v if k == 3 else fo_v.at[k]
        for e in range(n):
            wanted = near == e if across else both(half == e // 2, jnp.logical_or(e != me, secondary))
            copy = rcopy(source, landing(k, block), b_s.at[k], b_r.at[k, block], dev(e, group))
            begin(both(wanted, gate), copy, sent=True)
        if across:
            several = lambda c: sv_v.at[pl.ds(0, c)] if k == 3 else fw_v.at[pl.ds(0, c), k]
            settle(both(gate, primary), several(2), b_s.at[k])
            settle(both(gate, secondary), several(3), b_s.at[k])

    def hand_on(k, gate, early=None):
        for b in range(n):
            cond = both(both(middle, half != b // 2), gate)
            if early is not None:
                cond = both(cond, core == b % 2 if early else core != b % 2)
            at = landing(k, b)
            arrived(cond, at, b_r.at[k, b])
            begin(cond, rcopy(at, at, bh_s.at[k], b_r.at[k, b], dev(mate, ten)), sent=True)
        two = sv_v.at[pl.ds(0, 2)] if k == 3 else fw_v.at[pl.ds(0, 2), k]
        if not early:
            settle(both(middle, gate), two, bh_s.at[k])

    def collect_block(k):
        for b in range(n):
            handed = both(middle, half != b // 2)
            cond = both(jnp.logical_or(b != me, secondary), jnp.logical_not(handed))
            arrived(cond, landing(k, b), b_r.at[k, b])

    spread_dp(0, lambda j: own_v, sm_v)
    sm_v[me] = own_v[...]
    my_quarter = wl_ref.at[pl.ds(pl.multiple_of(ten * quarter, quarter), quarter)]
    for level in (near, mate):
        begin(me >= 0, rcopy(my_quarter, wl_v.at[me, ten], wz_s.at[0], wz_r.at[me], dev(level, ten)), sent=True)
    settle(me >= 0, wl_v.at[0, pl.ds(0, 2)], wz_s.at[0])
    weights = ((wq_ref, wq_v), (we_ref, we_v), (wo_ref, wo_v))

    begin(primary, rcopy(saved_ref, xs_v, x_s.at[0], x_r.at[0], dev(mate, ten)))

    def give(k, gate=True):
        ref, store = weights[k]
        for i in range(n // 2):
            level = 2 * i + core
            copy = rcopy(ref, store.at[me], w_s.at[k], w_r.at[k, me], dev(level, ten))
            begin(both(level != me, gate), copy, sent=True)
        settle(both(primary, gate), store.at[pl.ds(0, n // 2 - 1)], w_s.at[k])
        settle(both(secondary, gate), store.at[pl.ds(0, n // 2)], w_s.at[k])
        copy = rcopy(ref, store.at[me], f_s.at[k], f_r.at[k], dev(me, partner))
        begin(both(primary, gate), copy, sent=True)

    def give_rest(gate):
        give(1, gate)
        for s in range(n_t):
            copy = rcopy(u_v.at[s], u_v.at[s], uf_s.at[0], uf_r.at[0], dev(mate, ten))
            begin(both(both(last, primary), gate), copy, sent=True)
        give(2, gate)
        spread_z(2, um_cols, uc_v, me, ten, gate=both(last, gate))

    um_cols = lambda e: um_v.at[:, pl.ds(e * wcol, wcol)]
    give(0)
    give_rest(jnp.logical_not(middle))

    for j in range(n_t):
        wl_v[me, j] = wl_ref[j * quarter : (j + 1) * quarter]

    @pl.when(primary)
    def _():
        for ref, store in weights:
            store[me] = ref[...]

        by_share(x_store, saved_ref)

    def to_ten(b, valid):
        for j in range(n_t):
            begin(
                both(valid, j != ten),
                rcopy(wl_v.at[b, ten], wl_v.at[b, ten], wt_s.at[0], wt_r.at[0], dev(me, j)),
                sent=True,
            )

    for b in range(n):
        arrived(b != me, wl_v.at[b, ten], wz_r.at[b])
        begin(
            both(middle, half != b // 2),
            rcopy(wl_v.at[b, ten], wl_v.at[b, ten], wh_s.at[0], wz_r.at[b], dev(mate, ten)),
            sent=True,
        )
        to_ten(b, b != me)
    settle(middle, wl_v.at[0, pl.ds(0, 2)], wh_s.at[0])
    wl_peers = wl_v.at[pl.ds(0, n - 1), pl.ds(0, n_t - 1)]
    settle(me >= 0, wl_peers, wt_s.at[0])
    give_rest(middle)

    collect_dp(0, sm_v)
    gain = jnp.concatenate([sm_v[d][0:1, :wcol] for d in range(n)], axis=1)
    lgain = jnp.concatenate([sm_v[d][0:1, wcol : wcol + ccol] for d in range(n)], axis=1)
    x_my = mine(saved_ref).astype(F32)
    r_my = lax.rsqrt(jnp.mean(x_my * x_my, axis=1, keepdims=True) + EPS)
    nm_v[...] = (x_my * r_my * gain).astype(BF)
    spread_z(0, lambda e: nm_v.at[:, pl.ds(e * wcol, wcol)], nc_v, me, ten)
    for j in range(n):
        @pl.when(j == me)
        def _():
            nc_v[j, ten] = nm_v[:, cols(j, wcol)]

    @pl.when(secondary)
    def _():
        rcopy(xs_v, xs_v, x_s.at[0], x_r.at[0], dev(me, partner)).wait_recv()
        by_share(x_store, xs_v)

    x32 = x_v[...].astype(F32)
    r = lax.rsqrt(jnp.mean(x32 * x32, axis=1, keepdims=True) + EPS)
    nb = (x32 * r * gain).astype(BF)

    def take(k):
        store = weights[k][1]
        for d in range(n):
            cond = both(primary, d != me)
            arrived(cond, store.at[d], w_r.at[k, d])
            begin(cond, rcopy(store.at[d], store.at[d], f_s.at[k], f_r.at[k], dev(me, partner)), sent=True)
        settle(primary, store, f_s.at[k])
        arrived(secondary, store, f_r.at[k])

    take(0)
    arrived(me >= 0, wl_peers, wt_r.at[0])

    wq = wq_v[...].reshape(width, wq_v.shape[2])
    wl = [wl_v[d].reshape(n_t * quarter, wcol) for d in range(n)]
    q = mm(nb, wq)
    lat = jnp.zeros((rows, n_t * quarter), F32)
    for d in range(n):
        lat = lat + mm_nt(nb[:, cols(d, wcol)], wl[d])
    l32 = lat[:, :rank]
    rl = lax.rsqrt(jnp.mean(l32 * l32, axis=1, keepdims=True) + EPS)
    cb = (l32 * rl * lgain).astype(BF)
    cb_v[...] = cb
    my_rows = pl.ds(pl.multiple_of(group * share, share), share)
    spread_z(1, lambda e: cb_v.at[my_rows, pl.ds(e * ccol, ccol)], cc_v, block, group)
    for j in range(n):
        @pl.when(both(j == me, primary))
        def _():
            cc_v[j, ten] = cb_v[my_rows, cols(j, ccol)]

    cosine, sine = cos_ref[...], sin_ref[...]
    lr = lat[:, rank:]
    lr2 = jnp.concatenate([lr, lr], axis=1)
    rk = (lr2 * cosine + half_swap(lr2) * sine).astype(BF)
    ro_v[...] = rk
    spread_z(4, lambda e: ro_v.at[my_rows], rk_v, block, group)

    @pl.when(primary)
    def _():
        rk_v[me, ten] = ro_v[my_rows]

    lane = lax.broadcasted_iota(jnp.int32, (rows, 2 * ROPE), 1)
    low = lane < ROPE
    q1, q2 = q[:, NOPE : 2 * NOPE], q[:, 2 * NOPE :]
    nope = (q[:, :NOPE], pltpu.roll(jnp.where(low, q2, q1), ROPE, 1))
    for h in range(2):
        fo_v[0, :, cols(h, NOPE)] = nope[h].astype(BF)
    spread_block(0, lower, True)
    spread_block(0, lower, False)
    qr_all = jnp.where(low, q1, q2)
    qr = qr_all * cosine + half_swap(qr_all) * sine
    row = lax.broadcasted_iota(jnp.int32, (rows, rows), 0)
    col = lax.broadcasted_iota(jnp.int32, (rows, rows), 1)

    def place(i):
        return (i // share) * chunk + lax.rem(i, chunk)

    same = lax.rem(row, share) // chunk == lax.rem(col, share) // chunk
    keep = jnp.logical_and(same, place(row) >= place(col))
    picks = [jnp.where(place(row) + h * seq == col, 1.0, 0.0).astype(BF) for h in range(2)]
    scale = (NOPE + ROPE) ** (-0.5)
    masks = (low, jnp.logical_not(low))
    take(1)
    we = we_v[...].reshape(n * ccol, we_v.shape[2])
    ex = mm(cb, we)
    for h in range(2):
        fo_v[1, :, cols(h, NOPE)] = ex[:, cols(2 * h, NOPE)].astype(BF)
    spread_block(1, lower, True)
    spread_block(1, lower, False)
    heads = []
    for h in range(2):
        qn = nope[h].astype(BF)
        kn = ex[:, h * (NOPE + VDIM) : h * (NOPE + VDIM) + NOPE].astype(BF)
        vv = ex[:, h * (NOPE + VDIM) + NOPE : (h + 1) * (NOPE + VDIM)].astype(BF)
        qh = jnp.where(masks[h], qr, 0.0).astype(BF)
        scores = (mm_nt(qn, kn) + mm_nt(qh, rk)) * scale
        scores = jnp.where(keep, scores, -1e30)
        e = jnp.exp(scores - jnp.max(scores, axis=1, keepdims=True))
        w32 = e / jnp.sum(e, axis=1, keepdims=True)
        wb = w32.astype(BF)
        fo_v[2, :, cols(h, VDIM)] = mm(wb, vv).astype(BF)
        heads.append((qn, kn, vv, qh, w32, wb))

    @pl.when(primary)
    def _():
        fw_v[me] = fo_v[...]

    spread_block(2, lower, True)
    spread_block(2, lower, False)
    take(2)
    relay(0, nc_v, gate=lower)
    relay(1, cc_v, gate=lower)
    relay(4, rk_v, gate=lower)
    for k in range(3):
        hand_on(k, lower)

    for s in range(n_t):
        cond = both(lower, primary)
        arrived(cond, u_v.at[s], u_r.at[s])
        begin(cond, rcopy(u_v.at[s], u_v.at[s], uf_s.at[0], uf_r.at[0], dev(mate, ten)), sent=True)
    settle(primary, u_v, uf_s.at[0])

    @pl.when(both(lower, primary))
    def _():
        um_v[...] = u_v[ten]

    arrived(both(lower, secondary), um_v, um_r.at[0])
    spread_z(2, um_cols, uc_v, me, ten, gate=lower)
    for j in range(n):
        @pl.when(j == me)
        def _():
            uc_v[j, ten] = um_v[:, cols(j, wcol)]

    arrived(secondary, u_v, uf_r.at[0])

    ub = u_v[...].reshape(rows, width)
    dm = jnp.zeros((rows, wo_v.shape[1]), F32)
    for j in range(n):
        dm = dm + mm_nt(ub[:, cols(j, wcol)], wo_v[j])
    dm = dm.astype(BF)

    def query_grad(slope, kn0, kn1, rk_b):
        dqr = jnp.where(low, mm(slope[0], rk_b), mm(slope[1], rk_b))
        dqr = dqr * cosine - half_swap(dqr) * sine
        turned = pltpu.roll(mm(slope[1], kn1), ROPE, 1)
        return jnp.concatenate(
            [
                mm(slope[0], kn0).astype(BF),
                jnp.where(low, dqr, turned).astype(BF),
                jnp.where(low, turned, dqr).astype(BF),
            ],
            axis=1,
        )

    drk = jnp.zeros((rows, 2 * ROPE), F32)
    slopes, pieces = [], []
    for h, (qn, kn, vv, qh, w32, wb) in enumerate(heads):
        dmh = dm[:, cols(h, VDIM)]
        dw = mm_nt(dmh, vv).astype(BF).astype(F32)
        ds = (w32 * (dw - jnp.sum(dw * w32, axis=1, keepdims=True)) * scale).astype(BF)
        drk = drk + mm_tn(ds, qh)
        slopes.append(ds)
        pieces += [mm_tn(ds, qn).astype(BF), mm_tn(wb, dmh).astype(BF)]
    drk = drk * cosine - half_swap(drk) * sine
    drk = drk + pltpu.roll(drk, ROPE, 1)
    so_v[:, cols(0, NOPE)] = (mm(slopes[0], picks[0]) + mm(slopes[1], picks[1])).astype(BF)
    so_v[:, cols(1, VDIM)] = pieces[1]
    so_v[:, cols(2, VDIM)] = pieces[3]
    dc = mm_nt(jnp.concatenate(pieces, axis=1), we)
    dlg = jnp.sum(dc * l32 * rl, axis=0, keepdims=True)
    dcg = dc * lgain
    dl = rl * dcg - l32 * (rl * rl * rl) * jnp.mean(l32 * dcg, axis=1, keepdims=True)
    dlat = jnp.concatenate([dl.astype(BF), drk[:, :ROPE].astype(BF)], axis=1)
    lp_v[...] = dlat.reshape(n_t, share, dlat.shape[1])

    @pl.when(primary)
    def _():
        ls_v[group] = lp_v[ten]

    shared = ((part_v, rs_v), (lp_v, ls_v))

    def share_out(k, gate):
        source, dest = shared[k]
        for i in range(n_t):
            s = lax.rem(ten - core + 2 + i, n_t)
            copy = rcopy(source.at[s], dest.at[group], rs_s.at[k], rs_r.at[k], dev(block, s))
            begin(both(jnp.logical_or(s != ten, secondary), gate), copy, sent=True)
        settle(both(primary, gate), dest.at[pl.ds(0, n_t - 1)], rs_s.at[k])
        settle(both(secondary, gate), dest, rs_s.at[k])

    share_out(1, lower)
    dq = query_grad(slopes, heads[0][1], heads[1][1], rk)
    dn = mm_nt(dq, wq) + jnp.concatenate([mm(dlat, wl[d]) for d in range(n)], axis=1)
    part_v[...] = dn.astype(BF).reshape(n_t, share, width)

    @pl.when(primary)
    def _():
        rs_v[group] = part_v[ten]
        sv_v[me] = so_v[...]

    share_out(0, last)
    share_out(1, last)
    spread_block(3, lower, False)
    spread_block(3, lower, True)

    def collect_shares(k, gate=True):
        dest = shared[k][1]
        arrived(both(primary, gate), dest.at[pl.ds(0, n_t - 1)], rs_r.at[k])
        arrived(both(secondary, gate), dest, rs_r.at[k])

    def sum_latent(gate):
        collect_shares(1, gate)

        @pl.when(gate)
        def _():
            dl_v[me, ten] = jnp.sum(ls_v[...].astype(F32), axis=0).astype(BF)

        spread_z(3, lambda e: dl_v.at[me, ten], dl_v, me, ten, gate=gate)

    for k, dest in ((0, nc_v), (1, cc_v), (4, rk_v)):
        pass_on(k, dest, lower)
    hand_on(3, lower, early=True)
    sum_latent(lower)
    share_out(0, lower)
    relay(2, uc_v, gate=lower)
    hand_on(3, lower, early=False)
    relay(3, dl_v, gate=lower)
    lanes = 128
    below = jnp.maximum(sec - 1, 0)

    def finish(gate):
        collect_shares(0, gate)

        @pl.when(gate)
        def _():
            dns = jnp.sum(rs_v[...].astype(F32), axis=0)
            dng = dns * gain
            u_my = um_v[...].astype(F32)
            dx = u_my + r_my * dng - x_my * (r_my * r_my * r_my) * jnp.mean(x_my * dng, axis=1, keepdims=True)
            dx_v[...] = dx.astype(BF)

        for i in range(n_t // 2):
            to = lax.rem(ten - core + 2 + 2 * i, n_t) + par
            copy = rcopy(dx_v, u_v.at[ten], p_s.at[i], u_r.at[ten], (below, me, to))
            begin(both(sec > 0, gate), copy)
        copy = rcopy(dx_v, um_v, p_s.at[n_t // 2], um_r.at[0], (below, me, ten))
        begin(both(both(sec > 0, secondary), gate), copy)

        @pl.when(gate)
        def _():
            dgain = jnp.sum(jnp.sum(rs_v[...].astype(F32), axis=0) * x_my * r_my, axis=0, keepdims=True)
            for j in range(n):
                piece = jnp.concatenate([dgain[:, cols(j, wcol)], dlg[:, cols(j, ccol)]], axis=1)
                for i in range(piece.shape[1] // lanes):
                    sg_v[j, i : i + 1] = piece[:, cols(i, lanes)]
            sr_v[me * n_t + ten] = sg_v[me]
            for m in range(micros):
                ig_ref[m] = dx_v[m * chunk : (m + 1) * chunk]

        for j in range(n):
            for t in range(n_t):
                copy = rcopy(sg_v.at[j], sr_v.at[me * n_t + ten], sg_s.at[0], sg_r.at[0], dev(j, t))
                begin(both(jnp.logical_or(j != me, t != ten), gate), copy, sent=True)
        settle(gate, sr_v.at[pl.ds(0, n * n_t - 1)], sg_s.at[0])

    finish(lower)
    finish(last)
    for across in (True, False):
        for k in range(4):
            spread_block(k, last, across)
    sum_latent(last)
    relay(0, nc_v, gate=last)
    relay(1, cc_v, gate=last)
    relay(4, rk_v, gate=last)
    relay(2, uc_v, gate=last)
    for k, dest in ((0, nc_v), (1, cc_v), (4, rk_v)):
        pass_on(k, dest, last)
    for k in range(4):
        hand_on(k, last)
    relay(3, dl_v, gate=last)
    for k in range(4):
        collect_block(k)
    pass_on(2, uc_v)
    collect(4, rk_v)
    for b in range(n):
        few = sv_v[b, :, :NOPE]
        ds = [jnp.where(same, mm_nt(few, picks[h]), 0.0).astype(BF) for h in range(2)]
        part = lambda i: fw_v[b, i // 2, :, cols(i % 2, NOPE)]
        dq_v[b] = query_grad(ds, part(2), part(3), rk_v[b].reshape(rows, 2 * ROPE))
        for h in range(2):
            de_v[b, :, cols(2 * h, NOPE)] = mm_tn(ds[h], part(h)).astype(BF)
            de_v[b, :, cols(2 * h + 1, NOPE)] = sv_v[b, :, cols(1 + h, VDIM)]
    pass_on(3, dl_v)
    collect(0, nc_v)
    collect(1, cc_v)
    gq_ref[...] = mm_tn(nc_v[...].reshape(n * rows, wcol), dq_v[...].reshape(n * rows, dq_v.shape[2]))
    ge_ref[...] = mm_tn(cc_v[...].reshape(n * rows, ccol), de_v[...].reshape(n * rows, de_v.shape[2]))
    collect(2, uc_v)
    mixed = fw_v[:, 2].reshape(n * rows, 2 * VDIM)
    go_ref[...] = mm_tn(mixed, uc_v[...].reshape(n * rows, wcol))
    collect(3, dl_v)
    gl_ref[...] = mm_tn(dl_v[...].reshape(n * rows, dl_v.shape[3]), nc_v[...].reshape(n * rows, wcol))
    arrived(me >= 0, sr_v.at[pl.ds(0, n * n_t - 1)], sg_r.at[0])
    summed = jnp.sum(sr_v[...], axis=0)
    for i in range(wcol // lanes):
        gg_ref[:, cols(i, lanes)] = summed[i : i + 1]
    for i in range(ccol // lanes):
        glg_ref[:, cols(i, lanes)] = summed[wcol // lanes + i : wcol // lanes + i + 1]
    for cond, copy in drains:
        @pl.when(cond)
        def _(copy=copy):
            copy.wait_send()


def hand_over(*refs):
    copies = [pltpu.make_async_copy(refs[i], refs[7 + i], refs[14].at[i]) for i in range(7)]
    for copy in copies:
        copy.start()
    for copy in copies:
        copy.wait()


def section_step(saved, top_grad, gain, w_query, w_latent, compressed_gain, expand_weight, w_output):
    n_pipe, n, n_t = (lax.axis_size(a) for a in ("pipe", "dp", "tensor"))
    micros, seq, width = saved.shape[1:]
    wcol, ccol = gain.shape[1], compressed_gain.shape[1]
    rows, share = micros * seq, micros * seq // n_t
    qcols, lcols = w_query.shape[2], w_latent.shape[2]
    ecols, orows = expand_weight.shape[2], w_output.shape[1]
    order = np.arange(rows)
    place = (order // share) * (seq // n_t) + order % (seq // n_t)
    pair = np.arange(2 * ROPE) % (ROPE // 2)
    angle = place[:, None] * np.exp(-np.log(10000.0) * pair / (ROPE // 2))[None, :]
    sign = np.where(np.arange(2 * ROPE) % ROPE < ROPE // 2, -1.0, 1.0)
    cosine = jnp.asarray(np.cos(angle), F32)
    sine = jnp.asarray(np.sin(angle) * sign, F32)
    operands = (
        saved[0], top_grad, gain, compressed_gain, w_query[0], w_latent[0].T,
        expand_weight[0], w_output[0], cosine, sine,
    )
    vm = pl.BlockSpec(memory_space=pltpu.VMEM)
    shape = jax.ShapeDtypeStruct
    kept = pltpu.VMEM
    sem = lambda *dims: pltpu.SemaphoreType.DMA(dims)
    small = wcol + ccol
    ig, gg, gq, gl, glg, ge, go = pl.pallas_call(
        lambda *refs: section_kernel((n_pipe, n, n_t, micros, seq), *refs),
        name="section_step",
        out_shape=(
            kept((micros, seq // n_t, width), BF),
            kept((1, wcol), F32),
            kept((wcol, qcols), F32),
            kept((lcols, wcol), F32),
            kept((1, ccol), F32),
            kept((ccol, ecols), F32),
            kept((orows, wcol), F32),
        ),
        in_specs=[pl.BlockSpec(memory_space=pl.ANY)] * 10,
        out_specs=(vm,) * 7,
        scratch_shapes=[
            *(pltpu.VMEM(a.shape, a.dtype) for a in operands),
            pltpu.VMEM((rows, width), BF),
            pltpu.VMEM((micros, seq, width), BF),
            pltpu.VMEM((8, small), F32),
            pltpu.VMEM((n, 8, small), F32),
            pltpu.VMEM((share, width), BF),
            pltpu.VMEM((n_t, share, width), BF),
            pltpu.VMEM((share, width), BF),
            pltpu.VMEM((rows, n * ccol), BF),
            pltpu.VMEM((n, wcol, qcols), BF),
            pltpu.VMEM((n, n_t, lcols // n_t, wcol), BF),
            pltpu.VMEM((n, ccol, ecols), BF),
            pltpu.VMEM((n, orows, wcol), BF),
            pltpu.VMEM((n, n_t, share, wcol), BF),
            pltpu.VMEM((n, n_t, share, ccol), BF),
            pltpu.VMEM((n, n_t, share, wcol), BF),
            pltpu.VMEM((n, n_t, share, lcols), BF),
            pltpu.VMEM((n, n_t, share, 2 * ROPE), BF),
            pltpu.VMEM((rows, 2 * ROPE), BF),
            pltpu.VMEM((3, rows, orows), BF),
            pltpu.VMEM((n, 3, rows, orows), BF),
            pltpu.VMEM((rows, NOPE + orows), BF),
            pltpu.VMEM((n, rows, NOPE + orows), BF),
            pltpu.VMEM((n_t, share, width), BF),
            pltpu.VMEM((n_t, share, width), BF),
            pltpu.VMEM((n_t, share, lcols), BF),
            pltpu.VMEM((n_t, share, lcols), BF),
            pltpu.VMEM((share, width), BF),
            pltpu.VMEM((n, 8 * -(-small // 1024), 128), F32),
            pltpu.VMEM((n * n_t, 8 * -(-small // 1024), 128), F32),
            pltpu.VMEM((n, rows, qcols), BF),
            pltpu.VMEM((n, rows, ecols), BF),
            sem(1), sem(1), sem(1), sem(1), sem(1), sem(n), sem(1), sem(1), sem(1),
            sem(3), sem(3, n), sem(3), sem(3), sem(5), sem(5), sem(n), sem(5), sem(5), sem(5),
            sem(4), sem(4, n), sem(4), sem(2), sem(2), sem(n_t // 2 + 1), sem(n_t), sem(1), sem(1), sem(1),
            sem(1), sem(1), sem(len(operands)),
        ],
        compiler_params=pltpu.CompilerParams(
            collective_id=0, has_side_effects=True, vmem_limit_bytes=60 * 1024 * 1024
        ),
    )(*operands)
    parts = [pltpu.with_memory_space_constraint(p, pltpu.VMEM) for p in (ig, gg, gq, gl, glg, ge, go)]
    ig, gg, gq, gl, glg, ge, go = pl.pallas_call(
        hand_over,
        name="hand_over",
        out_shape=tuple(shape(p.shape, p.dtype) for p in parts),
        in_specs=[vm] * 7,
        out_specs=(pl.BlockSpec(memory_space=pl.ANY),) * 7,
        scratch_shapes=[sem(7)],
    )(*parts)
    return ig[None], gg, gq[None], gl.T[None], glg, ge[None], go[None]


def choose(saved, top_grad, gain, w_query, w_latent, compressed_gain, expand_weight, w_output):
    arrays = (saved, top_grad, gain, w_query, w_latent, compressed_gain, expand_weight, w_output)
    n, n_t = lax.axis_size("dp"), lax.axis_size("tensor")
    fits = (
        n == 4
        and n_t == 4
        and saved.shape[1] == 2
        and saved.shape[2] == ROPE
        and w_query.shape[2] == 2 * (NOPE + ROPE)
        and w_output.shape[1] == 2 * VDIM
        and gain.shape[1] % 128 == 0
        and compressed_gain.shape[1] % 128 == 0
        and n * compressed_gain.shape[1] + ROPE == w_latent.shape[2]
        and w_latent.shape[2] % (16 * n_t) == 0
    )
    return section_step(*arrays) if fits else shards(*arrays)


def solution(mesh):
    in_specs = (
        P("pipe", None, "dp", None),
        P(None, "dp", None),
        P("pipe", "dp"),
        P("pipe", "dp", "tensor"),
        P("pipe", "dp", None),
        P("pipe", "dp"),
        P("pipe", "dp", "tensor"),
        P("pipe", "tensor", "dp"),
    )
    out_specs = (
        P("pipe", None, ("dp", "tensor"), None),
        P("pipe", "dp"),
        P("pipe", "dp", "tensor"),
        P("pipe", "dp", None),
        P("pipe", "dp"),
        P("pipe", "dp", "tensor"),
        P("pipe", "tensor", "dp"),
    )
    return jax.shard_map(choose, mesh=mesh, in_specs=in_specs, out_specs=out_specs, check_vma=False)
```
